8 devices in a mesh: dp: 1 (over z), tp: 2 (over y), ctx: 4 (over x, core).
Axes of the slice: x: 2, y: 2, z: 1, core: 2. Of those that a mesh axis runs over, the one named last changes fastest.
Arguments:
- x_tokens: bfloat16 [1024, 6144], P(('dp', 'ctx'))
- positions: int32 [1024], P(('dp', 'ctx'))
- w_dq: bfloat16 [6144, 1536], replicated
- g_q: bfloat16 [1536], replicated
- w_uq: bfloat16 [1536, 8192], P(None, 'tp')
- w_qr: bfloat16 [1536, 4096], P(None, 'tp')
- w_dkv: bfloat16 [6144, 512], replicated
- g_kv: bfloat16 [512], replicated
- w_kr: bfloat16 [6144, 64], replicated
- w_uk: bfloat16 [512, 8192], P(None, 'tp')
- w_uv: bfloat16 [512, 8192], P(None, 'tp')
- w_o: bfloat16 [8192, 6144], P('tp')
Outputs:
- output: bfloat16 [1024, 6144], P(('dp', 'ctx'))
All inputs are finite; a program needn't handle non-finite values.
Results may differ from the reference program's by a relative error of at most 0.00851886.
Values are sent between devices in bfloat16 or wider.
A program may use at most 1 GiB of HBM per device.

```python
import jax
import jax.numpy as jnp
from jax import lax

MODEL_DIM = 6144
NUM_HEADS = 64
QUERY_RANK = 1536
LATENT_RANK = 512
NOPE_DIM = 128
ROPE_DIM = 64
VALUE_DIM = 128
CTX_SIZE = 4
SEQ_LEN = 1024
QUERY_BLOCK = 64
PIECE_LEN = SEQ_LEN // (2 * CTX_SIZE)
ROPE_BASE = 10000.0
NORM_EPS = 1e-6


def draw_weight(key, fan_in, fan_out, gain):
    return (jax.random.normal(key, (fan_in, fan_out), jnp.float32) * gain).astype(jnp.bfloat16)


def draw_positions(pos_key):
    step_key, start_key = jax.random.split(pos_key)
    pos_steps = jax.random.randint(step_key, (SEQ_LEN,), 1, 3, jnp.int32)
    pos_start = jax.random.randint(start_key, (), 0, SEQ_LEN, jnp.int32)
    logical = (pos_start + jnp.cumsum(pos_steps)).astype(jnp.int32)
    pos_pieces = logical.reshape(2 * CTX_SIZE, PIECE_LEN)
    stored = jnp.stack([pos_pieces[:CTX_SIZE], pos_pieces[CTX_SIZE:][::-1]], axis=1)
    return stored.reshape(SEQ_LEN)


def setup_inputs(seed: int = 0, part: int = 0) -> dict:
    base_key = jax.random.key(seed)
    weight_keys = jax.random.split(base_key, 10)
    part_key = jax.random.fold_in(base_key, part)
    tok_key, pos_key = jax.random.split(part_key)
    x_tokens = jax.random.normal(tok_key, (SEQ_LEN, MODEL_DIM), jnp.float32).astype(jnp.bfloat16)
    out_gain = (NUM_HEADS * VALUE_DIM) ** -0.5 * SEQ_LEN ** 0.25
    return {
        'x_tokens': x_tokens,
        'positions': draw_positions(pos_key),
        'w_dq': draw_weight(weight_keys[0], MODEL_DIM, QUERY_RANK, MODEL_DIM ** -0.5),
        'g_q': jax.random.uniform(weight_keys[1], (QUERY_RANK,), jnp.float32, 0.5, 1.5).astype(jnp.bfloat16),
        'w_uq': draw_weight(weight_keys[2], QUERY_RANK, NUM_HEADS * NOPE_DIM, QUERY_RANK ** -0.5),
        'w_qr': draw_weight(weight_keys[3], QUERY_RANK, NUM_HEADS * ROPE_DIM, QUERY_RANK ** -0.5),
        'w_dkv': draw_weight(weight_keys[4], MODEL_DIM, LATENT_RANK, MODEL_DIM ** -0.5),
        'g_kv': jax.random.uniform(weight_keys[5], (LATENT_RANK,), jnp.float32, 0.5, 1.5).astype(jnp.bfloat16),
        'w_kr': draw_weight(weight_keys[6], MODEL_DIM, ROPE_DIM, MODEL_DIM ** -0.5),
        'w_uk': draw_weight(weight_keys[7], LATENT_RANK, NUM_HEADS * NOPE_DIM, LATENT_RANK ** -0.5),
        'w_uv': draw_weight(weight_keys[8], LATENT_RANK, NUM_HEADS * VALUE_DIM, LATENT_RANK ** -0.5),
        'w_o': draw_weight(weight_keys[9], NUM_HEADS * VALUE_DIM, MODEL_DIM, out_gain),
    }


def rms_norm(act_in, gain_vec):
    inv_rms = lax.rsqrt(jnp.mean(act_in * act_in, axis=-1, keepdims=True) + NORM_EPS)
    return act_in * inv_rms * gain_vec.astype(jnp.float32)


def rope_tables(pos_vals):
    half_dim = ROPE_DIM // 2
    inv_freq = ROPE_BASE ** (-jnp.arange(half_dim, dtype=jnp.float32) * 2.0 / ROPE_DIM)
    angles = pos_vals.astype(jnp.float32)[..., None] * inv_freq
    return jnp.cos(angles), jnp.sin(angles)


def apply_rope(act_in, cos_t, sin_t):
    half_dim = act_in.shape[-1] // 2
    first_half = act_in[..., :half_dim]
    second_half = act_in[..., half_dim:]
    return jnp.concatenate([first_half * cos_t - second_half * sin_t, second_half * cos_t + first_half * sin_t], axis=-1)


def reference(x_tokens, positions, w_dq, g_q, w_uq, w_qr, w_dkv, g_kv, w_kr, w_uk, w_uv, w_o):
    cos_t, sin_t = rope_tables(positions)
    c_q = rms_norm(jnp.dot(x_tokens, w_dq, preferred_element_type=jnp.float32), g_q).astype(jnp.bfloat16)
    q_nope = jnp.dot(c_q, w_uq, preferred_element_type=jnp.float32).astype(jnp.bfloat16)
    q_rot = jnp.dot(c_q, w_qr, preferred_element_type=jnp.float32).reshape(SEQ_LEN, NUM_HEADS, ROPE_DIM)
    q_pe = apply_rope(q_rot, cos_t[:, None, :], sin_t[:, None, :]).astype(jnp.bfloat16)
    c_kv = rms_norm(jnp.dot(x_tokens, w_dkv, preferred_element_type=jnp.float32), g_kv).astype(jnp.bfloat16)
    k_pe = apply_rope(jnp.dot(x_tokens, w_kr, preferred_element_type=jnp.float32), cos_t, sin_t).astype(jnp.bfloat16).astype(jnp.float32)
    k_nope = jnp.dot(c_kv, w_uk, preferred_element_type=jnp.float32).astype(jnp.bfloat16).astype(jnp.float32).reshape(SEQ_LEN, NUM_HEADS, NOPE_DIM)
    values = jnp.dot(c_kv, w_uv, preferred_element_type=jnp.float32).astype(jnp.bfloat16).astype(jnp.float32).reshape(SEQ_LEN, NUM_HEADS, VALUE_DIM)
    score_scale = (NOPE_DIM + ROPE_DIM) ** -0.5
    block_count = SEQ_LEN // QUERY_BLOCK

    def attend_block(q_block):
        qn_blk, qp_blk, qpos_blk = q_block
        scores = jnp.einsum('qhn,khn->hqk', qn_blk.astype(jnp.float32), k_nope) + jnp.einsum('qhr,kr->hqk', qp_blk.astype(jnp.float32), k_pe)
        visible = positions[None, None, :] <= qpos_blk[None, :, None]
        scores = jnp.where(visible, scores * score_scale, -jnp.inf)
        prob_tile = jax.nn.softmax(scores, axis=-1)
        return jnp.einsum('hqk,khv->qhv', prob_tile, values).astype(jnp.bfloat16)

    attn_out = lax.map(attend_block, (q_nope.reshape(block_count, QUERY_BLOCK, NUM_HEADS, NOPE_DIM), q_pe.reshape(block_count, QUERY_BLOCK, NUM_HEADS, ROPE_DIM), positions.reshape(block_count, QUERY_BLOCK)))
    attn_out = attn_out.reshape(SEQ_LEN, NUM_HEADS * VALUE_DIM)
    return jnp.dot(attn_out, w_o, preferred_element_type=jnp.float32).astype(jnp.bfloat16)
```

```python
import functools

import jax
import jax.numpy as jnp
from jax import lax
from jax.experimental import pallas as pl
from jax.experimental.pallas import tpu as pltpu
from jax.sharding import PartitionSpec as P

ROPE_BASE = 10000.0
NORM_EPS = 1e-6
NEG_BIG = -1e30
MESH = pl.DeviceIdType.MESH
F32 = jnp.float32
BF16 = jnp.bfloat16

KCH = 6
NBLK = 256
RING = 3
WO_SLOTS = 9


def _dot(a, b):
    return jnp.dot(a, b, preferred_element_type=F32)


def _dot_nt(a, b):
    return lax.dot_general(a, b, (((1,), (1,)), ((), ())), preferred_element_type=F32)


def layer_kernel(dims, x_hbm, pos_ref, wdq_hbm, gq_ref, wuq_hbm, wqr_hbm, wdkv_hbm, gkv_ref, wkr_hbm, wuk_hbm, wuv_hbm,
                 wo_hbm, y_hbm,
                 xv, wkv, wkr, arena, lat, kplo, kphi, cq, accq, acckv, acckr, cosr, sinr,
                 uqb, qrb, ukb, uvb, ov, sendb, recvb, ownb, resb,
                 xsem, kvsem, krsem, bsem, csem, wosem, lats, latr, ps, pr, rs, rr, ys):
    D, QR, LR, HL, half, score_scale = dims
    nheads2 = HL // 2
    kc = D // KCH
    nb_q = QR // NBLK
    own_cols = D // 2
    nblk = own_cols // NBLK
    hv = HL * 128
    tp = lax.axis_index("tp")
    ci = lax.axis_index("ctx")
    xpeer = lax.rem(ci + 2, 4)
    dpeer = ci + 1 - 2 * lax.rem(ci, 2)

    def a_copies(k):
        col = pl.multiple_of(k * kc, 128)
        return (pltpu.make_async_copy(x_hbm.at[:, pl.ds(col, kc)], xv.at[:, pl.ds(col, kc)], xsem.at[k]),
                pltpu.make_async_copy(wdkv_hbm.at[pl.ds(col, kc), :], wkv.at[k], kvsem.at[k]),
                pltpu.make_async_copy(wkr_hbm.at[:, pl.ds(col, kc)], wkr.at[k], krsem.at[k]))

    def b_copy(n):
        return pltpu.make_async_copy(wdq_hbm.at[:, pl.ds(pl.multiple_of(n * NBLK, NBLK), NBLK)],
                                     arena.at[pl.ds(pl.multiple_of(n * D, D), D), :], bsem.at[n])

    def c_copies(g):
        hp = lax.rem(g, nheads2)
        s = lax.rem(g, RING)
        c2 = pl.ds(pl.multiple_of(hp * 256, 256), 256)
        c1 = pl.ds(pl.multiple_of(hp * 128, 128), 128)
        return (pltpu.make_async_copy(wuq_hbm.at[:, c2], uqb.at[s], csem.at[s, 0]),
                pltpu.make_async_copy(wqr_hbm.at[:, c1], qrb.at[s], csem.at[s, 1]),
                pltpu.make_async_copy(wuk_hbm.at[:, c2], ukb.at[s], csem.at[s, 2]),
                pltpu.make_async_copy(wuv_hbm.at[:, c2], uvb.at[s], csem.at[s, 3]))

    def wo_copy(L):
        j = lax.rem(L, nblk)
        side = jnp.where(L < 2 * nblk, 1 - tp, tp)
        s = lax.rem(L, WO_SLOTS)
        col = pl.multiple_of(side * own_cols + j * NBLK, NBLK)
        return pltpu.make_async_copy(wo_hbm.at[:, pl.ds(col, NBLK)],
                                     arena.at[pl.ds(pl.multiple_of(s * hv, hv), hv), :], wosem.at[s])

    def start(cps):
        for c in cps:
            c.start()

    def wait(cps):
        for c in cps:
            c.wait()

    for k in range(KCH):
        start(a_copies(k))
    b_copy(0).start()

    bar = pltpu.get_barrier_semaphore()
    for dev in ({"tp": 1 - tp}, {"ctx": xpeer}, {"ctx": dpeer}):
        pl.semaphore_signal(bar, inc=1, device_id=dev, device_id_type=MESH)

    lane = lax.broadcasted_iota(jnp.int32, (1, 128), 1)
    fidx = lax.rem(lane, 32)
    freq = jnp.zeros((1, 128), F32)
    for j in range(32):
        freq = jnp.where(fidx == j, ROPE_BASE ** (-j * 2.0 / 64), freq)
    first_half = lax.rem(lane, 64) < 32
    eye = lax.broadcasted_iota(jnp.int32, (128, 128), 0) == lax.broadcasted_iota(jnp.int32, (128, 128), 1)
    for hf in range(2):
        prow = pos_ref[hf:hf + 1, :].astype(F32)
        pcol = jnp.sum(jnp.where(eye, jnp.broadcast_to(prow, (128, 128)), 0.0), axis=1, keepdims=True)
        ang = pcol * freq
        cosr[hf * half:(hf + 1) * half, :] = jnp.cos(ang)
        sn = jnp.sin(ang)
        sinr[hf * half:(hf + 1) * half, :] = jnp.where(first_half, -sn, sn)

    def rope(a, row0):
        n = a.shape[0]
        swapped = jnp.where(first_half, pltpu.roll(a, 96, 1), pltpu.roll(a, 32, 1))
        return a * cosr[row0:row0 + n, :] + swapped * sinr[row0:row0 + n, :]

    acckv[...] = jnp.zeros_like(acckv)
    acckr[...] = jnp.zeros_like(acckr)

    def a_step(k, carry):
        @pl.when(k >= 1)
        def _():
            b_copy(k).start()
        wait(a_copies(k))
        xk = xv[:, pl.ds(pl.multiple_of(k * kc, 128), kc)]
        acckv[...] += _dot(xk, wkv[k])
        acckr[...] += _dot_nt(xk, wkr[k])
        return carry

    lax.fori_loop(0, KCH, a_step, 0)

    pieces = (ci, 7 - ci)

    def lat_rows(piece):
        return lat.at[pl.ds(pl.multiple_of(piece * half, half), half), :]

    def lat_send(piece, slot, dev):
        ref = lat_rows(piece)
        return pltpu.make_async_remote_copy(src_ref=ref, dst_ref=ref, send_sem=lats.at[slot], recv_sem=latr.at[piece],
                                            device_id={"ctx": dev}, device_id_type=MESH)

    gkv = gkv_ref[...].astype(F32)
    for hf in range(2):
        rows = slice(hf * half, (hf + 1) * half)
        a = acckv[rows, :]
        inv = lax.rsqrt(jnp.mean(a * a, axis=-1, keepdims=True) + NORM_EPS)
        kr = acckr[rows, :]
        kr2 = rope(jnp.concatenate([kr, kr], axis=1), hf * half)
        row0 = pl.multiple_of(pieces[hf] * half, half)
        lat[pl.ds(row0, half), 0:LR] = (a * inv * gkv).astype(BF16)
        lat[pl.ds(row0, half), LR:LR + 128] = kr2.astype(BF16)
        if hf == 0:
            pl.semaphore_wait(bar, 3)
        lat_send(pieces[hf], 2 * hf, xpeer).start()
        lat_send(pieces[hf], 2 * hf + 1, dpeer).start()

    def b_step(n, carry):
        @pl.when(n >= nb_q - RING)
        def _():
            start(c_copies(n - (nb_q - RING)))
        b_copy(n).wait()
        w = arena[pl.ds(pl.multiple_of(n * D, D), D), :]
        accq[:, pl.ds(pl.multiple_of(n * NBLK, NBLK), NBLK)] = _dot(xv[...], w)
        return carry

    lax.fori_loop(0, nb_q, b_step, 0)
    gq = gq_ref[...].astype(F32)
    aq = accq[...]
    invq = lax.rsqrt(jnp.mean(aq * aq, axis=-1, keepdims=True) + NORM_EPS)
    cq[...] = (aq * invq * gq).astype(BF16)

    far = (xpeer, 7 - xpeer)
    near = (dpeer, 7 - dpeer)
    relayed = (3 - ci, 4 + ci)

    def lat_recv(piece):
        lat_send(piece, 0, dpeer).wait_recv()

    def relay(hf):
        lat_recv(far[hf])
        lat_send(far[hf], 4 + hf, dpeer).start()
        lat_recv(near[hf])
        lat_recv(relayed[hf])
        rows = slice(hf * 4 * half, (hf + 1) * 4 * half)
        kp = lat[rows, LR:LR + 128].astype(F32)
        low = lane < 64
        kplo[rows, :] = jnp.where(low, kp, 0.0).astype(BF16)
        kphi[rows, :] = jnp.where(low, 0.0, kp).astype(BF16)

    def heads(chunk, nk, q_index):
        rows = slice(chunk * half, (chunk + 1) * half)
        base = q_index * half

        def body(hp, carry):
            g = hp + chunk * nheads2
            s = lax.rem(g, RING)
            wait(c_copies(g))
            c = cq[rows, :]
            qn = _dot(c, uqb[s]).astype(BF16)
            qp = rope(_dot(c, qrb[s]), chunk * half).astype(BF16)
            lt = lat[0:nk, 0:LR]
            kn = _dot(lt, ukb[s]).astype(BF16)
            vv = _dot(lt, uvb[s]).astype(BF16)

            @pl.when(g + RING < 2 * nheads2)
            def _():
                start(c_copies(g + RING))
            if chunk == 0:
                @pl.when(lax.rem(hp, 2) == 0)
                def _():
                    wo_copy(lax.div(hp, 2)).start()
            vis = (lax.broadcasted_iota(jnp.int32, (half, nk), 1)
                   <= lax.broadcasted_iota(jnp.int32, (half, nk), 0) + base)
            for h in range(2):
                kp = kplo if h == 0 else kphi
                qh = jnp.concatenate([qn[:, h * 128:(h + 1) * 128], qp], axis=1)
                kh = jnp.concatenate([kn[:, h * 128:(h + 1) * 128], kp[0:nk, :]], axis=1)
                sc = jnp.where(vis, _dot_nt(qh, kh), NEG_BIG)
                top = jnp.max(sc, axis=1, keepdims=True)
                p = jnp.exp((sc - top) * score_scale)
                tot = jnp.sum(p, axis=1, keepdims=True)
                acc = _dot(p.astype(BF16), vv[:, h * 128:(h + 1) * 128])
                ov[rows, pl.ds(pl.multiple_of(hp * 256 + h * 128, 128), 128)] = (acc / tot).astype(BF16)
            return carry

        lax.fori_loop(0, nheads2, body, 0)

    def part_send(t):
        return pltpu.make_async_remote_copy(src_ref=sendb.at[t], dst_ref=recvb.at[t], send_sem=ps.at[t], recv_sem=pr.at[t],
                                            device_id={"tp": 1 - tp}, device_id_type=MESH)

    total_wo = 3 * nblk
    ahead = WO_SLOTS - 1

    def wo_block(L):
        wo_copy(L).wait()
        s = lax.rem(L, WO_SLOTS)
        return arena[pl.ds(pl.multiple_of(s * hv, hv), hv), :]

    def wo_next(L):
        @pl.when(L + ahead < total_wo)
        def _():
            wo_copy(L + ahead).start()

    def project_partner(chunk):
        rows = slice(chunk * half, (chunk + 1) * half)

        def body(j, carry):
            t = chunk * nblk + j
            wo_next(t)
            sendb[t] = _dot(ov[rows, :], wo_block(t))
            part_send(t).start()
            return carry

        lax.fori_loop(0, nblk, body, 0)

    relay(0)
    heads(0, 4 * half, ci)
    project_partner(0)
    relay(1)
    heads(1, 8 * half, 7 - ci)
    project_partner(1)

    def own_body(j, carry):
        L = 2 * nblk + j
        wo_next(L)
        r = _dot(ov[...], wo_block(L))
        ownb[j] = r[:half]
        ownb[nblk + j] = r[half:]
        return carry

    lax.fori_loop(0, nblk, own_body, 0)

    def y_block(t, side):
        c = lax.div(t, nblk)
        j = lax.rem(t, nblk)
        return y_hbm.at[pl.ds(pl.multiple_of(c * half, half), half),
                        pl.ds(pl.multiple_of(side * own_cols + j * NBLK, NBLK), NBLK)]

    def result_send(t):
        return pltpu.make_async_remote_copy(src_ref=resb.at[t], dst_ref=y_block(t, tp), send_sem=rs.at[t], recv_sem=rr.at[t],
                                            device_id={"tp": 1 - tp}, device_id_type=MESH)

    def result_store(t):
        return pltpu.make_async_copy(resb.at[t], y_block(t, tp), ys.at[t])

    def ret_body(t, carry):
        part_send(t).wait_recv()
        resb[t] = (recvb[t] + ownb[t]).astype(BF16)
        result_send(t).start()
        result_store(t).start()
        return carry

    lax.fori_loop(0, 2 * nblk, ret_body, 0)

    def drain(t, carry):
        part_send(t).wait_send()
        result_send(t).wait_send()
        result_store(t).wait()
        pltpu.make_async_remote_copy(src_ref=resb.at[t], dst_ref=y_block(t, 1 - tp), send_sem=rs.at[t], recv_sem=rr.at[t],
                                     device_id={"tp": 1 - tp}, device_id_type=MESH).wait_recv()
        return carry

    lax.fori_loop(0, 2 * nblk, drain, 0)
    for slot, piece in ((0, pieces[0]), (1, pieces[0]), (2, pieces[1]), (3, pieces[1]), (4, far[0]), (5, far[1])):
        lat_send(piece, slot, dpeer).wait_send()


def solution(mesh):
    tok_spec = P(('dp', 'ctx'), None)
    pos_spec = P(('dp', 'ctx'))
    full_mat = P(None, None)
    full_vec = P(None)
    col_spec = P(None, 'tp')
    row_spec = P('tp', None)

    def local_step(tok_x, tok_pos, w_dq, g_q, w_uq, w_qr, w_dkv, g_kv, w_kr, w_uk, w_uv, w_o):
        rows, D = tok_x.shape
        half = rows // 2
        QR = w_dq.shape[1]
        LR = w_dkv.shape[1]
        HL = w_qr.shape[1] // w_kr.shape[1]
        scale = (128 + w_kr.shape[1]) ** -0.5
        nblk = D // 2 // NBLK
        kc = D // KCH
        ntok = 8 * half
        dims = (D, QR, LR, HL, half, scale)
        anyspec = pl.BlockSpec(memory_space=pl.ANY)
        vspec = pl.BlockSpec(memory_space=pltpu.VMEM)
        dma = pltpu.SemaphoreType.DMA
        arena_rows = max(QR // NBLK * D, WO_SLOTS * HL * 128)
        return pl.pallas_call(
            functools.partial(layer_kernel, dims),
            out_shape=jax.ShapeDtypeStruct((rows, D), BF16),
            in_specs=[anyspec, vspec, anyspec, vspec, anyspec, anyspec, anyspec, vspec, anyspec, anyspec, anyspec, anyspec],
            out_specs=anyspec,
            scratch_shapes=[
                pltpu.VMEM((rows, D), BF16),
                pltpu.VMEM((KCH, kc, LR), BF16),
                pltpu.VMEM((KCH, 64, kc), BF16),
                pltpu.VMEM((arena_rows, NBLK), BF16),
                pltpu.VMEM((ntok, LR + 128), BF16),
                pltpu.VMEM((ntok, 128), BF16),
                pltpu.VMEM((ntok, 128), BF16),
                pltpu.VMEM((rows, QR), BF16),
                pltpu.VMEM((rows, QR), F32),
                pltpu.VMEM((rows, LR), F32),
                pltpu.VMEM((rows, 64), F32),
                pltpu.VMEM((rows, 128), F32),
                pltpu.VMEM((rows, 128), F32),
                pltpu.VMEM((RING, QR, 256), BF16),
                pltpu.VMEM((RING, QR, 128), BF16),
                pltpu.VMEM((RING, LR, 256), BF16),
                pltpu.VMEM((RING, LR, 256), BF16),
                pltpu.VMEM((rows, HL * 128), BF16),
                pltpu.VMEM((2 * nblk, half, NBLK), F32),
                pltpu.VMEM((2 * nblk, half, NBLK), F32),
                pltpu.VMEM((2 * nblk, half, NBLK), F32),
                pltpu.VMEM((2 * nblk, half, NBLK), BF16),
                dma((KCH,)), dma((KCH,)), dma((KCH,)), dma((QR // NBLK,)), dma((RING, 4)), dma((WO_SLOTS,)),
                dma((6,)), dma((8,)), dma((2 * nblk,)), dma((2 * nblk,)), dma((2 * nblk,)), dma((2 * nblk,)), dma((2 * nblk,)),
            ],
            compiler_params=pltpu.CompilerParams(collective_id=0, has_side_effects=True,
                                                 vmem_limit_bytes=60 * 1024 * 1024),
        )(tok_x, tok_pos.reshape(2, half), w_dq, g_q.reshape(1, QR), w_uq, w_qr, w_dkv, g_kv.reshape(1, LR), w_kr.T,
          w_uk, w_uv, w_o)

    return jax.shard_map(local_step, mesh=mesh,
                         in_specs=(tok_spec, pos_spec, full_mat, full_vec, col_spec, col_spec, full_mat, full_vec, full_mat, col_spec, col_spec, row_spec),
                         out_specs=tok_spec, check_vma=False)
```

```python
import functools

import jax
import jax.numpy as jnp
from jax import lax
from jax.experimental import pallas as pl
from jax.experimental.pallas import tpu as pltpu
from jax.sharding import PartitionSpec as P

ROPE_BASE = 10000.0
NORM_EPS = 1e-6
NEG_BIG = -1e30
MESH = pl.DeviceIdType.MESH
F32 = jnp.float32
BF16 = jnp.bfloat16

KCH = 6
NBLK = 256
RING = 3
WO_SLOTS = 9


def _dot(a, b):
    return jnp.dot(a, b, preferred_element_type=F32)


def _dot_nt(a, b):
    return lax.dot_general(a, b, (((1,), (1,)), ((), ())), preferred_element_type=F32)


def layer_kernel(dims, x_hbm, pos_ref, wdq_hbm, gq_ref, wuq_hbm, wqr_hbm, wdkv_hbm, gkv_ref, wkr_hbm, wuk_hbm, wuv_hbm,
                 wo_hbm, y_hbm,
                 xv, kvs, wkr, upw, arena, lat, kplo, kphi, cq, acckv, acckr, rot,
                 uqb, qrb, qn, qp, os, orx, sendb, recvb, ownb, resb,
                 xsem, kvsem, krsem, bsem, qsem, upsem, wosem, lats, latr, cqs, cqr, rots, rotr, oss, osr, ps, pr, rs, rr, ys):
    D, QR, LR, HL, half, score_scale = dims
    HC = HL // 2
    ngrp = HC // 4
    kc = D // KCH
    nb_q = QR // NBLK
    own_cols = D // 2
    nblk = own_cols // NBLK
    hv = HL * 128
    ntok = 8 * half
    tp = lax.axis_index("tp")
    ci = lax.axis_index("ctx")
    core = lax.rem(ci, 2)
    xpeer = lax.rem(ci + 2, 4)
    dpeer = ci + 1 - 2 * core
    pieces = (ci, 7 - ci)
    mine = tuple(pl.ds(pl.multiple_of(sl * half, half), half) for sl in (core, 1 - core))
    theirs = tuple(pl.ds(pl.multiple_of(sl * half, half), half) for sl in (1 - core, core))
    first_pos = (2 * half * lax.div(ci, 2), half * (6 - 2 * lax.div(ci, 2)))
    half_rows = (slice(0, half), slice(half, 2 * half))

    def x_copy(hf, k):
        col = pl.multiple_of(k * kc, 128)
        rows = pl.ds(hf * half, half)
        return pltpu.make_async_copy(x_hbm.at[rows, pl.ds(col, kc)], xv.at[rows, pl.ds(col, kc)], xsem.at[hf, k])

    def a_copies(k):
        col = pl.multiple_of(k * kc, 128)
        return (pltpu.make_async_copy(wkr_hbm.at[:, pl.ds(col, kc)], wkr.at[:, pl.ds(col, kc)], krsem.at[k]),
                pltpu.make_async_copy(wdkv_hbm.at[pl.ds(col, kc), :], kvs.at[pl.ds(col, kc), :], kvsem.at[k]))

    def b_copy(n):
        return pltpu.make_async_copy(wdq_hbm.at[:, pl.ds(pl.multiple_of(n * NBLK, NBLK), NBLK)],
                                     arena.at[pl.ds(pl.multiple_of(n * D, D), D), :], bsem.at[n])

    def q_copies(g):
        i = lax.rem(g, ngrp) + core * ngrp
        s = lax.rem(g, RING)
        c4 = pl.ds(pl.multiple_of(i * 512, 512), 512)
        c2 = pl.ds(pl.multiple_of(i * 256, 256), 256)
        return (pltpu.make_async_copy(wuq_hbm.at[:, c4], uqb.at[s], qsem.at[s, 0]),
                pltpu.make_async_copy(wqr_hbm.at[:, c2], qrb.at[s], qsem.at[s, 1]))

    def up_copies(i):
        c4 = pl.ds(pl.multiple_of((i + core * ngrp) * 512, 512), 512)
        return (pltpu.make_async_copy(wuk_hbm.at[:, c4], upw.at[i], upsem.at[i, 0]),
                pltpu.make_async_copy(wuv_hbm.at[:, c4], upw.at[ngrp + i], upsem.at[i, 1]))

    def wo_copy(L):
        j = lax.rem(L, nblk)
        side = jnp.where(L < 2 * nblk, 1 - tp, tp)
        s = lax.rem(L, WO_SLOTS)
        col = pl.multiple_of(side * own_cols + j * NBLK, NBLK)
        return pltpu.make_async_copy(wo_hbm.at[:, pl.ds(col, NBLK)],
                                     arena.at[pl.ds(pl.multiple_of(s * hv, hv), hv), :], wosem.at[s])

    def start(cps):
        for c in cps:
            c.start()

    def wait(cps):
        for c in cps:
            c.wait()

    for k in range(KCH):
        x_copy(0, k).start()
        start(a_copies(k))
    for k in range(KCH):
        x_copy(1, k).start()

    bar = pltpu.get_barrier_semaphore()
    for dev in ({"tp": 1 - tp}, {"ctx": xpeer}, {"ctx": dpeer}):
        pl.semaphore_signal(bar, inc=1, device_id=dev, device_id_type=MESH)

    lane = lax.broadcasted_iota(jnp.int32, (1, 128), 1)
    first_half = lax.rem(lane, 64) < 32

    def rotary(hf):
        fidx = lax.rem(lane, 32)
        freq = jnp.zeros((1, 128), F32)
        for j in range(32):
            freq = jnp.where(fidx == j, ROPE_BASE ** (-j * 2.0 / 64), freq)
        eye = (lax.broadcasted_iota(jnp.int32, (half, half), 0) == lax.broadcasted_iota(jnp.int32, (half, half), 1))
        prow = pos_ref[hf:hf + 1, :].astype(F32)
        pcol = jnp.sum(jnp.where(eye, jnp.broadcast_to(prow, (half, half)), 0.0), axis=1, keepdims=True)
        ang = pcol * freq
        rot[hf, mine[hf], 0:128] = jnp.cos(ang)
        sn = jnp.sin(ang)
        rot[hf, mine[hf], 128:256] = jnp.where(first_half, -sn, sn)

    def turn(a, table):
        swapped = jnp.where(first_half, pltpu.roll(a, 96, 1), pltpu.roll(a, 32, 1))
        return a * table[:, 0:128] + swapped * table[:, 128:256]

    def to_core(ref, ssem, rsem):
        return pltpu.make_async_remote_copy(src_ref=ref, dst_ref=ref, send_sem=ssem, recv_sem=rsem,
                                            device_id={"ctx": dpeer}, device_id_type=MESH)

    def rot_send(hf):
        return to_core(rot.at[hf, mine[hf], :], rots.at[hf], rotr.at[hf])

    def rot_recv(hf):
        return to_core(rot.at[hf, theirs[hf], :], rots.at[hf], rotr.at[hf])

    def lat_send(piece, slot, dev):
        ref = lat.at[pl.ds(pl.multiple_of(piece * half, half), half), :]
        return pltpu.make_async_remote_copy(src_ref=ref, dst_ref=ref, send_sem=lats.at[slot], recv_sem=latr.at[piece],
                                            device_id={"ctx": dev}, device_id_type=MESH)

    def lat_finish(hf, a, kr):
        inv = lax.rsqrt(jnp.mean(a * a, axis=-1, keepdims=True) + NORM_EPS)
        kr2 = turn(jnp.concatenate([kr, kr], axis=1), rot[hf, mine[hf], :])
        row0 = pl.multiple_of(pieces[hf] * half, half)
        for c in range(LR // 128):
            cols = slice(c * 128, (c + 1) * 128)
            lat[pl.ds(row0, half), cols] = (a[:, cols] * inv * gkv_ref[c:c + 1, :].astype(F32)).astype(BF16)
        lat[pl.ds(row0, half), LR:LR + 128] = kr2.astype(BF16)

    def lat_share(hf):
        lat_send(pieces[hf], 2 * hf, xpeer).start()
        lat_send(pieces[hf], 2 * hf + 1, dpeer).start()

    far = (xpeer, 7 - xpeer)
    near = (dpeer, 7 - dpeer)
    relayed = (3 - ci, 4 + ci)

    def lat_recv(piece):
        lat_send(piece, 0, dpeer).wait_recv()

    def forward(hf):
        lat_recv(far[hf])
        lat_send(far[hf], 4 + hf, dpeer).start()

    def gathered(hf):
        lat_recv(near[hf])
        lat_recv(relayed[hf])
        rows = slice(hf * 4 * half, (hf + 1) * 4 * half)
        kp = lat[rows, LR:LR + 128].astype(F32)
        low = lane < 64
        kplo[rows, :] = jnp.where(low, kp, 0.0).astype(BF16)
        kphi[rows, :] = jnp.where(low, 0.0, kp).astype(BF16)

    def qlat_finish(hf):
        sq = 0.0
        for n in range(nb_q):
            a = ownb[hf * nb_q + n]
            sq = sq + jnp.sum(a * a, axis=-1, keepdims=True)
        inv = lax.rsqrt(sq * (1.0 / QR) + NORM_EPS)
        for n in range(nb_q):
            a = ownb[hf * nb_q + n] * inv
            for u in range(NBLK // 128):
                c = n * (NBLK // 128) + u
                cq[hf, mine[hf], c * 128:(c + 1) * 128] = (
                    a[:, u * 128:(u + 1) * 128] * gq_ref[c:c + 1, :].astype(F32)).astype(BF16)

    def cq_send(hf):
        return to_core(cq.at[hf, mine[hf], :], cqs.at[hf], cqr.at[hf])

    def cq_recv(hf):
        return to_core(cq.at[hf, theirs[hf], :], cqs.at[hf], cqr.at[hf])

    def queries(chunk):
        def body(i, carry):
            g = i + chunk * ngrp
            s = lax.rem(g, RING)
            wait(q_copies(g))
            c = cq[chunk]
            r = _dot(c, qrb[s])
            qn[:, pl.ds(pl.multiple_of(i * 512, 512), 512)] = _dot(c, uqb[s]).astype(BF16)
            for u in range(2):
                qp[:, pl.ds(pl.multiple_of(i * 256 + u * 128, 128), 128)] = turn(r[:, u * 128:(u + 1) * 128], rot[chunk]).astype(BF16)

            @pl.when(g + RING < 2 * ngrp)
            def _():
                start(q_copies(g + RING))
            return carry

        lax.fori_loop(0, ngrp, body, 0)

    def kv_rows(i, n):
        return pl.ds(pl.multiple_of(i * ntok, ntok), n)

    def keys_values(chunk, nk):
        def body(i, carry):
            if chunk == 0:
                wait(up_copies(i))
            lt = lat[0:nk, 0:LR]
            kvs[kv_rows(i, nk), :] = _dot(lt, upw[i]).astype(BF16)
            kvs[kv_rows(ngrp + i, nk), :] = _dot(lt, upw[ngrp + i]).astype(BF16)
            return carry

        lax.fori_loop(0, ngrp, body, 0)

    c2e = score_scale * 1.4426950408889634

    def o_send(chunk, i):
        cols = pl.ds(pl.multiple_of(i * 512, 512), 512)
        return pltpu.make_async_remote_copy(src_ref=os.at[chunk, theirs[chunk], cols], dst_ref=orx.at[chunk, :, cols],
                                            send_sem=oss.at[chunk, i], recv_sem=osr.at[chunk, i],
                                            device_id={"ctx": dpeer}, device_id_type=MESH)

    def attention(chunk, nk):
        nq = 2 * half

        def body(i, carry):
            if chunk == 0:
                wo_copy(2 * i).start()
                wo_copy(2 * i + 1).start()
            vis = (lax.broadcasted_iota(jnp.int32, (nq, nk), 1)
                   <= lax.broadcasted_iota(jnp.int32, (nq, nk), 0) + first_pos[chunk])

            def scores(h):
                kp = kphi if h % 2 else kplo
                qpe = qp[:, pl.ds(pl.multiple_of(i * 256 + (h // 2) * 128, 128), 128)]
                qh = jnp.concatenate([qn[:, pl.ds(pl.multiple_of(i * 512 + h * 128, 128), 128)], qpe], axis=1)
                kh = jnp.concatenate([kvs[kv_rows(i, nk), h * 128:(h + 1) * 128], kp[0:nk, :]], axis=1)
                return _dot_nt(qh, kh)

            def values(h, sc):
                sc = jnp.where(vis, sc, NEG_BIG)
                top = jnp.max(sc, axis=1, keepdims=True)
                p = jnp.exp2((sc - top) * c2e)
                tot = jnp.sum(p, axis=1, keepdims=True)
                acc = _dot(p.astype(BF16), kvs[kv_rows(ngrp + i, nk), h * 128:(h + 1) * 128])
                os[chunk, :, pl.ds(pl.multiple_of(i * 512 + h * 128, 128), 128)] = (acc / tot).astype(BF16)

            sc = scores(0)
            for h in range(4):
                nxt = scores(h + 1) if h < 3 else None
                values(h, sc)
                sc = nxt
            o_send(chunk, i).start()
            return carry

        lax.fori_loop(0, ngrp, body, 0)

        def arrive(i, carry):
            o_send(chunk, i).wait_recv()
            return carry

        lax.fori_loop(0, ngrp, arrive, 0)

    total_wo = 3 * nblk
    ahead = WO_SLOTS - 1
    hc = HC * 128

    def wo_next(L):
        wo_copy(L).wait()

        @pl.when(L + ahead < total_wo)
        def _():
            wo_copy(L + ahead).start()

    def project(chunk, L):
        base = lax.rem(L, WO_SLOTS) * hv
        w_here = arena[pl.ds(pl.multiple_of(base + core * hc, hc), hc), :]
        w_there = arena[pl.ds(pl.multiple_of(base + (1 - core) * hc, hc), hc), :]
        return _dot(os[chunk, mine[chunk], :], w_here) + _dot(orx[chunk], w_there)

    def part_send(t):
        return pltpu.make_async_remote_copy(src_ref=sendb.at[lax.rem(t, nblk)], dst_ref=recvb.at[t], send_sem=ps.at[t],
                                            recv_sem=pr.at[t],
                                            device_id={"tp": 1 - tp}, device_id_type=MESH)

    def project_partner(chunk):
        def body(j, carry):
            t = chunk * nblk + j
            wo_next(t)
            if chunk == 1:
                part_send(j).wait_send()
            sendb[j] = project(chunk, t)
            part_send(t).start()
            return carry

        lax.fori_loop(0, nblk, body, 0)

    def y_block(chunk, j, side):
        return y_hbm.at[pl.ds(chunk * half, half), pl.ds(pl.multiple_of(side * own_cols + j * NBLK, NBLK), NBLK)]

    def result_send(chunk, j, side):
        t = chunk * nblk + j
        return pltpu.make_async_remote_copy(src_ref=resb.at[t], dst_ref=y_block(chunk, j, side), send_sem=rs.at[t],
                                            recv_sem=rr.at[t], device_id={"tp": 1 - tp}, device_id_type=MESH)

    def result_store(chunk, j):
        t = chunk * nblk + j
        return pltpu.make_async_copy(resb.at[t], y_block(chunk, j, tp), ys.at[t])

    def give_back(chunk, j, own):
        t = chunk * nblk + j
        part_send(t).wait_recv()
        resb[t] = (recvb[t] + own).astype(BF16)
        result_send(chunk, j, tp).start()
        result_store(chunk, j).start()

    acckv[...] = jnp.zeros_like(acckv)
    acckr[...] = jnp.zeros_like(acckr)
    with jax.named_scope('rot0'):
        rotary(0)

    def a_step(k, carry):
        x_copy(0, k).wait()
        wait(a_copies(k))

        @pl.when(k % 2 == 1)
        def _():
            b_copy(lax.div(k, 2)).start()
        cols = pl.ds(pl.multiple_of(k * kc, 128), kc)
        xk = xv[half_rows[0], cols]
        acckv[...] += _dot(xk, kvs[cols, :])
        acckr[...] += _dot_nt(xk, wkr[:, cols])
        return carry

    with jax.named_scope('lat0'):
        lax.fori_loop(0, KCH, a_step, 0)
        lat_finish(0, acckv[...], acckr[...])
        pl.semaphore_wait(bar, 3)
        lat_share(0)
        rot_send(0).start()
    with jax.named_scope('rot1'):
        rotary(1)
        rot_send(1).start()
        for k in range(KCH):
            x_copy(1, k).wait()

    def b_step(n, carry):
        b_copy(n).wait()

        @pl.when(n < nb_q - 3)
        def _():
            b_copy(n + 3).start()

        @pl.when(n < ngrp)
        def _():
            start(up_copies(n))

        @pl.when(n >= nb_q - RING)
        def _():
            start(q_copies(n - (nb_q - RING)))
        w = arena[pl.ds(pl.multiple_of(n * D, D), D), :]
        r = _dot(xv[...], w)
        ownb[n] = r[:half]
        ownb[nb_q + n] = r[half:]
        return carry

    with jax.named_scope('qlat'):
        lax.fori_loop(0, nb_q, b_step, 0)
    with jax.named_scope('qfin'):
        forward(0)
        qlat_finish(0)
        cq_send(0).start()
    with jax.named_scope('lat1'):
        xs = xv[half_rows[1], :]
        lat_finish(1, _dot(xs, kvs[0:D, :]), _dot_nt(xs, wkr[...]))
        lat_share(1)
        qlat_finish(1)
        cq_send(1).start()
    with jax.named_scope('gather0'):
        gathered(0)
    with jax.named_scope('kv0'):
        keys_values(0, 4 * half)
    with jax.named_scope('q0'):
        cq_recv(0).wait_recv()
        rot_recv(0).wait_recv()
        queries(0)
    with jax.named_scope('att0'):
        attention(0, 4 * half)
    with jax.named_scope('part0'):
        project_partner(0)
    with jax.named_scope('gather1'):
        forward(1)
        gathered(1)
    with jax.named_scope('kv1'):
        keys_values(1, 8 * half)
    with jax.named_scope('q1'):
        cq_recv(1).wait_recv()
        rot_recv(1).wait_recv()
        queries(1)
    with jax.named_scope('att1'):
        attention(1, 8 * half)
    with jax.named_scope('part1'):
        project_partner(1)

    def own_body(j, carry):
        L = 2 * nblk + j
        wo_next(L)
        ownb[j] = project(1, L)
        give_back(0, j, project(0, L))
        return carry

    with jax.named_scope('own'):
        lax.fori_loop(0, nblk, own_body, 0)

    def ret_body(j, carry):
        give_back(1, j, ownb[j])
        return carry

    with jax.named_scope('ret'):
        lax.fori_loop(0, nblk, ret_body, 0)

    def drain(j, carry):
        part_send(nblk + j).wait_send()
        for chunk in range(2):
            result_send(chunk, j, tp).wait_send()
            result_store(chunk, j).wait()
            result_send(chunk, j, 1 - tp).wait_recv()
        return carry

    with jax.named_scope('drain'):
        lax.fori_loop(0, nblk, drain, 0)
    for slot, piece in ((0, pieces[0]), (1, pieces[0]), (2, pieces[1]), (3, pieces[1]), (4, far[0]), (5, far[1])):
        lat_send(piece, slot, dpeer).wait_send()
    for hf in range(2):
        rot_send(hf).wait_send()
        cq_send(hf).wait_send()
        for i in range(ngrp):
            o_send(hf, i).wait_send()


def solution(mesh):
    tok_spec = P(('dp', 'ctx'), None)
    pos_spec = P(('dp', 'ctx'))
    full_mat = P(None, None)
    full_vec = P(None)
    col_spec = P(None, 'tp')
    row_spec = P('tp', None)

    def local_step(tok_x, tok_pos, w_dq, g_q, w_uq, w_qr, w_dkv, g_kv, w_kr, w_uk, w_uv, w_o):
        rows, D = tok_x.shape
        half = rows // 2
        QR = w_dq.shape[1]
        LR = w_dkv.shape[1]
        HL = w_qr.shape[1] // w_kr.shape[1]
        scale = (128 + w_kr.shape[1]) ** -0.5
        nblk = D // 2 // NBLK
        ngrp = HL // 8
        ntok = 8 * half
        dims = (D, QR, LR, HL, half, scale)
        anyspec = pl.BlockSpec(memory_space=pl.ANY)
        vspec = pl.BlockSpec(memory_space=pltpu.VMEM)
        dma = pltpu.SemaphoreType.DMA
        arena_rows = max(QR // NBLK * D, WO_SLOTS * HL * 128)
        return pl.pallas_call(
            functools.partial(layer_kernel, dims),
            out_shape=jax.ShapeDtypeStruct((rows, D), BF16),
            in_specs=[anyspec, vspec, anyspec, vspec, anyspec, anyspec, anyspec, vspec, anyspec, anyspec, anyspec, anyspec],
            out_specs=anyspec,
            scratch_shapes=[
                pltpu.VMEM((rows, D), BF16),
                pltpu.VMEM((max(D, 2 * ngrp * ntok), LR), BF16),
                pltpu.VMEM((64, D), BF16),
                pltpu.VMEM((2 * ngrp, LR, 512), BF16),
                pltpu.VMEM((arena_rows, NBLK), BF16),
                pltpu.VMEM((ntok, LR + 128), BF16),
                pltpu.VMEM((ntok, 128), BF16),
                pltpu.VMEM((ntok, 128), BF16),
                pltpu.VMEM((2, rows, QR), BF16),
                pltpu.VMEM((half, LR), F32),
                pltpu.VMEM((half, 64), F32),
                pltpu.VMEM((2, rows, 256), F32),
                pltpu.VMEM((RING, QR, 512), BF16),
                pltpu.VMEM((RING, QR, 256), BF16),
                pltpu.VMEM((rows, HL * 64), BF16),
                pltpu.VMEM((rows, HL * 32), BF16),
                pltpu.VMEM((2, rows, HL * 64), BF16),
                pltpu.VMEM((2, half, HL * 64), BF16),
                pltpu.VMEM((nblk, half, NBLK), F32),
                pltpu.VMEM((2 * nblk, half, NBLK), F32),
                pltpu.VMEM((max(nblk, 2 * QR // NBLK), half, NBLK), F32),
                pltpu.VMEM((2 * nblk, half, NBLK), BF16),
                dma((2, KCH)), dma((KCH,)), dma((KCH,)), dma((QR // NBLK,)), dma((RING, 2)), dma((ngrp, 2)), dma((WO_SLOTS,)),
                dma((6,)), dma((8,)), dma((2,)), dma((2,)), dma((2,)), dma((2,)), dma((2, ngrp)), dma((2, ngrp)),
                dma((2 * nblk,)), dma((2 * nblk,)), dma((2 * nblk,)), dma((2 * nblk,)), dma((2 * nblk,)),
            ],
            compiler_params=pltpu.CompilerParams(collective_id=0, has_side_effects=True,
                                                 vmem_limit_bytes=65536 * 1000),
        )(tok_x, tok_pos.reshape(2, half), w_dq, g_q.reshape(QR // 128, 128), w_uq, w_qr, w_dkv, g_kv.reshape(LR // 128, 128), w_kr.T,
          w_uk, w_uv, w_o)

    return jax.shard_map(local_step, mesh=mesh,
                         in_specs=(tok_spec, pos_spec, full_mat, full_vec, col_spec, col_spec, full_mat, full_vec, full_mat, col_spec, col_spec, row_spec),
                         out_specs=tok_spec, check_vma=False)
```

```python
import functools

import jax
import jax.numpy as jnp
from jax import lax
from jax.experimental import pallas as pl
from jax.experimental.pallas import tpu as pltpu
from jax.sharding import PartitionSpec as P

ROPE_BASE = 10000.0
NORM_EPS = 1e-6
NEG_BIG = -1e30
MESH = pl.DeviceIdType.MESH
F32 = jnp.float32
BF16 = jnp.bfloat16

KCH = 6
NBLK = 256
RING = 3
DQ_SLOTS = 4
GROUP = 4
WO_SLOTS = 6


def _dot(a, b):
    return jnp.dot(a, b, preferred_element_type=F32)


def _dot_nt(a, b):
    return lax.dot_general(a, b, (((1,), (1,)), ((), ())), preferred_element_type=F32)


def layer_kernel(dims, x_hbm, pos_ref, wdq_hbm, gq_ref, wuq_hbm, wqr_hbm, wdkv_hbm, gkv_ref, wkr_hbm, wuk_hbm, wuv_hbm,
                 wo_hbm, y_ref,
                 xv, kvs, wkr, upw, arena, lat, kplo, kphi, cq, acckv, acckr, rot,
                 uqb, qrb, qn, qp, os, orx, sendb, recvb, ownb,
                 xsem, x2sem, kvsem, krsem, bsem, qsem, upsem, wosem, lats, latr, cqs, cqr, rots, rotr, oss, osr, ps, pr, rs, rr):
    D, QR, LR, HL, half, score_scale = dims
    HC = HL // 2
    ngrp = HC // 4
    kc = D // KCH
    nb_q = QR // NBLK
    own_cols = D // 2
    nblk = own_cols // NBLK
    hv = HL * 128
    ntok = 8 * half
    tp = lax.axis_index("tp")
    ci = lax.axis_index("ctx")
    core = lax.rem(ci, 2)
    xpeer = lax.rem(ci + 2, 4)
    dpeer = ci + 1 - 2 * core
    pieces = (ci, 7 - ci)
    mine = tuple(pl.ds(pl.multiple_of(sl * half, half), half) for sl in (core, 1 - core))
    theirs = tuple(pl.ds(pl.multiple_of(sl * half, half), half) for sl in (1 - core, core))
    first_pos = (2 * half * lax.div(ci, 2), half * (6 - 2 * lax.div(ci, 2)))
    half_rows = (slice(0, half), slice(half, 2 * half))

    def x_copy(k):
        rows, cols = pl.ds(0, half), pl.ds(pl.multiple_of(k * kc, 128), kc)
        return pltpu.make_async_copy(x_hbm.at[rows, cols], xv.at[rows, cols], xsem.at[k])

    def x2_copy():
        rows = pl.ds(half, half)
        return pltpu.make_async_copy(x_hbm.at[rows, :], xv.at[rows, :], x2sem.at[0])

    def a_copies(k):
        col = pl.multiple_of(k * kc, 128)
        return (pltpu.make_async_copy(wkr_hbm.at[:, pl.ds(col, kc)], wkr.at[:, pl.ds(col, kc)], krsem.at[k]),
                pltpu.make_async_copy(wdkv_hbm.at[pl.ds(col, kc), :], kvs.at[pl.ds(col, kc), :], kvsem.at[k]))

    def b_copy(n):
        s = lax.rem(n, DQ_SLOTS)
        return pltpu.make_async_copy(wdq_hbm.at[:, pl.ds(pl.multiple_of(n * NBLK, NBLK), NBLK)],
                                     arena.at[pl.ds(pl.multiple_of(s * D, D), D), :], bsem.at[s])

    def q_copies(g):
        i = lax.rem(g, ngrp) + core * ngrp
        s = lax.rem(g, RING)
        c4 = pl.ds(pl.multiple_of(i * 512, 512), 512)
        c2 = pl.ds(pl.multiple_of(i * 256, 256), 256)
        return (pltpu.make_async_copy(wuq_hbm.at[:, c4], uqb.at[s], qsem.at[s, 0]),
                pltpu.make_async_copy(wqr_hbm.at[:, c2], qrb.at[s], qsem.at[s, 1]))

    def up_copies(i):
        c4 = pl.ds(pl.multiple_of((i + core * ngrp) * 512, 512), 512)
        return (pltpu.make_async_copy(wuk_hbm.at[:, c4], upw.at[i], upsem.at[i, 0]),
                pltpu.make_async_copy(wuv_hbm.at[:, c4], upw.at[ngrp + i], upsem.at[i, 1]))

    def wo_copy(L):
        j = lax.rem(L, nblk)
        side = jnp.where(L < 2 * nblk, 1 - tp, tp)
        s = lax.rem(L, WO_SLOTS)
        col = pl.multiple_of(side * own_cols + j * NBLK, NBLK)
        return pltpu.make_async_copy(wo_hbm.at[:, pl.ds(col, NBLK)],
                                     arena.at[pl.ds(pl.multiple_of(s * hv, hv), hv), :], wosem.at[s])

    def start(cps):
        for c in cps:
            c.start()

    def wait(cps):
        for c in cps:
            c.wait()

    for k in range(KCH):
        x_copy(k).start()
        start(a_copies(k))
    x2_copy().start()

    bar = pltpu.get_barrier_semaphore()
    for dev in ({"tp": 1 - tp}, {"ctx": xpeer}, {"ctx": dpeer}):
        pl.semaphore_signal(bar, inc=1, device_id=dev, device_id_type=MESH)

    lane = lax.broadcasted_iota(jnp.int32, (1, 128), 1)
    first_half = lax.rem(lane, 64) < 32

    def rotary(hf):
        fidx = lax.rem(lane, 32)
        freq = jnp.zeros((1, 128), F32)
        for j in range(32):
            freq = jnp.where(fidx == j, ROPE_BASE ** (-j * 2.0 / 64), freq)
        eye = (lax.broadcasted_iota(jnp.int32, (half, half), 0) == lax.broadcasted_iota(jnp.int32, (half, half), 1))
        prow = pos_ref[hf:hf + 1, :].astype(F32)
        pcol = jnp.sum(jnp.where(eye, jnp.broadcast_to(prow, (half, half)), 0.0), axis=1, keepdims=True)
        ang = pcol * freq
        rot[hf, mine[hf], 0:128] = jnp.cos(ang)
        sn = jnp.sin(ang)
        rot[hf, mine[hf], 128:256] = jnp.where(first_half, -sn, sn)

    def turn(a, table):
        swapped = jnp.where(first_half, pltpu.roll(a, 96, 1), pltpu.roll(a, 32, 1))
        return a * table[:, 0:128] + swapped * table[:, 128:256]

    def to_core(ref, ssem, rsem):
        return pltpu.make_async_remote_copy(src_ref=ref, dst_ref=ref, send_sem=ssem, recv_sem=rsem,
                                            device_id={"ctx": dpeer}, device_id_type=MESH)

    def rot_send(hf):
        return to_core(rot.at[hf, mine[hf], :], rots.at[hf], rotr.at[hf])

    def rot_recv(hf):
        return to_core(rot.at[hf, theirs[hf], :], rots.at[hf], rotr.at[hf])

    def lat_send(piece, slot, dev):
        ref = lat.at[pl.ds(pl.multiple_of(piece * half, half), half), :]
        return pltpu.make_async_remote_copy(src_ref=ref, dst_ref=ref, send_sem=lats.at[slot], recv_sem=latr.at[piece],
                                            device_id={"ctx": dev}, device_id_type=MESH)

    def lat_finish(hf, a, kr):
        inv = lax.rsqrt(jnp.mean(a * a, axis=-1, keepdims=True) + NORM_EPS)
        kr2 = turn(jnp.concatenate([kr, kr], axis=1), rot[hf, mine[hf], :])
        row0 = pl.multiple_of(pieces[hf] * half, half)
        for c in range(LR // 128):
            cols = slice(c * 128, (c + 1) * 128)
            lat[pl.ds(row0, half), cols] = (a[:, cols] * inv * gkv_ref[c:c + 1, :].astype(F32)).astype(BF16)
        lat[pl.ds(row0, half), LR:LR + 128] = kr2.astype(BF16)

    def lat_share(hf):
        lat_send(pieces[hf], 2 * hf, xpeer).start()
        lat_send(pieces[hf], 2 * hf + 1, dpeer).start()

    far = (xpeer, 7 - xpeer)
    near = (dpeer, 7 - dpeer)
    relayed = (3 - ci, 4 + ci)

    def lat_recv(piece):
        lat_send(piece, 0, dpeer).wait_recv()

    def forward(hf):
        lat_recv(far[hf])
        lat_send(far[hf], 4 + hf, dpeer).start()

    def gathered(hf):
        lat_recv(near[hf])
        lat_recv(relayed[hf])
        rows = slice(hf * 4 * half, (hf + 1) * 4 * half)
        kp = lat[rows, LR:LR + 128].astype(F32)
        low = lane < 64
        kplo[rows, :] = jnp.where(low, kp, 0.0).astype(BF16)
        kphi[rows, :] = jnp.where(low, 0.0, kp).astype(BF16)

    def qlat_finish(hf):
        sq = 0.0
        for n in range(nb_q):
            a = ownb[hf * nb_q + n]
            sq = sq + jnp.sum(a * a, axis=-1, keepdims=True)
        inv = lax.rsqrt(sq * (1.0 / QR) + NORM_EPS)
        for n in range(nb_q):
            a = ownb[hf * nb_q + n] * inv
            for u in range(NBLK // 128):
                c = n * (NBLK // 128) + u
                cq[hf, mine[hf], c * 128:(c + 1) * 128] = (
                    a[:, u * 128:(u + 1) * 128] * gq_ref[c:c + 1, :].astype(F32)).astype(BF16)

    def cq_send(hf):
        return to_core(cq.at[hf, mine[hf], :], cqs.at[hf], cqr.at[hf])

    def cq_recv(hf):
        return to_core(cq.at[hf, theirs[hf], :], cqs.at[hf], cqr.at[hf])

    def queries(chunk):
        def body(i, carry):
            g = i + chunk * ngrp
            s = lax.rem(g, RING)
            wait(q_copies(g))
            c = cq[chunk]
            r = _dot(c, qrb[s])
            qn[:, pl.ds(pl.multiple_of(i * 512, 512), 512)] = _dot(c, uqb[s]).astype(BF16)
            for u in range(2):
                qp[:, pl.ds(pl.multiple_of(i * 256 + u * 128, 128), 128)] = turn(r[:, u * 128:(u + 1) * 128], rot[chunk]).astype(BF16)

            @pl.when(g + RING < 2 * ngrp)
            def _():
                start(q_copies(g + RING))
            return carry

        lax.fori_loop(0, ngrp, body, 0)

    def kv_rows(i, n):
        return pl.ds(pl.multiple_of(i * ntok, ntok), n)

    def keys_values(chunk, nk):
        def body(i, carry):
            if chunk == 0:
                wait(up_copies(i))
            lt = lat[0:nk, 0:LR]
            kvs[kv_rows(i, nk), :] = _dot(lt, upw[i]).astype(BF16)
            kvs[kv_rows(ngrp + i, nk), :] = _dot(lt, upw[ngrp + i]).astype(BF16)
            return carry

        lax.fori_loop(0, ngrp, body, 0)

    c2e = score_scale * 1.4426950408889634

    def o_send(chunk, i):
        cols = pl.ds(pl.multiple_of(i * 512, 512), 512)
        return pltpu.make_async_remote_copy(src_ref=os.at[chunk, theirs[chunk], cols], dst_ref=orx.at[chunk, :, cols],
                                            send_sem=oss.at[chunk], recv_sem=osr.at[chunk],
                                            device_id={"ctx": dpeer}, device_id_type=MESH)

    def attention(chunk, nk):
        nq = 2 * half

        def body(i, carry):
            if chunk == 0:
                wo_copy(i).start()

                @pl.when(i == ngrp - 1)
                def _():
                    for extra in range(ngrp, WO_SLOTS - 1):
                        wo_copy(extra).start()
            vis = (lax.broadcasted_iota(jnp.int32, (nq, nk), 1)
                   <= lax.broadcasted_iota(jnp.int32, (nq, nk), 0) + first_pos[chunk])

            def scores(h):
                kp = kphi if h % 2 else kplo
                qpe = qp[:, pl.ds(pl.multiple_of(i * 256 + (h // 2) * 128, 128), 128)]
                qh = jnp.concatenate([qn[:, pl.ds(pl.multiple_of(i * 512 + h * 128, 128), 128)], qpe], axis=1)
                kh = jnp.concatenate([kvs[kv_rows(i, nk), h * 128:(h + 1) * 128], kp[0:nk, :]], axis=1)
                return _dot_nt(qh, kh)

            def values(h, sc):
                sc = jnp.where(vis, sc, NEG_BIG)
                top = jnp.max(sc, axis=1, keepdims=True)
                p = jnp.exp2((sc - top) * c2e)
                tot = jnp.sum(p, axis=1, keepdims=True)
                acc = _dot(p.astype(BF16), kvs[kv_rows(ngrp + i, nk), h * 128:(h + 1) * 128])
                os[chunk, :, pl.ds(pl.multiple_of(i * 512 + h * 128, 128), 128)] = (acc / tot).astype(BF16)

            sc = scores(0)
            for h in range(4):
                nxt = scores(h + 1) if h < 3 else None
                values(h, sc)
                sc = nxt
            o_send(chunk, i).start()
            return carry

        lax.fori_loop(0, ngrp, body, 0)

    def o_all(chunk):
        return pltpu.make_async_remote_copy(src_ref=os.at[chunk, theirs[chunk], :], dst_ref=orx.at[chunk],
                                            send_sem=oss.at[chunk], recv_sem=osr.at[chunk],
                                            device_id={"ctx": dpeer}, device_id_type=MESH)

    total_wo = 3 * nblk
    ahead = WO_SLOTS - 1
    hc = HC * 128

    def wo_next(L):
        wo_copy(L).wait()
        wo_refill(L)

    def wo_refill(L):
        @pl.when(L + ahead < total_wo)
        def _():
            wo_copy(L + ahead).start()

    def project_here(chunk, L):
        w = arena[pl.ds(pl.multiple_of(lax.rem(L, WO_SLOTS) * hv + core * hc, hc), hc), :]
        return _dot(os[chunk, mine[chunk], :], w)

    def project_there(chunk, L):
        w = arena[pl.ds(pl.multiple_of(lax.rem(L, WO_SLOTS) * hv + (1 - core) * hc, hc), hc), :]
        return _dot(orx[chunk], w)

    def part_copy(chunk, q, src, dst):
        return pltpu.make_async_remote_copy(src_ref=src, dst_ref=dst, send_sem=ps.at[chunk, q], recv_sem=pr.at[chunk, q],
                                            device_id={"tp": 1 - tp}, device_id_type=MESH)

    def part_send(chunk, j):
        return part_copy(chunk, lax.div(j, GROUP), sendb.at[j], recvb.at[chunk * nblk + j])

    def part_group(chunk, q):
        return part_copy(chunk, q, sendb.at[pl.ds(q * GROUP, GROUP)], recvb.at[pl.ds(chunk * nblk + q * GROUP, GROUP)])

    def project_partner(chunk):
        early = 2
        base = chunk * nblk

        def send_slot(j):
            if chunk == 1:
                @pl.when(lax.rem(j, GROUP) == 0)
                def _():
                    part_group(0, lax.div(j, GROUP)).wait_send()

        for j in range(early):
            wo_copy(base + j).wait()
            if j == 0:
                wo_refill(base)
            send_slot(j)
            sendb[j] = project_here(chunk, base + j)
        o_all(chunk).wait_recv()
        for j in range(early):
            sendb[j] += project_there(chunk, base + j)
            part_send(chunk, j).start()
            if j + 1 < early:
                wo_refill(base + j + 1)

        def body(j, carry):
            wo_next(base + j)
            send_slot(j)
            sendb[j] = project_here(chunk, base + j) + project_there(chunk, base + j)
            part_send(chunk, j).start()
            return carry

        lax.fori_loop(early, nblk, body, 0)

    def y_cols(side, j, n):
        return pl.ds(pl.multiple_of(side * own_cols + j * NBLK, NBLK), n)

    def result_copy(ref):
        return pltpu.make_async_remote_copy(src_ref=ref, dst_ref=ref, send_sem=rs.at[0], recv_sem=rr.at[0],
                                            device_id={"tp": 1 - tp}, device_id_type=MESH)

    def give_back(chunk, j, own):
        @pl.when(lax.rem(j, GROUP) == 0)
        def _():
            part_group(chunk, lax.div(j, GROUP)).wait_recv()
        cols = y_cols(tp, j, NBLK)
        y_ref[half_rows[chunk], cols] = (recvb[chunk * nblk + j] + own).astype(BF16)
        result_copy(y_ref.at[half_rows[chunk], cols]).start()

    acckv[...] = jnp.zeros_like(acckv)
    acckr[...] = jnp.zeros_like(acckr)
    with jax.named_scope('rot0'):
        rotary(0)

    def a_step(k, carry):
        x_copy(k).wait()
        wait(a_copies(k))

        @pl.when(k % 2 == 1)
        def _():
            b_copy(lax.div(k, 2)).start()
        cols = pl.ds(pl.multiple_of(k * kc, 128), kc)
        xk = xv[half_rows[0], cols]
        acckv[...] += _dot(xk, kvs[cols, :])
        acckr[...] += _dot_nt(xk, wkr[:, cols])
        return carry

    with jax.named_scope('lat0'):
        lax.fori_loop(0, KCH, a_step, 0)
        lat_finish(0, acckv[...], acckr[...])
        pl.semaphore_wait(bar, 3)
        lat_share(0)
        rot_send(0).start()
    with jax.named_scope('rot1'):
        rotary(1)
        rot_send(1).start()
        x2_copy().wait()

    def b_step(n, carry):
        b_copy(n).wait()

        @pl.when(n < nb_q - 3)
        def _():
            b_copy(n + 3).start()

        @pl.when(n < ngrp)
        def _():
            start(up_copies(n))

        @pl.when(n >= nb_q - RING)
        def _():
            start(q_copies(n - (nb_q - RING)))
        w = arena[pl.ds(pl.multiple_of(lax.rem(n, DQ_SLOTS) * D, D), D), :]
        r = _dot(xv[...], w)
        ownb[n] = r[:half]
        ownb[nb_q + n] = r[half:]
        return carry

    with jax.named_scope('qlat'):
        lax.fori_loop(0, nb_q, b_step, 0)
    with jax.named_scope('qfin'):
        forward(0)
        qlat_finish(0)
        cq_send(0).start()
    with jax.named_scope('lat1'):
        xs = xv[half_rows[1], :]
        lat_finish(1, _dot(xs, kvs[0:D, :]), _dot_nt(xs, wkr[...]))
        lat_share(1)
        qlat_finish(1)
        cq_send(1).start()
    with jax.named_scope('gather0'):
        gathered(0)
    with jax.named_scope('kv0'):
        keys_values(0, 4 * half)
    with jax.named_scope('q0'):
        cq_recv(0).wait_recv()
        rot_recv(0).wait_recv()
        queries(0)
    with jax.named_scope('att0'):
        attention(0, 4 * half)
    with jax.named_scope('part0'):
        project_partner(0)
    with jax.named_scope('gather1'):
        forward(1)
        gathered(1)
    with jax.named_scope('kv1'):
        keys_values(1, 8 * half)
    with jax.named_scope('q1'):
        cq_recv(1).wait_recv()
        rot_recv(1).wait_recv()
        queries(1)
    with jax.named_scope('att1'):
        attention(1, 8 * half)
    with jax.named_scope('part1'):
        project_partner(1)

    def own_body(j, carry):
        L = 2 * nblk + j
        wo_next(L)
        ownb[j] = project_here(1, L) + project_there(1, L)
        give_back(0, j, project_here(0, L) + project_there(0, L))
        return carry

    with jax.named_scope('own'):
        lax.fori_loop(0, nblk, own_body, 0)

    def ret_body(j, carry):
        give_back(1, j, ownb[j])
        return carry

    with jax.named_scope('ret'):
        lax.fori_loop(0, nblk, ret_body, 0)

    with jax.named_scope('drain'):
        for q in range(nblk // GROUP):
            part_group(1, q).wait_send()
        result_copy(y_ref.at[:, y_cols(tp, 0, own_cols)]).wait_send()
        result_copy(y_ref.at[:, y_cols(1 - tp, 0, own_cols)]).wait_recv()
    for slot, piece in ((0, pieces[0]), (1, pieces[0]), (2, pieces[1]), (3, pieces[1]), (4, far[0]), (5, far[1])):
        lat_send(piece, slot, dpeer).wait_send()
    for hf in range(2):
        rot_send(hf).wait_send()
        cq_send(hf).wait_send()
        o_all(hf).wait_send()


def solution(mesh):
    tok_spec = P(('dp', 'ctx'), None)
    pos_spec = P(('dp', 'ctx'))
    full_mat = P(None, None)
    full_vec = P(None)
    col_spec = P(None, 'tp')
    row_spec = P('tp', None)

    def local_step(tok_x, tok_pos, w_dq, g_q, w_uq, w_qr, w_dkv, g_kv, w_kr, w_uk, w_uv, w_o):
        rows, D = tok_x.shape
        half = rows // 2
        QR = w_dq.shape[1]
        LR = w_dkv.shape[1]
        HL = w_qr.shape[1] // w_kr.shape[1]
        scale = (128 + w_kr.shape[1]) ** -0.5
        nblk = D // 2 // NBLK
        ngrp = HL // 8
        ntok = 8 * half
        dims = (D, QR, LR, HL, half, scale)
        anyspec = pl.BlockSpec(memory_space=pl.ANY)
        vspec = pl.BlockSpec(memory_space=pltpu.VMEM)
        dma = pltpu.SemaphoreType.DMA
        arena_rows = max(DQ_SLOTS * D, WO_SLOTS * HL * 128)
        return pl.pallas_call(
            functools.partial(layer_kernel, dims),
            out_shape=pltpu.VMEM((rows, D), BF16),
            in_specs=[anyspec, vspec, anyspec, vspec, anyspec, anyspec, anyspec, vspec, anyspec, anyspec, anyspec, anyspec],
            out_specs=vspec,
            scratch_shapes=[
                pltpu.VMEM((rows, D), BF16),
                pltpu.VMEM((max(D, 2 * ngrp * ntok), LR), BF16),
                pltpu.VMEM((64, D), BF16),
                pltpu.VMEM((2 * ngrp, LR, 512), BF16),
                pltpu.VMEM((arena_rows, NBLK), BF16),
                pltpu.VMEM((ntok, LR + 128), BF16),
                pltpu.VMEM((ntok, 128), BF16),
                pltpu.VMEM((ntok, 128), BF16),
                pltpu.VMEM((2, rows, QR), BF16),
                pltpu.VMEM((half, LR), F32),
                pltpu.VMEM((half, 64), F32),
                pltpu.VMEM((2, rows, 256), F32),
                pltpu.VMEM((RING, QR, 512), BF16),
                pltpu.VMEM((RING, QR, 256), BF16),
                pltpu.VMEM((rows, HL * 64), BF16),
                pltpu.VMEM((rows, HL * 32), BF16),
                pltpu.VMEM((2, rows, HL * 64), BF16),
                pltpu.VMEM((2, half, HL * 64), BF16),
                pltpu.VMEM((nblk, half, NBLK), F32),
                pltpu.VMEM((2 * nblk, half, NBLK), F32),
                pltpu.VMEM((max(nblk, 2 * QR // NBLK), half, NBLK), F32),
                dma((KCH,)), dma((1,)), dma((KCH,)), dma((KCH,)), dma((DQ_SLOTS,)), dma((RING, 2)), dma((ngrp, 2)), dma((WO_SLOTS,)),
                dma((6,)), dma((8,)), dma((2,)), dma((2,)), dma((2,)), dma((2,)), dma((2,)), dma((2,)),
                dma((2, nblk // GROUP)), dma((2, nblk // GROUP)), dma((1,)), dma((1,)),
            ],
            compiler_params=pltpu.CompilerParams(collective_id=0, has_side_effects=True,
                                                 vmem_limit_bytes=60500 * 1000),
        )(tok_x, tok_pos.reshape(2, half), w_dq, g_q.reshape(QR // 128, 128), w_uq, w_qr, w_dkv, g_kv.reshape(LR // 128, 128), w_kr.T,
          w_uk, w_uv, w_o)

    return jax.shard_map(local_step, mesh=mesh,
                         in_specs=(tok_spec, pos_spec, full_mat, full_vec, col_spec, col_spec, full_mat, full_vec, full_mat, col_spec, col_spec, row_spec),
                         out_specs=tok_spec, check_vma=False)
```

```python
import functools

import jax
import jax.numpy as jnp
from jax import lax
from jax.experimental import pallas as pl
from jax.experimental.pallas import tpu as pltpu
from jax.sharding import PartitionSpec as P

ROPE_BASE = 10000.0
NORM_EPS = 1e-6
NEG_BIG = -1e30
MESH = pl.DeviceIdType.MESH
F32 = jnp.float32
BF16 = jnp.bfloat16

KCH = 6
NBLK = 256
RING = 3
DQ_SLOTS = 4
GROUP = 4
WO_SLOTS = 6


def _dot(a, b):
    return jnp.dot(a, b, preferred_element_type=F32)


def _dot_nt(a, b):
    return lax.dot_general(a, b, (((1,), (1,)), ((), ())), preferred_element_type=F32)


def layer_kernel(dims, x_hbm, pos_ref, wdq_hbm, gq_ref, wuq_hbm, wqr_hbm, wdkv_hbm, gkv_ref, wkr_hbm, wuk_hbm, wuv_hbm,
                 wo_hbm, y_ref,
                 xc, x2, kvs, wkr, upw, arena, lat, kplo, kphi, cq, acckv, acckr, rot,
                 uqb, qrb, qn, qp, os, orx, sendb, recvb, ownb,
                 xsem, x2sem, xps, xpr, kvsem, krsem, bsem, qsem, upsem, wosem, lats, latr, cqs, cqr, hs, hr, rots, rotr, oss, osr, ps, pr, rs, rr):
    D, QR, LR, HL, half, score_scale = dims
    HC = HL // 2
    ngrp = HC // 4
    kc = D // KCH
    nb_q = QR // NBLK
    own_cols = D // 2
    nblk = own_cols // NBLK
    hv = HL * 128
    ntok = 8 * half
    tp = lax.axis_index("tp")
    ci = lax.axis_index("ctx")
    core = lax.rem(ci, 2)
    xpeer = lax.rem(ci + 2, 4)
    dpeer = ci + 1 - 2 * core
    pieces = (ci, 7 - ci)
    mine = tuple(pl.ds(pl.multiple_of(sl * half, half), half) for sl in (core, 1 - core))
    theirs = tuple(pl.ds(pl.multiple_of(sl * half, half), half) for sl in (1 - core, core))
    first_pos = (2 * half * lax.div(ci, 2), half * (6 - 2 * lax.div(ci, 2)))
    half_rows = (slice(0, half), slice(half, 2 * half))

    def x_copy(k):
        cols = pl.ds(pl.multiple_of(k * kc, 128), kc)
        return pltpu.make_async_copy(x_hbm.at[pl.ds(0, half), cols], xc.at[mine[0], cols], xsem.at[k])

    def x2_copy():
        return pltpu.make_async_copy(x_hbm.at[pl.ds(half, half), :], x2, x2sem.at[0])

    def x_share(rows):
        return pltpu.make_async_remote_copy(src_ref=x_hbm.at[pl.ds(0, half), :], dst_ref=xc.at[rows, :], send_sem=xps.at[0],
                                            recv_sem=xpr.at[0], device_id={"ctx": dpeer}, device_id_type=MESH)

    def a_copies(k):
        col = pl.multiple_of(k * kc, 128)
        return (pltpu.make_async_copy(wkr_hbm.at[:, pl.ds(col, kc)], wkr.at[:, pl.ds(col, kc)], krsem.at[k]),
                pltpu.make_async_copy(wdkv_hbm.at[pl.ds(col, kc), :], kvs.at[pl.ds(col, kc), :], kvsem.at[k]))

    def b_copy(m, n):
        s = lax.rem(m, DQ_SLOTS)
        return pltpu.make_async_copy(wdq_hbm.at[:, pl.ds(pl.multiple_of(n * NBLK, NBLK), NBLK)],
                                     arena.at[pl.ds(pl.multiple_of(s * D, D), D), :], bsem.at[s])

    def q_copies(g):
        i = lax.rem(g, ngrp) + core * ngrp
        s = lax.rem(g, RING)
        c4 = pl.ds(pl.multiple_of(i * 512, 512), 512)
        c2 = pl.ds(pl.multiple_of(i * 256, 256), 256)
        return (pltpu.make_async_copy(wuq_hbm.at[:, c4], uqb.at[s], qsem.at[s, 0]),
                pltpu.make_async_copy(wqr_hbm.at[:, c2], qrb.at[s], qsem.at[s, 1]))

    def up_copies(i):
        c4 = pl.ds(pl.multiple_of((i + core * ngrp) * 512, 512), 512)
        return (pltpu.make_async_copy(wuk_hbm.at[:, c4], upw.at[i], upsem.at[i, 0]),
                pltpu.make_async_copy(wuv_hbm.at[:, c4], upw.at[ngrp + i], upsem.at[i, 1]))

    def wo_copy(L):
        j = lax.rem(L, nblk)
        side = jnp.where(L < 2 * nblk, 1 - tp, tp)
        s = lax.rem(L, WO_SLOTS)
        col = pl.multiple_of(side * own_cols + j * NBLK, NBLK)
        return pltpu.make_async_copy(wo_hbm.at[:, pl.ds(col, NBLK)],
                                     arena.at[pl.ds(pl.multiple_of(s * hv, hv), hv), :], wosem.at[s])

    def start(cps):
        for c in cps:
            c.start()

    def wait(cps):
        for c in cps:
            c.wait()

    for k in range(KCH):
        x_copy(k).start()
        start(a_copies(k))

    bar = pltpu.get_barrier_semaphore()
    for dev in ({"tp": 1 - tp}, {"ctx": xpeer}, {"ctx": dpeer}):
        pl.semaphore_signal(bar, inc=1, device_id=dev, device_id_type=MESH)

    lane = lax.broadcasted_iota(jnp.int32, (1, 128), 1)
    first_half = lax.rem(lane, 64) < 32

    def rotary(hf):
        fidx = lax.rem(lane, 32)
        freq = jnp.zeros((1, 128), F32)
        for j in range(32):
            freq = jnp.where(fidx == j, ROPE_BASE ** (-j * 2.0 / 64), freq)
        eye = (lax.broadcasted_iota(jnp.int32, (half, half), 0) == lax.broadcasted_iota(jnp.int32, (half, half), 1))
        prow = pos_ref[hf:hf + 1, :].astype(F32)
        pcol = jnp.sum(jnp.where(eye, jnp.broadcast_to(prow, (half, half)), 0.0), axis=1, keepdims=True)
        ang = pcol * freq
        rot[hf, mine[hf], 0:128] = jnp.cos(ang)
        sn = jnp.sin(ang)
        rot[hf, mine[hf], 128:256] = jnp.where(first_half, -sn, sn)

    def turn(a, table):
        swapped = jnp.where(first_half, pltpu.roll(a, 96, 1), pltpu.roll(a, 32, 1))
        return a * table[:, 0:128] + swapped * table[:, 128:256]

    def to_core(ref, ssem, rsem):
        return pltpu.make_async_remote_copy(src_ref=ref, dst_ref=ref, send_sem=ssem, recv_sem=rsem,
                                            device_id={"ctx": dpeer}, device_id_type=MESH)

    def rot_send(hf):
        return to_core(rot.at[hf, mine[hf], :], rots.at[hf], rotr.at[hf])

    def rot_recv(hf):
        return to_core(rot.at[hf, theirs[hf], :], rots.at[hf], rotr.at[hf])

    def lat_send(piece, slot, dev):
        ref = lat.at[pl.ds(pl.multiple_of(piece * half, half), half), :]
        return pltpu.make_async_remote_copy(src_ref=ref, dst_ref=ref, send_sem=lats.at[slot], recv_sem=latr.at[piece],
                                            device_id={"ctx": dev}, device_id_type=MESH)

    def lat_finish(hf, a, kr):
        inv = lax.rsqrt(jnp.mean(a * a, axis=-1, keepdims=True) + NORM_EPS)
        kr2 = turn(jnp.concatenate([kr, kr], axis=1), rot[hf, mine[hf], :])
        row0 = pl.multiple_of(pieces[hf] * half, half)
        for c in range(LR // 128):
            cols = slice(c * 128, (c + 1) * 128)
            lat[pl.ds(row0, half), cols] = (a[:, cols] * inv * gkv_ref[c:c + 1, :].astype(F32)).astype(BF16)
        lat[pl.ds(row0, half), LR:LR + 128] = kr2.astype(BF16)

    def lat_share(hf):
        lat_send(pieces[hf], 2 * hf, xpeer).start()
        lat_send(pieces[hf], 2 * hf + 1, dpeer).start()

    far = (xpeer, 7 - xpeer)
    near = (dpeer, 7 - dpeer)
    relayed = (3 - ci, 4 + ci)

    def lat_recv(piece):
        lat_send(piece, 0, dpeer).wait_recv()

    def forward(hf):
        lat_recv(far[hf])
        lat_send(far[hf], 4 + hf, dpeer).start()

    def gathered(hf):
        lat_recv(near[hf])
        lat_recv(relayed[hf])
        rows = slice(hf * 4 * half, (hf + 1) * 4 * half)
        kp = lat[rows, LR:LR + 128].astype(F32)
        low = lane < 64
        kplo[rows, :] = jnp.where(low, kp, 0.0).astype(BF16)
        kphi[rows, :] = jnp.where(low, 0.0, kp).astype(BF16)

    nb_c = nb_q // 2

    def half_send(m):
        ref = ownb.at[pl.ds(2 * (core * nb_c + m), 2)]
        return to_core(ref, hs.at[0], hr.at[0])

    def half_all(side):
        ref = ownb.at[pl.ds(2 * side * nb_c, 2 * nb_c)]
        return to_core(ref, hs.at[0], hr.at[0])

    def norm_queries(chunk, rows, block):
        sq = 0.0
        for n in range(nb_q):
            a = ownb[block(n)]
            sq = sq + jnp.sum(a * a, axis=-1, keepdims=True)
        inv = lax.rsqrt(sq * (1.0 / QR) + NORM_EPS)
        for n in range(nb_q):
            a = ownb[block(n)] * inv
            for u in range(NBLK // 128):
                c = n * (NBLK // 128) + u
                cq[chunk, rows, c * 128:(c + 1) * 128] = (
                    a[:, u * 128:(u + 1) * 128] * gq_ref[c:c + 1, :].astype(F32)).astype(BF16)

    def cq_share(rows):
        return to_core(cq.at[1, rows, :], cqs.at[0], cqr.at[0])

    def queries(chunk):
        def group(i):
            g = i + chunk * ngrp
            s = lax.rem(g, RING)
            wait(q_copies(g))
            c = cq[chunk]
            r = _dot(c, qrb[s])
            qn[:, pl.ds(pl.multiple_of(i * 512, 512), 512)] = _dot(c, uqb[s]).astype(BF16)
            for u in range(2):
                qp[:, pl.ds(pl.multiple_of(i * 256 + u * 128, 128), 128)] = turn(r[:, u * 128:(u + 1) * 128], rot[chunk]).astype(BF16)

            @pl.when(g + RING < 2 * ngrp)
            def _():
                start(q_copies(g + RING))

        def body(i, carry):
            if chunk == 0:
                @pl.when(i == ngrp // 2)
                def _():
                    forward(0)
            group(i)
            return carry

        lax.fori_loop(0, ngrp, body, 0)

    def kv_rows(i, n):
        return pl.ds(pl.multiple_of(i * ntok, ntok), n)

    def keys_values(chunk, nk):
        per = 2 if chunk == 0 else 1

        def body(t, carry):
            if chunk == 0:
                for u in range(per):
                    wait(up_copies(per * t + u))
            lt = lat[0:nk, 0:LR]
            for u in range(per):
                i = per * t + u
                kvs[kv_rows(i, nk), :] = _dot(lt, upw[i]).astype(BF16)
                kvs[kv_rows(ngrp + i, nk), :] = _dot(lt, upw[ngrp + i]).astype(BF16)
            return carry

        lax.fori_loop(0, ngrp // per, body, 0)

    c2e = score_scale * 1.4426950408889634

    def o_send(chunk, i):
        cols = pl.ds(pl.multiple_of(i * 512, 512), 512)
        return pltpu.make_async_remote_copy(src_ref=os.at[chunk, theirs[chunk], cols], dst_ref=orx.at[chunk, :, cols],
                                            send_sem=oss.at[chunk], recv_sem=osr.at[chunk],
                                            device_id={"ctx": dpeer}, device_id_type=MESH)

    def attention(chunk, nk):
        nq = 2 * half

        def body(i, carry):
            wo_copy(chunk * nblk + i).start()

            @pl.when(i == ngrp - 1)
            def _():
                for extra in range(ngrp, WO_SLOTS - 1):
                    wo_copy(chunk * nblk + extra).start()
            vis = (lax.broadcasted_iota(jnp.int32, (nq, nk), 1)
                   <= lax.broadcasted_iota(jnp.int32, (nq, nk), 0) + first_pos[chunk])

            def scores(h):
                kp = kphi if h % 2 else kplo
                qpe = qp[:, pl.ds(pl.multiple_of(i * 256 + (h // 2) * 128, 128), 128)]
                qh = jnp.concatenate([qn[:, pl.ds(pl.multiple_of(i * 512 + h * 128, 128), 128)], qpe], axis=1)
                kh = jnp.concatenate([kvs[kv_rows(i, nk), h * 128:(h + 1) * 128], kp[0:nk, :]], axis=1)
                return _dot_nt(qh, kh)

            def values(h, sc):
                sc = jnp.where(vis, sc, NEG_BIG)
                top = jnp.max(sc, axis=1, keepdims=True)
                p = jnp.exp2((sc - top) * c2e)
                tot = jnp.sum(p, axis=1, keepdims=True)
                acc = _dot(p.astype(BF16), kvs[kv_rows(ngrp + i, nk), h * 128:(h + 1) * 128])
                os[chunk, :, pl.ds(pl.multiple_of(i * 512 + h * 128, 128), 128)] = (acc / tot).astype(BF16)

            sc = scores(0)
            for h in range(4):
                nxt = scores(h + 1) if h < 3 else None
                values(h, sc)
                sc = nxt
            o_send(chunk, i).start()
            return carry

        lax.fori_loop(0, ngrp, body, 0)

    def o_all(chunk):
        return pltpu.make_async_remote_copy(src_ref=os.at[chunk, theirs[chunk], :], dst_ref=orx.at[chunk],
                                            send_sem=oss.at[chunk], recv_sem=osr.at[chunk],
                                            device_id={"ctx": dpeer}, device_id_type=MESH)

    total_wo = 3 * nblk
    ahead = WO_SLOTS - 1
    hc = HC * 128

    def wo_next(L):
        wo_copy(L).wait()
        wo_refill(L)

    def wo_refill(L):
        @pl.when(jnp.logical_and(L + ahead < total_wo, jnp.logical_or(L >= nblk, L + ahead < nblk)))
        def _():
            wo_copy(L + ahead).start()

    def project_here(chunk, L):
        w = arena[pl.ds(pl.multiple_of(lax.rem(L, WO_SLOTS) * hv + core * hc, hc), hc), :]
        return _dot(os[chunk, mine[chunk], :], w)

    def project_there(chunk, L):
        w = arena[pl.ds(pl.multiple_of(lax.rem(L, WO_SLOTS) * hv + (1 - core) * hc, hc), hc), :]
        return _dot(orx[chunk], w)

    def part_copy(chunk, q, src, dst):
        return pltpu.make_async_remote_copy(src_ref=src, dst_ref=dst, send_sem=ps.at[chunk, q], recv_sem=pr.at[chunk, q],
                                            device_id={"tp": 1 - tp}, device_id_type=MESH)

    def part_send(chunk, j):
        return part_copy(chunk, lax.div(j, GROUP), sendb.at[j], recvb.at[chunk * nblk + j])

    def part_group(chunk, q):
        return part_copy(chunk, q, sendb.at[pl.ds(q * GROUP, GROUP)], recvb.at[pl.ds(chunk * nblk + q * GROUP, GROUP)])

    def project_partner(chunk):
        early = 2
        base = chunk * nblk

        def send_slot(j):
            if chunk == 1:
                @pl.when(lax.rem(j, GROUP) == 0)
                def _():
                    part_group(0, lax.div(j, GROUP)).wait_send()

        for j in range(early):
            wo_copy(base + j).wait()
            if j == 0:
                wo_refill(base)
            send_slot(j)
            sendb[j] = project_here(chunk, base + j)
        o_all(chunk).wait_recv()
        for j in range(early):
            sendb[j] += project_there(chunk, base + j)
            part_send(chunk, j).start()
            if j + 1 < early:
                wo_refill(base + j + 1)

        def body(j, carry):
            wo_next(base + j)
            send_slot(j)
            sendb[j] = project_here(chunk, base + j) + project_there(chunk, base + j)
            part_send(chunk, j).start()
            return carry

        lax.fori_loop(early, nblk, body, 0)

    def y_cols(side, j, n):
        return pl.ds(pl.multiple_of(side * own_cols + j * NBLK, NBLK), n)

    def result_copy(ref):
        return pltpu.make_async_remote_copy(src_ref=ref, dst_ref=ref, send_sem=rs.at[0], recv_sem=rr.at[0],
                                            device_id={"tp": 1 - tp}, device_id_type=MESH)

    def give_back(chunk, j, own):
        @pl.when(lax.rem(j, GROUP) == 0)
        def _():
            part_group(chunk, lax.div(j, GROUP)).wait_recv()
        cols = y_cols(tp, j, NBLK)
        y_ref[half_rows[chunk], cols] = (recvb[chunk * nblk + j] + own).astype(BF16)
        result_copy(y_ref.at[half_rows[chunk], cols]).start()

    acckv[...] = jnp.zeros_like(acckv)
    acckr[...] = jnp.zeros_like(acckr)
    with jax.named_scope('rot0'):
        rotary(0)

    pl.semaphore_wait(bar, 3)
    x_share(mine[0]).start()

    def a_step(k, carry):
        x_copy(k).wait()
        wait(a_copies(k))

        @pl.when(lax.rem(k, 2) == 0)
        def _():
            m = lax.div(k, 2)
            b_copy(m, core * nb_c + m).start()
        cols = pl.ds(pl.multiple_of(k * kc, 128), kc)
        xk = xc[mine[0], cols]
        acckv[...] += _dot(xk, kvs[cols, :])
        acckr[...] += _dot_nt(xk, wkr[:, cols])
        return carry

    with jax.named_scope('lat0'):
        lax.fori_loop(0, KCH, a_step, 0)
        x2_copy().start()
        lat_finish(0, acckv[...], acckr[...])
        lat_share(0)
        rot_send(0).start()
    with jax.named_scope('xwait'):
        x_share(theirs[0]).wait_recv()

    def dq_block(m, rows):
        return _dot(rows, arena[pl.ds(pl.multiple_of(lax.rem(m, DQ_SLOTS) * D, D), D), :])

    def b_step(m, carry):
        n = core * nb_c + m
        b_copy(m, n).wait()
        start(q_copies(m))
        r = dq_block(m, xc[...])
        ownb[2 * n] = r[:half]
        ownb[2 * n + 1] = r[half:]
        half_send(m).start()
        return carry

    with jax.named_scope('qlat0'):
        lax.fori_loop(0, nb_c, b_step, 0)
        for m in range(nb_c, RING):
            start(q_copies(m))
        for i in range(ngrp):
            start(up_copies(i))
    with jax.named_scope('lat1'):
        rotary(1)
        rot_send(1).start()
        x2_copy().wait()
        xs = x2[...]
        lat_finish(1, _dot(xs, kvs[0:D, :]), _dot_nt(xs, wkr[...]))
        lat_share(1)
    with jax.named_scope('qfin0'):
        half_all(1 - core).wait_recv()
        for sl in range(2):
            norm_queries(0, half_rows[sl], lambda n, sl=sl: 2 * n + sl)
        rot_recv(0).wait_recv()
    with jax.named_scope('q0'):
        queries(0)
    with jax.named_scope('gather0'):
        gathered(0)
    with jax.named_scope('kv0'):
        keys_values(0, 4 * half)
    with jax.named_scope('att0'):
        attention(0, 4 * half)
    with jax.named_scope('part0'):
        project_partner(0)

    def b1_step(n, carry):
        @pl.when(n + 3 < nb_q)
        def _():
            b_copy(n + 3, n + 3).start()
        b_copy(n, n).wait()
        ownb[n] = dq_block(n, x2[...])
        return carry

    with jax.named_scope('qlat1'):
        half_all(core).wait_send()
        for n in range(3):
            b_copy(n, n).start()
        forward(1)
        lax.fori_loop(0, nb_q, b1_step, 0)
        norm_queries(1, mine[1], lambda n: n)
        cq_share(mine[1]).start()
    with jax.named_scope('gather1'):
        gathered(1)
    with jax.named_scope('kv1'):
        keys_values(1, 8 * half)
    with jax.named_scope('q1'):
        cq_share(theirs[1]).wait_recv()
        rot_recv(1).wait_recv()
        queries(1)
    with jax.named_scope('att1'):
        attention(1, 8 * half)
    with jax.named_scope('part1'):
        project_partner(1)

    def own_body(j, carry):
        L = 2 * nblk + j
        wo_next(L)
        ownb[j] = project_here(1, L) + project_there(1, L)
        give_back(0, j, project_here(0, L) + project_there(0, L))
        return carry

    with jax.named_scope('own'):
        lax.fori_loop(0, nblk, own_body, 0)

    def ret_body(j, carry):
        give_back(1, j, ownb[j])
        return carry

    with jax.named_scope('ret'):
        lax.fori_loop(0, nblk, ret_body, 0)

    with jax.named_scope('drain'):
        for q in range(nblk // GROUP):
            part_group(1, q).wait_send()
        result_copy(y_ref.at[:, y_cols(tp, 0, own_cols)]).wait_send()
        result_copy(y_ref.at[:, y_cols(1 - tp, 0, own_cols)]).wait_recv()
    for slot, piece in ((0, pieces[0]), (1, pieces[0]), (2, pieces[1]), (3, pieces[1]), (4, far[0]), (5, far[1])):
        lat_send(piece, slot, dpeer).wait_send()
    x_share(mine[0]).wait_send()
    cq_share(mine[1]).wait_send()
    for hf in range(2):
        rot_send(hf).wait_send()
        o_all(hf).wait_send()


def solution(mesh):
    tok_spec = P(('dp', 'ctx'), None)
    pos_spec = P(('dp', 'ctx'))
    full_mat = P(None, None)
    full_vec = P(None)
    col_spec = P(None, 'tp')
    row_spec = P('tp', None)

    def local_step(tok_x, tok_pos, w_dq, g_q, w_uq, w_qr, w_dkv, g_kv, w_kr, w_uk, w_uv, w_o):
        rows, D = tok_x.shape
        half = rows // 2
        QR = w_dq.shape[1]
        LR = w_dkv.shape[1]
        HL = w_qr.shape[1] // w_kr.shape[1]
        scale = (128 + w_kr.shape[1]) ** -0.5
        nblk = D // 2 // NBLK
        ngrp = HL // 8
        ntok = 8 * half
        dims = (D, QR, LR, HL, half, scale)
        anyspec = pl.BlockSpec(memory_space=pl.ANY)
        vspec = pl.BlockSpec(memory_space=pltpu.VMEM)
        dma = pltpu.SemaphoreType.DMA
        arena_rows = max(DQ_SLOTS * D, WO_SLOTS * HL * 128)
        return pl.pallas_call(
            functools.partial(layer_kernel, dims),
            out_shape=pltpu.VMEM((rows, D), BF16),
            in_specs=[anyspec, vspec, anyspec, vspec, anyspec, anyspec, anyspec, vspec, anyspec, anyspec, anyspec, anyspec],
            out_specs=vspec,
            scratch_shapes=[
                pltpu.VMEM((rows, D), BF16),
                pltpu.VMEM((half, D), BF16),
                pltpu.VMEM((max(D, 2 * ngrp * ntok), LR), BF16),
                pltpu.VMEM((64, D), BF16),
                pltpu.VMEM((2 * ngrp, LR, 512), BF16),
                pltpu.VMEM((arena_rows, NBLK), BF16),
                pltpu.VMEM((ntok, LR + 128), BF16),
                pltpu.VMEM((ntok, 128), BF16),
                pltpu.VMEM((ntok, 128), BF16),
                pltpu.VMEM((2, rows, QR), BF16),
                pltpu.VMEM((half, LR), F32),
                pltpu.VMEM((half, 64), F32),
                pltpu.VMEM((2, rows, 256), F32),
                pltpu.VMEM((RING, QR, 512), BF16),
                pltpu.VMEM((RING, QR, 256), BF16),
                pltpu.VMEM((rows, HL * 64), BF16),
                pltpu.VMEM((rows, HL * 32), BF16),
                pltpu.VMEM((2, rows, HL * 64), BF16),
                pltpu.VMEM((2, half, HL * 64), BF16),
                pltpu.VMEM((nblk, half, NBLK), F32),
                pltpu.VMEM((2 * nblk, half, NBLK), F32),
                pltpu.VMEM((max(nblk, 2 * QR // NBLK), half, NBLK), F32),
                dma((KCH,)), dma((1,)), dma((1,)), dma((1,)), dma((KCH,)), dma((KCH,)), dma((DQ_SLOTS,)), dma((RING, 2)), dma((ngrp, 2)), dma((WO_SLOTS,)),
                dma((6,)), dma((8,)), dma((1,)), dma((1,)), dma((1,)), dma((1,)), dma((2,)), dma((2,)), dma((2,)), dma((2,)),
                dma((2, nblk // GROUP)), dma((2, nblk // GROUP)), dma((1,)), dma((1,)),
            ],
            compiler_params=pltpu.CompilerParams(collective_id=0, has_side_effects=True,
                                                 vmem_limit_bytes=60500 * 1000),
        )(tok_x, tok_pos.reshape(2, half), w_dq, g_q.reshape(QR // 128, 128), w_uq, w_qr, w_dkv, g_kv.reshape(LR // 128, 128), w_kr.T,
          w_uk, w_uv, w_o)

    return jax.shard_map(local_step, mesh=mesh,
                         in_specs=(tok_spec, pos_spec, full_mat, full_vec, col_spec, col_spec, full_mat, full_vec, full_mat, col_spec, col_spec, row_spec),
                         out_specs=tok_spec, check_vma=False)
```

```python
import functools

import jax
import jax.numpy as jnp
from jax import lax
from jax.experimental import pallas as pl
from jax.experimental.pallas import tpu as pltpu
from jax.sharding import PartitionSpec as P

ROPE_BASE = 10000.0
NORM_EPS = 1e-6
NEG_BIG = -1e30
MESH = pl.DeviceIdType.MESH
F32 = jnp.float32
BF16 = jnp.bfloat16

KCH = 6
NBLK = 256
RING = 4
DQ_SLOTS = 4
GROUP = 4
WO_SLOTS = 6


def _dot(a, b):
    return jnp.dot(a, b, preferred_element_type=F32)


def _dot_nt(a, b):
    return lax.dot_general(a, b, (((1,), (1,)), ((), ())), preferred_element_type=F32)


def layer_kernel(dims, x_hbm, pos_hbm, wdq_hbm, gq_hbm, wuq_hbm, wqr_hbm, wdkv_hbm, gkv_hbm, wkr_hbm, wuk_hbm, wuv_hbm,
                 wo_hbm, y_ref,
                 pos_ref, gq_ref, gkv_ref, xc, x2, kvs, wkr, upw, arena, lat, kplo, kphi, cq, acckv, acckr, rot,
                 uqb, qrb, qn, qp, os, orx, sendb, recvb, ownb,
                 smsem, xsem, x2sem, xps, xpr, kvsem, krsem, bsem, qsem, upsem, wosem, lats, latr, cqs, cqr, hs, hr, rots, rotr, oss, osr, ps, pr, rs, rr):
    D, QR, LR, HL, half, score_scale = dims
    HC = HL // 2
    ngrp = HC // 4
    kc = D // KCH
    nb_q = QR // NBLK
    own_cols = D // 2
    nblk = own_cols // NBLK
    hv = HL * 128
    ntok = 8 * half
    tp = lax.axis_index("tp")
    ci = lax.axis_index("ctx")
    core = lax.rem(ci, 2)
    xpeer = lax.rem(ci + 2, 4)
    dpeer = ci + 1 - 2 * core
    pieces = (ci, 7 - ci)
    mine = tuple(pl.ds(pl.multiple_of(sl * half, half), half) for sl in (core, 1 - core))
    theirs = tuple(pl.ds(pl.multiple_of(sl * half, half), half) for sl in (1 - core, core))
    first_pos = (2 * half * lax.div(ci, 2), half * (6 - 2 * lax.div(ci, 2)))
    half_rows = (slice(0, half), slice(half, 2 * half))

    def x_copy(k):
        cols = pl.ds(pl.multiple_of(k * kc, 128), kc)
        return pltpu.make_async_copy(x_hbm.at[pl.ds(0, half), cols], xc.at[mine[0], cols], xsem.at[k])

    def x2_copy():
        return pltpu.make_async_copy(x_hbm.at[pl.ds(half, half), :], x2, x2sem.at[0])

    def x_share(rows):
        return pltpu.make_async_remote_copy(src_ref=x_hbm.at[pl.ds(0, half), :], dst_ref=xc.at[rows, :], send_sem=xps.at[0],
                                            recv_sem=xpr.at[0], device_id={"ctx": dpeer}, device_id_type=MESH)

    def a_copies(k):
        col = pl.multiple_of(k * kc, 128)
        return (pltpu.make_async_copy(wkr_hbm.at[:, pl.ds(col, kc)], wkr.at[:, pl.ds(col, kc)], krsem.at[k]),
                pltpu.make_async_copy(wdkv_hbm.at[pl.ds(col, kc), :], kvs.at[pl.ds(col, kc), :], kvsem.at[k]))

    def b_copy(m, n):
        s = lax.rem(m, DQ_SLOTS)
        return pltpu.make_async_copy(wdq_hbm.at[:, pl.ds(pl.multiple_of(n * NBLK, NBLK), NBLK)],
                                     arena.at[pl.ds(pl.multiple_of(s * D, D), D), :], bsem.at[s])

    def q_copies(g):
        i = lax.rem(g, ngrp) + core * ngrp
        s = lax.rem(g, RING)
        c4 = pl.ds(pl.multiple_of(i * 512, 512), 512)
        c2 = pl.ds(pl.multiple_of(i * 256, 256), 256)
        return (pltpu.make_async_copy(wuq_hbm.at[:, c4], uqb.at[s], qsem.at[s, 0]),
                pltpu.make_async_copy(wqr_hbm.at[:, c2], qrb.at[s], qsem.at[s, 1]))

    def up_copies(i):
        c4 = pl.ds(pl.multiple_of((i + core * ngrp) * 512, 512), 512)
        return (pltpu.make_async_copy(wuk_hbm.at[:, c4], upw.at[i], upsem.at[i, 0]),
                pltpu.make_async_copy(wuv_hbm.at[:, c4], upw.at[ngrp + i], upsem.at[i, 1]))

    def wo_copy(L):
        j = lax.rem(L, nblk)
        side = jnp.where(L < 2 * nblk, 1 - tp, tp)
        s = lax.rem(L, WO_SLOTS)
        col = pl.multiple_of(side * own_cols + j * NBLK, NBLK)
        return pltpu.make_async_copy(wo_hbm.at[:, pl.ds(col, NBLK)],
                                     arena.at[pl.ds(pl.multiple_of(s * hv, hv), hv), :], wosem.at[s])

    def start(cps):
        for c in cps:
            c.start()

    def wait(cps):
        for c in cps:
            c.wait()

    bar = pltpu.get_barrier_semaphore()
    for dev in ({"ctx": xpeer}, {"tp": 1 - tp}, {"ctx": dpeer}):
        pl.semaphore_signal(bar, inc=1, device_id=dev, device_id_type=MESH)

    small = (pltpu.make_async_copy(pos_hbm, pos_ref, smsem.at[0]), pltpu.make_async_copy(gkv_hbm, gkv_ref, smsem.at[1]),
             pltpu.make_async_copy(gq_hbm, gq_ref, smsem.at[2]))
    start(small)
    for k in range(KCH):
        x_copy(k).start()
        start(a_copies(k))

    lane = lax.broadcasted_iota(jnp.int32, (1, 128), 1)
    first_half = lax.rem(lane, 64) < 32

    def rotary(hf):
        fidx = lax.rem(lane, 32)
        freq = jnp.zeros((1, 128), F32)
        for j in range(32):
            freq = jnp.where(fidx == j, ROPE_BASE ** (-j * 2.0 / 64), freq)
        eye = (lax.broadcasted_iota(jnp.int32, (half, half), 0) == lax.broadcasted_iota(jnp.int32, (half, half), 1))
        prow = pos_ref[hf:hf + 1, :].astype(F32)
        pcol = jnp.sum(jnp.where(eye, jnp.broadcast_to(prow, (half, half)), 0.0), axis=1, keepdims=True)
        ang = pcol * freq
        rot[hf, mine[hf], 0:128] = jnp.cos(ang)
        sn = jnp.sin(ang)
        rot[hf, mine[hf], 128:256] = jnp.where(first_half, -sn, sn)

    def turn(a, table):
        swapped = jnp.where(first_half, pltpu.roll(a, 96, 1), pltpu.roll(a, 32, 1))
        return a * table[:, 0:128] + swapped * table[:, 128:256]

    def to_core(ref, ssem, rsem):
        return pltpu.make_async_remote_copy(src_ref=ref, dst_ref=ref, send_sem=ssem, recv_sem=rsem,
                                            device_id={"ctx": dpeer}, device_id_type=MESH)

    def rot_send(hf):
        return to_core(rot.at[hf, mine[hf], :], rots.at[hf], rotr.at[hf])

    def rot_recv(hf):
        return to_core(rot.at[hf, theirs[hf], :], rots.at[hf], rotr.at[hf])

    def lat_send(piece, slot, dev):
        ref = lat.at[pl.ds(pl.multiple_of(piece * half, half), half), :]
        return pltpu.make_async_remote_copy(src_ref=ref, dst_ref=ref, send_sem=lats.at[slot], recv_sem=latr.at[piece],
                                            device_id={"ctx": dev}, device_id_type=MESH)

    def lat_finish(hf, a, kr):
        inv = lax.rsqrt(jnp.mean(a * a, axis=-1, keepdims=True) + NORM_EPS)
        kr2 = turn(jnp.concatenate([kr, kr], axis=1), rot[hf, mine[hf], :])
        row0 = pl.multiple_of(pieces[hf] * half, half)
        for c in range(LR // 128):
            cols = slice(c * 128, (c + 1) * 128)
            lat[pl.ds(row0, half), cols] = (a[:, cols] * inv * gkv_ref[c:c + 1, :].astype(F32)).astype(BF16)
        lat[pl.ds(row0, half), LR:LR + 128] = kr2.astype(BF16)

    def lat_share(hf):
        lat_send(pieces[hf], 2 * hf, xpeer).start()
        lat_send(pieces[hf], 2 * hf + 1, dpeer).start()

    far = (xpeer, 7 - xpeer)
    near = (dpeer, 7 - dpeer)
    relayed = (3 - ci, 4 + ci)

    def lat_recv(piece):
        lat_send(piece, 0, dpeer).wait_recv()

    def forward(hf):
        lat_recv(far[hf])
        lat_send(far[hf], 4 + hf, dpeer).start()

    def gathered(hf):
        lat_recv(near[hf])
        lat_recv(relayed[hf])
        rows = slice(hf * 4 * half, (hf + 1) * 4 * half)
        kp = lat[rows, LR:LR + 128].astype(F32)
        low = lane < 64
        kplo[rows, :] = jnp.where(low, kp, 0.0).astype(BF16)
        kphi[rows, :] = jnp.where(low, 0.0, kp).astype(BF16)

    nb_c = nb_q // 2

    def half_send(m):
        ref = ownb.at[pl.ds(2 * (core * nb_c + m), 2)]
        return to_core(ref, hs.at[0], hr.at[0])

    def half_all(side):
        ref = ownb.at[pl.ds(2 * side * nb_c, 2 * nb_c)]
        return to_core(ref, hs.at[0], hr.at[0])

    def norm_queries(chunk, rows, block):
        sq = 0.0
        for n in range(nb_q):
            a = ownb[block(n)]
            sq = sq + jnp.sum(a * a, axis=-1, keepdims=True)
        inv = lax.rsqrt(sq * (1.0 / QR) + NORM_EPS)
        for n in range(nb_q):
            a = ownb[block(n)] * inv
            for u in range(NBLK // 128):
                c = n * (NBLK // 128) + u
                cq[chunk, rows, c * 128:(c + 1) * 128] = (
                    a[:, u * 128:(u + 1) * 128] * gq_ref[c:c + 1, :].astype(F32)).astype(BF16)

    def cq_share(rows):
        return to_core(cq.at[1, rows, :], cqs.at[0], cqr.at[0])

    def queries(chunk):
        def body(t, carry):
            if chunk == 0:
                @pl.when(t == 1)
                def _():
                    forward(0)
            gs = [2 * t + u + chunk * ngrp for u in range(2)]
            for g in gs:
                wait(q_copies(g))
            c = cq[chunk]
            for u in range(2):
                i = 2 * t + u
                s = lax.rem(gs[u], RING)
                r = _dot(c, qrb[s])
                qn[:, pl.ds(pl.multiple_of(i * 512, 512), 512)] = _dot(c, uqb[s]).astype(BF16)
                for v in range(2):
                    qp[:, pl.ds(pl.multiple_of(i * 256 + v * 128, 128), 128)] = turn(
                        r[:, v * 128:(v + 1) * 128], rot[chunk]).astype(BF16)
            for g in gs:
                @pl.when(g + RING < 2 * ngrp)
                def _():
                    start(q_copies(g + RING))
            return carry

        lax.fori_loop(0, ngrp // 2, body, 0)

    def kv_rows(i, n):
        return pl.ds(pl.multiple_of(i * ntok, ntok), n)

    def keys_values(chunk, nk):
        per = 2 if chunk == 0 else 1

        def body(t, carry):
            if chunk == 0:
                for u in range(per):
                    wait(up_copies(per * t + u))
            lt = lat[0:nk, 0:LR]
            for u in range(per):
                i = per * t + u
                kvs[kv_rows(i, nk), :] = _dot(lt, upw[i]).astype(BF16)
                kvs[kv_rows(ngrp + i, nk), :] = _dot(lt, upw[ngrp + i]).astype(BF16)
            return carry

        lax.fori_loop(0, ngrp // per, body, 0)

    c2e = score_scale * 1.4426950408889634

    def o_send(chunk, i):
        cols = pl.ds(pl.multiple_of(i * 512, 512), 512)
        return pltpu.make_async_remote_copy(src_ref=os.at[chunk, theirs[chunk], cols], dst_ref=orx.at[chunk, :, cols],
                                            send_sem=oss.at[chunk], recv_sem=osr.at[chunk],
                                            device_id={"ctx": dpeer}, device_id_type=MESH)

    def attention(chunk, nk):
        nq = 2 * half

        def body(i, carry):
            wo_copy(chunk * nblk + i).start()

            @pl.when(i == ngrp - 1)
            def _():
                for extra in range(ngrp, WO_SLOTS - 1):
                    wo_copy(chunk * nblk + extra).start()
            vis = (lax.broadcasted_iota(jnp.int32, (nq, nk), 1)
                   <= lax.broadcasted_iota(jnp.int32, (nq, nk), 0) + first_pos[chunk])

            def scores(h):
                kp = kphi if h % 2 else kplo
                qpe = qp[:, pl.ds(pl.multiple_of(i * 256 + (h // 2) * 128, 128), 128)]
                qh = jnp.concatenate([qn[:, pl.ds(pl.multiple_of(i * 512 + h * 128, 128), 128)], qpe], axis=1)
                kh = jnp.concatenate([kvs[kv_rows(i, nk), h * 128:(h + 1) * 128], kp[0:nk, :]], axis=1)
                return _dot_nt(qh, kh)

            def values(h, sc):
                sc = jnp.where(vis, sc, NEG_BIG)
                top = jnp.max(sc, axis=1, keepdims=True)
                p = jnp.exp2((sc - top) * c2e)
                tot = jnp.sum(p, axis=1, keepdims=True)
                acc = _dot(p.astype(BF16), kvs[kv_rows(ngrp + i, nk), h * 128:(h + 1) * 128])
                os[chunk, :, pl.ds(pl.multiple_of(i * 512 + h * 128, 128), 128)] = (acc / tot).astype(BF16)

            sc = scores(0)
            for h in range(4):
                nxt = scores(h + 1) if h < 3 else None
                values(h, sc)
                sc = nxt
            o_send(chunk, i).start()
            return carry

        lax.fori_loop(0, ngrp, body, 0)

    def o_all(chunk):
        return pltpu.make_async_remote_copy(src_ref=os.at[chunk, theirs[chunk], :], dst_ref=orx.at[chunk],
                                            send_sem=oss.at[chunk], recv_sem=osr.at[chunk],
                                            device_id={"ctx": dpeer}, device_id_type=MESH)

    total_wo = 3 * nblk
    ahead = WO_SLOTS - 1
    hc = HC * 128

    def wo_next(L):
        wo_copy(L).wait()
        wo_refill(L)

    def wo_refill(L):
        @pl.when(jnp.logical_and(L + ahead < total_wo, jnp.logical_or(L >= nblk, L + ahead < nblk)))
        def _():
            wo_copy(L + ahead).start()

    def project_here(chunk, L):
        w = arena[pl.ds(pl.multiple_of(lax.rem(L, WO_SLOTS) * hv + core * hc, hc), hc), :]
        return _dot(os[chunk, mine[chunk], :], w)

    def project_there(chunk, L):
        w = arena[pl.ds(pl.multiple_of(lax.rem(L, WO_SLOTS) * hv + (1 - core) * hc, hc), hc), :]
        return _dot(orx[chunk], w)

    def part_copy(chunk, q, src, dst):
        return pltpu.make_async_remote_copy(src_ref=src, dst_ref=dst, send_sem=ps.at[chunk, q], recv_sem=pr.at[chunk, q],
                                            device_id={"tp": 1 - tp}, device_id_type=MESH)

    def part_send(chunk, j):
        return part_copy(chunk, lax.div(j, GROUP), sendb.at[j], recvb.at[chunk * nblk + j])

    def part_group(chunk, q):
        return part_copy(chunk, q, sendb.at[pl.ds(q * GROUP, GROUP)], recvb.at[pl.ds(chunk * nblk + q * GROUP, GROUP)])

    def project_partner(chunk):
        early = 2
        base = chunk * nblk

        def send_slot(j):
            if chunk == 1:
                @pl.when(lax.rem(j, GROUP) == 0)
                def _():
                    part_group(0, lax.div(j, GROUP)).wait_send()

        for j in range(early):
            wo_copy(base + j).wait()
            if j == 0:
                wo_refill(base)
            send_slot(j)
            sendb[j] = project_here(chunk, base + j)
        o_all(chunk).wait_recv()
        for j in range(early):
            sendb[j] += project_there(chunk, base + j)
            part_send(chunk, j).start()
            if j + 1 < early:
                wo_refill(base + j + 1)

        def body(j, carry):
            wo_next(base + j)
            send_slot(j)
            sendb[j] = project_here(chunk, base + j) + project_there(chunk, base + j)
            part_send(chunk, j).start()
            return carry

        lax.fori_loop(early, nblk, body, 0)

    def y_cols(side, j, n):
        return pl.ds(pl.multiple_of(side * own_cols + j * NBLK, NBLK), n)

    def result_copy(ref):
        return pltpu.make_async_remote_copy(src_ref=ref, dst_ref=ref, send_sem=rs.at[0], recv_sem=rr.at[0],
                                            device_id={"tp": 1 - tp}, device_id_type=MESH)

    def give_back(chunk, j, own):
        @pl.when(lax.rem(j, GROUP) == 0)
        def _():
            part_group(chunk, lax.div(j, GROUP)).wait_recv()
        cols = y_cols(tp, j, NBLK)
        y_ref[half_rows[chunk], cols] = (recvb[chunk * nblk + j] + own).astype(BF16)

        @pl.when(lax.rem(j, GROUP) == GROUP - 1)
        def _():
            result_copy(y_ref.at[half_rows[chunk], y_cols(tp, j - (GROUP - 1), GROUP * NBLK)]).start()

    acckv[...] = jnp.zeros_like(acckv)
    acckr[...] = jnp.zeros_like(acckr)
    def a_step(k, carry):
        @pl.when(k == 1)
        def _():
            pl.semaphore_wait(bar, 3)
            x_share(mine[0]).start()
        x_copy(k).wait()
        wait(a_copies(k))

        @pl.when(k == 3)
        def _():
            wait(small)
            rotary(0)

        @pl.when(lax.rem(k, 2) == 0)
        def _():
            m = lax.div(k, 2)
            b_copy(m, core * nb_c + m).start()
        cols = pl.ds(pl.multiple_of(k * kc, 128), kc)
        xk = xc[mine[0], cols]
        acckv[...] += _dot(xk, kvs[cols, :])
        acckr[...] += _dot_nt(xk, wkr[:, cols])
        return carry

    with jax.named_scope('lat0'):
        lax.fori_loop(0, KCH, a_step, 0)
        x2_copy().start()
        lat_finish(0, acckv[...], acckr[...])
        lat_share(0)
        rot_send(0).start()
    with jax.named_scope('xwait'):
        x_share(theirs[0]).wait_recv()

    def dq_block(m, rows):
        return _dot(rows, arena[pl.ds(pl.multiple_of(lax.rem(m, DQ_SLOTS) * D, D), D), :])

    def b_step(m, carry):
        n = core * nb_c + m
        b_copy(m, n).wait()
        start(q_copies(m))
        r = dq_block(m, xc[...])
        ownb[2 * n] = r[:half]
        ownb[2 * n + 1] = r[half:]
        half_send(m).start()
        return carry

    with jax.named_scope('qlat0'):
        lax.fori_loop(0, nb_c, b_step, 0)
        for m in range(nb_c, RING):
            start(q_copies(m))
        for i in range(ngrp):
            start(up_copies(i))
    with jax.named_scope('lat1'):
        rotary(1)
        rot_send(1).start()
        x2_copy().wait()
        xs = x2[...]
        lat_finish(1, _dot(xs, kvs[0:D, :]), _dot_nt(xs, wkr[...]))
        lat_share(1)
    with jax.named_scope('qfin0'):
        half_all(1 - core).wait_recv()
        for sl in range(2):
            norm_queries(0, half_rows[sl], lambda n, sl=sl: 2 * n + sl)
        rot_recv(0).wait_recv()
    with jax.named_scope('q0'):
        queries(0)
    with jax.named_scope('gather0'):
        gathered(0)
    with jax.named_scope('kv0'):
        keys_values(0, 4 * half)
    with jax.named_scope('att0'):
        attention(0, 4 * half)
    with jax.named_scope('part0'):
        project_partner(0)

    def b1_step(n, carry):
        @pl.when(n + 3 < nb_q)
        def _():
            b_copy(n + 3, n + 3).start()
        b_copy(n, n).wait()
        ownb[n] = dq_block(n, x2[...])
        return carry

    with jax.named_scope('qlat1'):
        half_all(core).wait_send()
        for n in range(3):
            b_copy(n, n).start()
        forward(1)
        lax.fori_loop(0, nb_q, b1_step, 0)
        norm_queries(1, mine[1], lambda n: n)
        cq_share(mine[1]).start()
    with jax.named_scope('gather1'):
        gathered(1)
    with jax.named_scope('kv1'):
        keys_values(1, 8 * half)
    with jax.named_scope('q1'):
        cq_share(theirs[1]).wait_recv()
        rot_recv(1).wait_recv()
        queries(1)
    with jax.named_scope('att1'):
        attention(1, 8 * half)
    with jax.named_scope('part1'):
        project_partner(1)

    def own_body(j, carry):
        L = 2 * nblk + j
        wo_next(L)
        ownb[j] = project_here(1, L) + project_there(1, L)
        give_back(0, j, project_here(0, L) + project_there(0, L))
        return carry

    with jax.named_scope('own'):
        lax.fori_loop(0, nblk, own_body, 0)

    def ret_body(j, carry):
        give_back(1, j, ownb[j])
        return carry

    with jax.named_scope('ret'):
        lax.fori_loop(0, nblk, ret_body, 0)

    with jax.named_scope('drain'):
        for q in range(nblk // GROUP):
            part_group(1, q).wait_send()
        result_copy(y_ref.at[:, y_cols(tp, 0, own_cols)]).wait_send()
        result_copy(y_ref.at[:, y_cols(1 - tp, 0, own_cols)]).wait_recv()
    for slot, piece in ((0, pieces[0]), (1, pieces[0]), (2, pieces[1]), (3, pieces[1]), (4, far[0]), (5, far[1])):
        lat_send(piece, slot, dpeer).wait_send()
    x_share(mine[0]).wait_send()
    cq_share(mine[1]).wait_send()
    for hf in range(2):
        rot_send(hf).wait_send()
        o_all(hf).wait_send()


def solution(mesh):
    tok_spec = P(('dp', 'ctx'), None)
    pos_spec = P(('dp', 'ctx'))
    full_mat = P(None, None)
    full_vec = P(None)
    col_spec = P(None, 'tp')
    row_spec = P('tp', None)

    def local_step(tok_x, tok_pos, w_dq, g_q, w_uq, w_qr, w_dkv, g_kv, w_kr, w_uk, w_uv, w_o):
        rows, D = tok_x.shape
        half = rows // 2
        QR = w_dq.shape[1]
        LR = w_dkv.shape[1]
        HL = w_qr.shape[1] // w_kr.shape[1]
        scale = (128 + w_kr.shape[1]) ** -0.5
        nblk = D // 2 // NBLK
        ngrp = HL // 8
        ntok = 8 * half
        dims = (D, QR, LR, HL, half, scale)
        anyspec = pl.BlockSpec(memory_space=pl.ANY)
        vspec = pl.BlockSpec(memory_space=pltpu.VMEM)
        dma = pltpu.SemaphoreType.DMA
        arena_rows = max(DQ_SLOTS * D, WO_SLOTS * HL * 128)
        return pl.pallas_call(
            functools.partial(layer_kernel, dims),
            out_shape=pltpu.VMEM((rows, D), BF16),
            in_specs=[anyspec, anyspec, anyspec, anyspec, anyspec, anyspec, anyspec, anyspec, anyspec, anyspec, anyspec, anyspec],
            out_specs=vspec,
            scratch_shapes=[
                pltpu.VMEM((2, half), jnp.int32),
                pltpu.VMEM((QR // 128, 128), BF16),
                pltpu.VMEM((LR // 128, 128), BF16),
                pltpu.VMEM((rows, D), BF16),
                pltpu.VMEM((half, D), BF16),
                pltpu.VMEM((max(D, 2 * ngrp * ntok), LR), BF16),
                pltpu.VMEM((64, D), BF16),
                pltpu.VMEM((2 * ngrp, LR, 512), BF16),
                pltpu.VMEM((arena_rows, NBLK), BF16),
                pltpu.VMEM((ntok, LR + 128), BF16),
                pltpu.VMEM((ntok, 128), BF16),
                pltpu.VMEM((ntok, 128), BF16),
                pltpu.VMEM((2, rows, QR), BF16),
                pltpu.VMEM((half, LR), F32),
                pltpu.VMEM((half, 64), F32),
                pltpu.VMEM((2, rows, 256), F32),
                pltpu.VMEM((RING, QR, 512), BF16),
                pltpu.VMEM((RING, QR, 256), BF16),
                pltpu.VMEM((rows, HL * 64), BF16),
                pltpu.VMEM((rows, HL * 32), BF16),
                pltpu.VMEM((2, rows, HL * 64), BF16),
                pltpu.VMEM((2, half, HL * 64), BF16),
                pltpu.VMEM((nblk, half, NBLK), F32),
                pltpu.VMEM((2 * nblk, half, NBLK), F32),
                pltpu.VMEM((max(nblk, 2 * QR // NBLK), half, NBLK), F32),
                dma((3,)), dma((KCH,)), dma((1,)), dma((1,)), dma((1,)), dma((KCH,)), dma((KCH,)), dma((DQ_SLOTS,)), dma((RING, 2)), dma((ngrp, 2)), dma((WO_SLOTS,)),
                dma((6,)), dma((8,)), dma((1,)), dma((1,)), dma((1,)), dma((1,)), dma((2,)), dma((2,)), dma((2,)), dma((2,)),
                dma((2, nblk // GROUP)), dma((2, nblk // GROUP)), dma((1,)), dma((1,)),
            ],
            compiler_params=pltpu.CompilerParams(collective_id=0, has_side_effects=True,
                                                 vmem_limit_bytes=62500 * 1000),
        )(tok_x, tok_pos.reshape(2, half), w_dq, g_q.reshape(QR // 128, 128), w_uq, w_qr, w_dkv, g_kv.reshape(LR // 128, 128), w_kr.T,
          w_uk, w_uv, w_o)

    return jax.shard_map(local_step, mesh=mesh,
                         in_specs=(tok_spec, pos_spec, full_mat, full_vec, col_spec, col_spec, full_mat, full_vec, full_mat, col_spec, col_spec, row_spec),
                         out_specs=tok_spec, check_vma=False)
```

```python
import functools

import jax
import jax.numpy as jnp
from jax import lax
from jax.experimental import pallas as pl
from jax.experimental.pallas import tpu as pltpu
from jax.sharding import PartitionSpec as P

ROPE_BASE = 10000.0
NORM_EPS = 1e-6
NEG_BIG = -1e30
MESH = pl.DeviceIdType.MESH
F32 = jnp.float32
BF16 = jnp.bfloat16

KCH = 6
NBLK = 256
RING = 4
DQ_SLOTS = 4
GROUP = 4
WO_SLOTS = 6


def _dot(a, b):
    return jnp.dot(a, b, preferred_element_type=F32)


def _dot_nt(a, b):
    return lax.dot_general(a, b, (((1,), (1,)), ((), ())), preferred_element_type=F32)


def layer_kernel(dims, x_hbm, pos_hbm, wdq_hbm, gq_hbm, wuq_hbm, wqr_hbm, wdkv_hbm, gkv_hbm, wkr_hbm, wuk_hbm, wuv_hbm,
                 wo_hbm, y_ref,
                 pos_ref, gq_ref, gkv_ref, xc, x2, kvs, wkr, upw, arena, lat, kplo, kphi, cq, acckv, acckr, rot,
                 uqb, qrb, qn, qp, os, orx, sendb, recvb, ownb,
                 smsem, xsem, x2sem, xps, xpr, kvsem, krsem, bsem, qsem, upsem, wosem, lats, latr, cqs, cqr, hs, hr, rots, rotr, oss, osr, ps, pr, rs, rr):
    D, QR, LR, HL, half, score_scale = dims
    HC = HL // 2
    ngrp = HC // 4
    kc = D // KCH
    nb_q = QR // NBLK
    own_cols = D // 2
    nblk = own_cols // NBLK
    hv = HL * 128
    ntok = 8 * half
    tp = lax.axis_index("tp")
    ci = lax.axis_index("ctx")
    core = lax.rem(ci, 2)
    xpeer = lax.rem(ci + 2, 4)
    dpeer = ci + 1 - 2 * core
    pieces = (ci, 7 - ci)
    pair = lax.div(ci, 2)
    mine = tuple(pl.ds(pl.multiple_of(sl * half, half), half) for sl in (core, 1 - core))
    theirs = tuple(pl.ds(pl.multiple_of(sl * half, half), half) for sl in (1 - core, core))
    first_pos = (2 * half * lax.div(ci, 2), half * (6 - 2 * lax.div(ci, 2)))
    half_rows = (slice(0, half), slice(half, 2 * half))

    def x_copy(k):
        cols = pl.ds(pl.multiple_of(k * kc, 128), kc)
        return pltpu.make_async_copy(x_hbm.at[pl.ds(0, half), cols], xc.at[mine[0], cols], xsem.at[k])

    def x2_copy():
        return pltpu.make_async_copy(x_hbm.at[pl.ds(half, half), :], x2, x2sem.at[0])

    def x_share(rows):
        return pltpu.make_async_remote_copy(src_ref=x_hbm.at[pl.ds(0, half), :], dst_ref=xc.at[rows, :], send_sem=xps.at[0],
                                            recv_sem=xpr.at[0], device_id={"ctx": dpeer}, device_id_type=MESH)

    def a_copies(k):
        col = pl.multiple_of(k * kc, 128)
        return (pltpu.make_async_copy(wkr_hbm.at[:, pl.ds(col, kc)], wkr.at[:, pl.ds(col, kc)], krsem.at[k]),
                pltpu.make_async_copy(wdkv_hbm.at[pl.ds(col, kc), :], kvs.at[pl.ds(col, kc), :], kvsem.at[k]))

    def b_copy(m, n):
        s = lax.rem(m, DQ_SLOTS)
        return pltpu.make_async_copy(wdq_hbm.at[:, pl.ds(pl.multiple_of(n * NBLK, NBLK), NBLK)],
                                     arena.at[pl.ds(pl.multiple_of(s * D, D), D), :], bsem.at[s])

    def q_copies(g):
        i = lax.rem(g, ngrp) + core * ngrp
        s = lax.rem(g, RING)
        c4 = pl.ds(pl.multiple_of(i * 512, 512), 512)
        c2 = pl.ds(pl.multiple_of(i * 256, 256), 256)
        return (pltpu.make_async_copy(wuq_hbm.at[:, c4], uqb.at[s], qsem.at[s, 0]),
                pltpu.make_async_copy(wqr_hbm.at[:, c2], qrb.at[s], qsem.at[s, 1]))

    def up_copies(i):
        c4 = pl.ds(pl.multiple_of((i + core * ngrp) * 512, 512), 512)
        return (pltpu.make_async_copy(wuk_hbm.at[:, c4], upw.at[i], upsem.at[i, 0]),
                pltpu.make_async_copy(wuv_hbm.at[:, c4], upw.at[ngrp + i], upsem.at[i, 1]))

    def wo_copy(L):
        j = lax.rem(L, nblk)
        side = jnp.where(L < 2 * nblk, 1 - tp, tp)
        s = lax.rem(L, WO_SLOTS)
        col = pl.multiple_of(side * own_cols + j * NBLK, NBLK)
        return pltpu.make_async_copy(wo_hbm.at[:, pl.ds(col, NBLK)],
                                     arena.at[pl.ds(pl.multiple_of(s * hv, hv), hv), :], wosem.at[s])

    def start(cps):
        for c in cps:
            c.start()

    def wait(cps):
        for c in cps:
            c.wait()

    bar = pltpu.get_barrier_semaphore()
    for dev in ({"ctx": xpeer}, {"tp": 1 - tp}, {"ctx": dpeer}):
        pl.semaphore_signal(bar, inc=1, device_id=dev, device_id_type=MESH)

    small = (pltpu.make_async_copy(pos_hbm, pos_ref, smsem.at[0]), pltpu.make_async_copy(gkv_hbm, gkv_ref, smsem.at[1]),
             pltpu.make_async_copy(gq_hbm, gq_ref, smsem.at[2]))
    start(small)
    for k in range(KCH):
        x_copy(k).start()
        start(a_copies(k))

    lane = lax.broadcasted_iota(jnp.int32, (1, 128), 1)
    first_half = lax.rem(lane, 64) < 32

    def rotary(hf):
        fidx = lax.rem(lane, 32)
        freq = jnp.zeros((1, 128), F32)
        for j in range(32):
            freq = jnp.where(fidx == j, ROPE_BASE ** (-j * 2.0 / 64), freq)
        eye = (lax.broadcasted_iota(jnp.int32, (half, half), 0) == lax.broadcasted_iota(jnp.int32, (half, half), 1))
        prow = pos_ref[hf:hf + 1, :].astype(F32)
        pcol = jnp.sum(jnp.where(eye, jnp.broadcast_to(prow, (half, half)), 0.0), axis=1, keepdims=True)
        ang = pcol * freq
        rot[hf, mine[hf], 0:128] = jnp.cos(ang)
        sn = jnp.sin(ang)
        rot[hf, mine[hf], 128:256] = jnp.where(first_half, -sn, sn)

    def turn(a, table):
        swapped = jnp.where(first_half, pltpu.roll(a, 96, 1), pltpu.roll(a, 32, 1))
        return a * table[:, 0:128] + swapped * table[:, 128:256]

    def to_core(ref, ssem, rsem):
        return pltpu.make_async_remote_copy(src_ref=ref, dst_ref=ref, send_sem=ssem, recv_sem=rsem,
                                            device_id={"ctx": dpeer}, device_id_type=MESH)

    def rot_send(hf):
        return to_core(rot.at[hf, mine[hf], :], rots.at[hf], rotr.at[hf])

    def rot_recv(hf):
        return to_core(rot.at[hf, theirs[hf], :], rots.at[hf], rotr.at[hf])

    def lat_send(piece, slot, dev):
        ref = lat.at[pl.ds(pl.multiple_of(piece * half, half), half), :]
        return pltpu.make_async_remote_copy(src_ref=ref, dst_ref=ref, send_sem=lats.at[slot], recv_sem=latr.at[piece],
                                            device_id={"ctx": dev}, device_id_type=MESH)

    def lat_finish(hf, a, kr):
        inv = lax.rsqrt(jnp.mean(a * a, axis=-1, keepdims=True) + NORM_EPS)
        kr2 = turn(jnp.concatenate([kr, kr], axis=1), rot[hf, mine[hf], :])
        row0 = pl.multiple_of(pieces[hf] * half, half)
        for c in range(LR // 128):
            cols = slice(c * 128, (c + 1) * 128)
            lat[pl.ds(row0, half), cols] = (a[:, cols] * inv * gkv_ref[c:c + 1, :].astype(F32)).astype(BF16)
        lat[pl.ds(row0, half), LR:LR + 128] = kr2.astype(BF16)

    def lat_share(hf):
        lat_send(pieces[hf], 2 * hf, xpeer).start()
        lat_send(pieces[hf], 2 * hf + 1, dpeer).start()

    far = (xpeer, 7 - xpeer)
    near = (dpeer, 7 - dpeer)
    relayed = (3 - ci, 4 + ci)

    def lat_recv(piece):
        lat_send(piece, 0, dpeer).wait_recv()

    def forward(hf):
        lat_recv(far[hf])
        lat_send(far[hf], 4 + hf, dpeer).start()

    def split_rope(lo, hi):
        rows = slice(lo, hi)
        kp = lat[rows, LR:LR + 128].astype(F32)
        low = lane < 64
        kplo[rows, :] = jnp.where(low, kp, 0.0).astype(BF16)
        kphi[rows, :] = jnp.where(low, 0.0, kp).astype(BF16)

    nb_c = nb_q // 2

    def half_send(m):
        ref = ownb.at[pl.ds(2 * (core * nb_c + m), 2)]
        return to_core(ref, hs.at[0], hr.at[0])

    def half_all(side):
        ref = ownb.at[pl.ds(2 * side * nb_c, 2 * nb_c)]
        return to_core(ref, hs.at[0], hr.at[0])

    def norm_queries(chunk, rows, block):
        sq = 0.0
        for n in range(nb_q):
            a = ownb[block(n)]
            sq = sq + jnp.sum(a * a, axis=-1, keepdims=True)
        inv = lax.rsqrt(sq * (1.0 / QR) + NORM_EPS)
        for n in range(nb_q):
            a = ownb[block(n)] * inv
            for u in range(NBLK // 128):
                c = n * (NBLK // 128) + u
                cq[chunk, rows, c * 128:(c + 1) * 128] = (
                    a[:, u * 128:(u + 1) * 128] * gq_ref[c:c + 1, :].astype(F32)).astype(BF16)

    def cq_share(rows):
        return to_core(cq.at[1, rows, :], cqs.at[0], cqr.at[0])

    def queries(chunk):
        def body(t, carry):
            if chunk == 0:
                @pl.when(jnp.logical_and(t == 1, pair == 1))
                def _():
                    forward(0)
            gs = [2 * t + u + chunk * ngrp for u in range(2)]
            for g in gs:
                wait(q_copies(g))
            c = cq[chunk]
            for u in range(2):
                i = 2 * t + u
                s = lax.rem(gs[u], RING)
                r = _dot(c, qrb[s])
                qn[:, pl.ds(pl.multiple_of(i * 512, 512), 512)] = _dot(c, uqb[s]).astype(BF16)
                for v in range(2):
                    qp[:, pl.ds(pl.multiple_of(i * 256 + v * 128, 128), 128)] = turn(
                        r[:, v * 128:(v + 1) * 128], rot[chunk]).astype(BF16)
            for g in gs:
                @pl.when(g + RING < 2 * ngrp)
                def _():
                    start(q_copies(g + RING))
            return carry

        lax.fori_loop(0, ngrp // 2, body, 0)

    def kv_rows(i, n):
        return pl.ds(pl.multiple_of(i * ntok, ntok), n)

    def keys_values(chunk, nk):
        per = 2 if chunk == 0 else 1

        def body(t, carry):
            if chunk == 0:
                for u in range(per):
                    wait(up_copies(per * t + u))
            lt = lat[0:nk, 0:LR]
            for u in range(per):
                i = per * t + u
                kvs[kv_rows(i, nk), :] = _dot(lt, upw[i]).astype(BF16)
                kvs[kv_rows(ngrp + i, nk), :] = _dot(lt, upw[ngrp + i]).astype(BF16)
            return carry

        lax.fori_loop(0, ngrp // per, body, 0)

    c2e = score_scale * 1.4426950408889634

    def o_send(chunk, i):
        cols = pl.ds(pl.multiple_of(i * 512, 512), 512)
        return pltpu.make_async_remote_copy(src_ref=os.at[chunk, theirs[chunk], cols], dst_ref=orx.at[chunk, :, cols],
                                            send_sem=oss.at[chunk], recv_sem=osr.at[chunk],
                                            device_id={"ctx": dpeer}, device_id_type=MESH)

    def attention(chunk, nk, clear):
        nq = 2 * half

        def body(i, carry):
            wo_copy(chunk * nblk + i).start()

            @pl.when(i == ngrp - 1)
            def _():
                for extra in range(ngrp, WO_SLOTS - 1):
                    wo_copy(chunk * nblk + extra).start()
            vis = (lax.broadcasted_iota(jnp.int32, (nq, nk - clear), 1)
                   <= lax.broadcasted_iota(jnp.int32, (nq, nk - clear), 0) + (first_pos[chunk] - clear))

            def scores(h):
                kp = kphi if h % 2 else kplo
                qpe = qp[:, pl.ds(pl.multiple_of(i * 256 + (h // 2) * 128, 128), 128)]
                qh = jnp.concatenate([qn[:, pl.ds(pl.multiple_of(i * 512 + h * 128, 128), 128)], qpe], axis=1)
                kh = jnp.concatenate([kvs[kv_rows(i, nk), h * 128:(h + 1) * 128], kp[0:nk, :]], axis=1)
                return _dot_nt(qh, kh)

            def values(h, sc):
                late = jnp.where(vis, sc[:, clear:], NEG_BIG)
                sc = jnp.concatenate([sc[:, :clear], late], axis=1) if clear else late
                top = jnp.max(sc, axis=1, keepdims=True)
                p = jnp.exp2((sc - top) * c2e)
                tot = jnp.sum(p, axis=1, keepdims=True)
                acc = _dot(p.astype(BF16), kvs[kv_rows(ngrp + i, nk), h * 128:(h + 1) * 128])
                os[chunk, :, pl.ds(pl.multiple_of(i * 512 + h * 128, 128), 128)] = (acc / tot).astype(BF16)

            sc = scores(0)
            for h in range(4):
                nxt = scores(h + 1) if h < 3 else None
                values(h, sc)
                sc = nxt
            o_send(chunk, i).start()
            return carry

        lax.fori_loop(0, ngrp, body, 0)

    def o_all(chunk):
        return pltpu.make_async_remote_copy(src_ref=os.at[chunk, theirs[chunk], :], dst_ref=orx.at[chunk],
                                            send_sem=oss.at[chunk], recv_sem=osr.at[chunk],
                                            device_id={"ctx": dpeer}, device_id_type=MESH)

    total_wo = 3 * nblk
    ahead = WO_SLOTS - 1
    hc = HC * 128

    def wo_next(L):
        wo_copy(L).wait()
        wo_refill(L)

    def wo_refill(L):
        @pl.when(jnp.logical_and(L + ahead < total_wo, jnp.logical_or(L >= nblk, L + ahead < nblk)))
        def _():
            wo_copy(L + ahead).start()

    def project_here(chunk, L):
        w = arena[pl.ds(pl.multiple_of(lax.rem(L, WO_SLOTS) * hv + core * hc, hc), hc), :]
        return _dot(os[chunk, mine[chunk], :], w)

    def project_there(chunk, L):
        w = arena[pl.ds(pl.multiple_of(lax.rem(L, WO_SLOTS) * hv + (1 - core) * hc, hc), hc), :]
        return _dot(orx[chunk], w)

    def part_copy(chunk, q, src, dst):
        return pltpu.make_async_remote_copy(src_ref=src, dst_ref=dst, send_sem=ps.at[chunk, q], recv_sem=pr.at[chunk, q],
                                            device_id={"tp": 1 - tp}, device_id_type=MESH)

    def part_send(chunk, j):
        return part_copy(chunk, lax.div(j, GROUP), sendb.at[j], recvb.at[chunk * nblk + j])

    def part_group(chunk, q):
        return part_copy(chunk, q, sendb.at[pl.ds(q * GROUP, GROUP)], recvb.at[pl.ds(chunk * nblk + q * GROUP, GROUP)])

    def project_partner(chunk):
        early = 2
        base = chunk * nblk

        def send_slot(j):
            if chunk == 1:
                @pl.when(lax.rem(j, GROUP) == 0)
                def _():
                    part_group(0, lax.div(j, GROUP)).wait_send()

        for j in range(early):
            wo_copy(base + j).wait()
            if j == 0:
                wo_refill(base)
            send_slot(j)
            sendb[j] = project_here(chunk, base + j)
        o_all(chunk).wait_recv()
        for j in range(early):
            sendb[j] += project_there(chunk, base + j)
            part_send(chunk, j).start()
            if j + 1 < early:
                wo_refill(base + j + 1)

        def body(j, carry):
            wo_next(base + j)
            send_slot(j)
            sendb[j] = project_here(chunk, base + j) + project_there(chunk, base + j)
            part_send(chunk, j).start()
            return carry

        lax.fori_loop(early, nblk, body, 0)

    def y_cols(side, j, n):
        return pl.ds(pl.multiple_of(side * own_cols + j * NBLK, NBLK), n)

    def result_copy(ref):
        return pltpu.make_async_remote_copy(src_ref=ref, dst_ref=ref, send_sem=rs.at[0], recv_sem=rr.at[0],
                                            device_id={"tp": 1 - tp}, device_id_type=MESH)

    def give_back(chunk, j, own):
        @pl.when(lax.rem(j, GROUP) == 0)
        def _():
            part_group(chunk, lax.div(j, GROUP)).wait_recv()
        cols = y_cols(tp, j, NBLK)
        y_ref[half_rows[chunk], cols] = (recvb[chunk * nblk + j] + own).astype(BF16)

        @pl.when(lax.rem(j, GROUP) == GROUP - 1)
        def _():
            result_copy(y_ref.at[half_rows[chunk], y_cols(tp, j - (GROUP - 1), GROUP * NBLK)]).start()

    acckv[...] = jnp.zeros_like(acckv)
    acckr[...] = jnp.zeros_like(acckr)
    def a_step(k, carry):
        x_copy(k).wait()
        wait(a_copies(k))

        @pl.when(k == 3)
        def _():
            wait(small)
            rotary(0)

        @pl.when(jnp.logical_and(lax.rem(k, 2) == 0, k < 2 * nb_c - 2))
        def _():
            m = lax.div(k, 2) + 1
            b_copy(m, core * nb_c + m).start()

        @pl.when(k == KCH - 1)
        def _():
            start(q_copies(0))
        cols = pl.ds(pl.multiple_of(k * kc, 128), kc)
        xk = xc[mine[0], cols]
        acckv[...] += _dot(xk, kvs[cols, :])
        acckr[...] += _dot_nt(xk, wkr[:, cols])
        return carry

    b_copy(0, core * nb_c).start()
    pl.semaphore_wait(bar, 3)
    x_share(mine[0]).start()
    with jax.named_scope('lat0'):
        lax.fori_loop(0, KCH, a_step, 0)
        x2_copy().start()
        lat_finish(0, acckv[...], acckr[...])
        lat_share(0)
        rot_send(0).start()
    with jax.named_scope('xwait'):
        x_share(theirs[0]).wait_recv()

    def dq_block(m, rows):
        return _dot(rows, arena[pl.ds(pl.multiple_of(lax.rem(m, DQ_SLOTS) * D, D), D), :])

    def b_step(m, carry):
        n = core * nb_c + m
        b_copy(m, n).wait()
        start(q_copies(m + 1))
        r = dq_block(m, xc[...])
        ownb[2 * n] = r[:half]
        ownb[2 * n + 1] = r[half:]
        half_send(m).start()
        return carry

    with jax.named_scope('qlat0'):
        lax.fori_loop(0, nb_c, b_step, 0)
        for m in range(nb_c + 1, RING):
            start(q_copies(m))
        for i in range(ngrp):
            start(up_copies(i))
    with jax.named_scope('lat1'):
        x2_copy().wait()
        acckv[...] = _dot(x2[...], kvs[0:D, :])
    with jax.named_scope('qfin0'):
        half_all(1 - core).wait_recv()
        for sl in range(2):
            norm_queries(0, half_rows[sl], lambda n, sl=sl: 2 * n + sl)
        rot_recv(0).wait_recv()
    with jax.named_scope('q0'):
        queries(0)
    for which in range(2):
        @pl.when(pair == which)
        def _():
            nk = 2 * half * (which + 1)
            with jax.named_scope('gather0'):
                lat_recv(near[0])
                if which == 1:
                    lat_recv(relayed[0])
                split_rope(0, nk)
            with jax.named_scope('kv0'):
                keys_values(0, nk)
            with jax.named_scope('att0'):
                attention(0, nk, nk - 2 * half)
    with jax.named_scope('part0'):
        project_partner(0)

    def b1_step(n, carry):
        @pl.when(n + 3 < nb_q)
        def _():
            b_copy(n + 3, n + 3).start()
        b_copy(n, n).wait()
        ownb[n] = dq_block(n, x2[...])
        return carry

    with jax.named_scope('qlat1'):
        half_all(core).wait_send()
        for n in range(3):
            b_copy(n, n).start()
        rotary(1)
        rot_send(1).start()
        lat_finish(1, acckv[...], _dot_nt(x2[...], wkr[...]))
        lat_share(1)
        lax.fori_loop(0, nb_q, b1_step, 0)
        norm_queries(1, mine[1], lambda n: n)
        cq_share(mine[1]).start()
    with jax.named_scope('gather1'):
        forward(1)

        @pl.when(pair == 0)
        def _():
            forward(0)
            lat_recv(relayed[0])
            split_rope(2 * half, 4 * half)
        lat_recv(near[1])
        lat_recv(relayed[1])
        split_rope(4 * half, 8 * half)
    with jax.named_scope('kv1'):
        keys_values(1, 8 * half)
    with jax.named_scope('q1'):
        cq_share(theirs[1]).wait_recv()
        rot_recv(1).wait_recv()
        queries(1)
    with jax.named_scope('att1'):
        attention(1, 8 * half, 4 * half)
    with jax.named_scope('part1'):
        project_partner(1)

    def own_body(j, carry):
        L = 2 * nblk + j
        wo_next(L)
        ownb[j] = project_here(1, L) + project_there(1, L)
        give_back(0, j, project_here(0, L) + project_there(0, L))
        return carry

    with jax.named_scope('own'):
        lax.fori_loop(0, nblk, own_body, 0)

    def ret_body(j, carry):
        give_back(1, j, ownb[j])
        return carry

    with jax.named_scope('ret'):
        lax.fori_loop(0, nblk, ret_body, 0)

    with jax.named_scope('drain'):
        for q in range(nblk // GROUP):
            part_group(1, q).wait_send()
        result_copy(y_ref.at[:, y_cols(tp, 0, own_cols)]).wait_send()
        result_copy(y_ref.at[:, y_cols(1 - tp, 0, own_cols)]).wait_recv()
    for slot, piece in ((0, pieces[0]), (1, pieces[0]), (2, pieces[1]), (3, pieces[1]), (4, far[0]), (5, far[1])):
        lat_send(piece, slot, dpeer).wait_send()
    x_share(mine[0]).wait_send()
    cq_share(mine[1]).wait_send()
    for hf in range(2):
        rot_send(hf).wait_send()
        o_all(hf).wait_send()


def solution(mesh):
    tok_spec = P(('dp', 'ctx'), None)
    pos_spec = P(('dp', 'ctx'))
    full_mat = P(None, None)
    full_vec = P(None)
    col_spec = P(None, 'tp')
    row_spec = P('tp', None)

    def local_step(tok_x, tok_pos, w_dq, g_q, w_uq, w_qr, w_dkv, g_kv, w_kr, w_uk, w_uv, w_o):
        rows, D = tok_x.shape
        half = rows // 2
        QR = w_dq.shape[1]
        LR = w_dkv.shape[1]
        HL = w_qr.shape[1] // w_kr.shape[1]
        scale = (128 + w_kr.shape[1]) ** -0.5
        nblk = D // 2 // NBLK
        ngrp = HL // 8
        ntok = 8 * half
        dims = (D, QR, LR, HL, half, scale)
        anyspec = pl.BlockSpec(memory_space=pl.ANY)
        vspec = pl.BlockSpec(memory_space=pltpu.VMEM)
        dma = pltpu.SemaphoreType.DMA
        arena_rows = max(DQ_SLOTS * D, WO_SLOTS * HL * 128)
        return pl.pallas_call(
            functools.partial(layer_kernel, dims),
            out_shape=pltpu.VMEM((rows, D), BF16),
            in_specs=[anyspec, anyspec, anyspec, anyspec, anyspec, anyspec, anyspec, anyspec, anyspec, anyspec, anyspec, anyspec],
            out_specs=vspec,
            scratch_shapes=[
                pltpu.VMEM((2, half), jnp.int32),
                pltpu.VMEM((QR // 128, 128), BF16),
                pltpu.VMEM((LR // 128, 128), BF16),
                pltpu.VMEM((rows, D), BF16),
                pltpu.VMEM((half, D), BF16),
                pltpu.VMEM((max(D, 2 * ngrp * ntok), LR), BF16),
                pltpu.VMEM((64, D), BF16),
                pltpu.VMEM((2 * ngrp, LR, 512), BF16),
                pltpu.VMEM((arena_rows, NBLK), BF16),
                pltpu.VMEM((ntok, LR + 128), BF16),
                pltpu.VMEM((ntok, 128), BF16),
                pltpu.VMEM((ntok, 128), BF16),
                pltpu.VMEM((2, rows, QR), BF16),
                pltpu.VMEM((half, LR), F32),
                pltpu.VMEM((half, 64), F32),
                pltpu.VMEM((2, rows, 256), F32),
                pltpu.VMEM((RING, QR, 512), BF16),
                pltpu.VMEM((RING, QR, 256), BF16),
                pltpu.VMEM((rows, HL * 64), BF16),
                pltpu.VMEM((rows, HL * 32), BF16),
                pltpu.VMEM((2, rows, HL * 64), BF16),
                pltpu.VMEM((2, half, HL * 64), BF16),
                pltpu.VMEM((nblk, half, NBLK), F32),
                pltpu.VMEM((2 * nblk, half, NBLK), F32),
                pltpu.VMEM((max(nblk, 2 * QR // NBLK), half, NBLK), F32),
                dma((3,)), dma((KCH,)), dma((1,)), dma((1,)), dma((1,)), dma((KCH,)), dma((KCH,)), dma((DQ_SLOTS,)), dma((RING, 2)), dma((ngrp, 2)), dma((WO_SLOTS,)),
                dma((6,)), dma((8,)), dma((1,)), dma((1,)), dma((1,)), dma((1,)), dma((2,)), dma((2,)), dma((2,)), dma((2,)),
                dma((2, nblk // GROUP)), dma((2, nblk // GROUP)), dma((1,)), dma((1,)),
            ],
            compiler_params=pltpu.CompilerParams(collective_id=0, has_side_effects=True,
                                                 vmem_limit_bytes=62500 * 1000),
        )(tok_x, tok_pos.reshape(2, half), w_dq, g_q.reshape(QR // 128, 128), w_uq, w_qr, w_dkv, g_kv.reshape(LR // 128, 128), w_kr.T,
          w_uk, w_uv, w_o)

    return jax.shard_map(local_step, mesh=mesh,
                         in_specs=(tok_spec, pos_spec, full_mat, full_vec, col_spec, col_spec, full_mat, full_vec, full_mat, col_spec, col_spec, row_spec),
                         out_specs=tok_spec, check_vma=False)
```

```python
import functools

import jax
import jax.numpy as jnp
from jax import lax
from jax.experimental import pallas as pl
from jax.experimental.pallas import tpu as pltpu
from jax.sharding import PartitionSpec as P

ROPE_BASE = 10000.0
NORM_EPS = 1e-6
NEG_BIG = -1e30
MESH = pl.DeviceIdType.MESH
F32 = jnp.float32
BF16 = jnp.bfloat16

KCH = 6
NBLK = 256
RING = 4
DQ_SLOTS = 4
GROUP = 4
UNROLL = 4
WO_SLOTS = 6


def _dot(a, b):
    return jnp.dot(a, b, preferred_element_type=F32)


def _dot_nt(a, b):
    return lax.dot_general(a, b, (((1,), (1,)), ((), ())), preferred_element_type=F32)


def layer_kernel(dims, x_hbm, pos_hbm, wdq_hbm, gq_hbm, wuq_hbm, wqr_hbm, wdkv_hbm, gkv_hbm, wkr_hbm, wuk_hbm, wuv_hbm,
                 wo_hbm, y_ref,
                 pos_ref, gq_ref, gkv_ref, xc, x2, kvs, wkr, upw, arena, lat, kplo, kphi, cq, acckv, acckr, rot,
                 uqb, qrb, qn, qp, os, orx, sendb, recvb, ownb,
                 smsem, xsem, x2sem, xps, xpr, kvsem, krsem, bsem, qsem, upsem, wosem, lats, latr, cqs, cqr, hs, hr, rots, rotr, oss, osr, ps, pr, rs, rr):
    D, QR, LR, HL, half, score_scale = dims
    HC = HL // 2
    ngrp = HC // 4
    kc = D // KCH
    nb_q = QR // NBLK
    own_cols = D // 2
    nblk = own_cols // NBLK
    hv = HL * 128
    ntok = 8 * half
    tp = lax.axis_index("tp")
    ci = lax.axis_index("ctx")
    core = lax.rem(ci, 2)
    xpeer = lax.rem(ci + 2, 4)
    dpeer = ci + 1 - 2 * core
    pieces = (ci, 7 - ci)
    pair = lax.div(ci, 2)
    mine = tuple(pl.ds(pl.multiple_of(sl * half, half), half) for sl in (core, 1 - core))
    theirs = tuple(pl.ds(pl.multiple_of(sl * half, half), half) for sl in (1 - core, core))
    first_pos = (2 * half * lax.div(ci, 2), half * (6 - 2 * lax.div(ci, 2)))
    half_rows = (slice(0, half), slice(half, 2 * half))

    def x_copy(k):
        cols = pl.ds(pl.multiple_of(k * kc, 128), kc)
        return pltpu.make_async_copy(x_hbm.at[pl.ds(0, half), cols], xc.at[mine[0], cols], xsem.at[k])

    def x2_copy():
        return pltpu.make_async_copy(x_hbm.at[pl.ds(half, half), :], x2, x2sem.at[0])

    def x_share(rows):
        return pltpu.make_async_remote_copy(src_ref=x_hbm.at[pl.ds(0, half), :], dst_ref=xc.at[rows, :], send_sem=xps.at[0],
                                            recv_sem=xpr.at[0], device_id={"ctx": dpeer}, device_id_type=MESH)

    def a_copies(k):
        col = pl.multiple_of(k * kc, 128)
        return (pltpu.make_async_copy(wkr_hbm.at[:, pl.ds(col, kc)], wkr.at[:, pl.ds(col, kc)], krsem.at[k]),
                pltpu.make_async_copy(wdkv_hbm.at[pl.ds(col, kc), :], kvs.at[pl.ds(col, kc), :], kvsem.at[k]))

    def b_copy(m, n):
        s = lax.rem(m, DQ_SLOTS)
        return pltpu.make_async_copy(wdq_hbm.at[:, pl.ds(pl.multiple_of(n * NBLK, NBLK), NBLK)],
                                     arena.at[pl.ds(pl.multiple_of(s * D, D), D), :], bsem.at[s])

    def q_copies(g):
        i = lax.rem(g, ngrp) + core * ngrp
        s = lax.rem(g, RING)
        c4 = pl.ds(pl.multiple_of(i * 512, 512), 512)
        c2 = pl.ds(pl.multiple_of(i * 256, 256), 256)
        return (pltpu.make_async_copy(wuq_hbm.at[:, c4], uqb.at[s], qsem.at[s, 0]),
                pltpu.make_async_copy(wqr_hbm.at[:, c2], qrb.at[s], qsem.at[s, 1]))

    def up_copies(i):
        c4 = pl.ds(pl.multiple_of((i + core * ngrp) * 512, 512), 512)
        return (pltpu.make_async_copy(wuk_hbm.at[:, c4], upw.at[i], upsem.at[i, 0]),
                pltpu.make_async_copy(wuv_hbm.at[:, c4], upw.at[ngrp + i], upsem.at[i, 1]))

    def wo_copy(L):
        j = lax.rem(L, nblk)
        side = jnp.where(L < 2 * nblk, 1 - tp, tp)
        s = lax.rem(L, WO_SLOTS)
        col = pl.multiple_of(side * own_cols + j * NBLK, NBLK)
        return pltpu.make_async_copy(wo_hbm.at[:, pl.ds(col, NBLK)],
                                     arena.at[pl.ds(pl.multiple_of(s * hv, hv), hv), :], wosem.at[s])

    def start(cps):
        for c in cps:
            c.start()

    def wait(cps):
        for c in cps:
            c.wait()

    bar = pltpu.get_barrier_semaphore()
    for dev in ({"ctx": xpeer}, {"tp": 1 - tp}, {"ctx": dpeer}):
        pl.semaphore_signal(bar, inc=1, device_id=dev, device_id_type=MESH)

    small = (pltpu.make_async_copy(pos_hbm, pos_ref, smsem.at[0]), pltpu.make_async_copy(gkv_hbm, gkv_ref, smsem.at[1]),
             pltpu.make_async_copy(gq_hbm, gq_ref, smsem.at[2]))
    start(small)
    for k in range(KCH):
        x_copy(k).start()
        start(a_copies(k))

    lane = lax.broadcasted_iota(jnp.int32, (1, 128), 1)
    first_half = lax.rem(lane, 64) < 32

    def rotary(hf):
        fidx = lax.rem(lane, 32)
        freq = jnp.zeros((1, 128), F32)
        for j in range(32):
            freq = jnp.where(fidx == j, ROPE_BASE ** (-j * 2.0 / 64), freq)
        eye = (lax.broadcasted_iota(jnp.int32, (half, half), 0) == lax.broadcasted_iota(jnp.int32, (half, half), 1))
        prow = pos_ref[hf:hf + 1, :].astype(F32)
        pcol = jnp.sum(jnp.where(eye, jnp.broadcast_to(prow, (half, half)), 0.0), axis=1, keepdims=True)
        ang = pcol * freq
        rot[hf, mine[hf], 0:128] = jnp.cos(ang)
        sn = jnp.sin(ang)
        rot[hf, mine[hf], 128:256] = jnp.where(first_half, -sn, sn)

    def turn(a, table):
        swapped = jnp.where(first_half, pltpu.roll(a, 96, 1), pltpu.roll(a, 32, 1))
        return a * table[:, 0:128] + swapped * table[:, 128:256]

    def to_core(ref, ssem, rsem):
        return pltpu.make_async_remote_copy(src_ref=ref, dst_ref=ref, send_sem=ssem, recv_sem=rsem,
                                            device_id={"ctx": dpeer}, device_id_type=MESH)

    def rot_send(hf):
        return to_core(rot.at[hf, mine[hf], :], rots.at[hf], rotr.at[hf])

    def rot_recv(hf):
        return to_core(rot.at[hf, theirs[hf], :], rots.at[hf], rotr.at[hf])

    def lat_send(piece, slot, dev):
        ref = lat.at[pl.ds(pl.multiple_of(piece * half, half), half), :]
        return pltpu.make_async_remote_copy(src_ref=ref, dst_ref=ref, send_sem=lats.at[slot], recv_sem=latr.at[piece],
                                            device_id={"ctx": dev}, device_id_type=MESH)

    def lat_finish(hf, a, kr):
        inv = lax.rsqrt(jnp.mean(a * a, axis=-1, keepdims=True) + NORM_EPS)
        kr2 = turn(jnp.concatenate([kr, kr], axis=1), rot[hf, mine[hf], :])
        row0 = pl.multiple_of(pieces[hf] * half, half)
        for c in range(LR // 128):
            cols = slice(c * 128, (c + 1) * 128)
            lat[pl.ds(row0, half), cols] = (a[:, cols] * inv * gkv_ref[c:c + 1, :].astype(F32)).astype(BF16)
        lat[pl.ds(row0, half), LR:LR + 128] = kr2.astype(BF16)

    def lat_share(hf):
        lat_send(pieces[hf], 2 * hf, xpeer).start()
        lat_send(pieces[hf], 2 * hf + 1, dpeer).start()

    far = (xpeer, 7 - xpeer)
    near = (dpeer, 7 - dpeer)
    relayed = (3 - ci, 4 + ci)

    def lat_recv(piece):
        lat_send(piece, 0, dpeer).wait_recv()

    def forward(hf):
        lat_recv(far[hf])
        lat_send(far[hf], 4 + hf, dpeer).start()

    def split_rope(lo, hi):
        rows = slice(lo, hi)
        kp = lat[rows, LR:LR + 128].astype(F32)
        low = lane < 64
        kplo[rows, :] = jnp.where(low, kp, 0.0).astype(BF16)
        kphi[rows, :] = jnp.where(low, 0.0, kp).astype(BF16)

    nb_c = nb_q // 2

    def half_send(m):
        ref = ownb.at[pl.ds(2 * (core * nb_c + m), 2)]
        return to_core(ref, hs.at[0], hr.at[0])

    def half_all(side):
        ref = ownb.at[pl.ds(2 * side * nb_c, 2 * nb_c)]
        return to_core(ref, hs.at[0], hr.at[0])

    def norm_queries(chunk, rows, block):
        sq = 0.0
        for n in range(nb_q):
            a = ownb[block(n)]
            sq = sq + jnp.sum(a * a, axis=-1, keepdims=True)
        inv = lax.rsqrt(sq * (1.0 / QR) + NORM_EPS)
        for n in range(nb_q):
            a = ownb[block(n)] * inv
            for u in range(NBLK // 128):
                c = n * (NBLK // 128) + u
                cq[chunk, rows, c * 128:(c + 1) * 128] = (
                    a[:, u * 128:(u + 1) * 128] * gq_ref[c:c + 1, :].astype(F32)).astype(BF16)

    def cq_share(rows):
        return to_core(cq.at[1, rows, :], cqs.at[0], cqr.at[0])

    def queries(chunk):
        def body(t, carry):
            if chunk == 0:
                @pl.when(jnp.logical_and(t == 1, pair == 1))
                def _():
                    forward(0)
            gs = [2 * t + u + chunk * ngrp for u in range(2)]
            for g in gs:
                wait(q_copies(g))
            c = cq[chunk]
            for u in range(2):
                i = 2 * t + u
                s = lax.rem(gs[u], RING)
                r = _dot(c, qrb[s])
                qn[:, pl.ds(pl.multiple_of(i * 512, 512), 512)] = _dot(c, uqb[s]).astype(BF16)
                for v in range(2):
                    qp[:, pl.ds(pl.multiple_of(i * 256 + v * 128, 128), 128)] = turn(
                        r[:, v * 128:(v + 1) * 128], rot[chunk]).astype(BF16)
            for g in gs:
                @pl.when(g + RING < 2 * ngrp)
                def _():
                    start(q_copies(g + RING))
            return carry

        lax.fori_loop(0, ngrp // 2, body, 0)

    def kv_rows(i, n):
        return pl.ds(pl.multiple_of(i * ntok, ntok), n)

    def keys_values(chunk, nk):
        per = ngrp if chunk == 0 else 1

        def body(t, carry):
            if chunk == 0:
                for u in range(per):
                    wait(up_copies(per * t + u))
            lt = lat[0:nk, 0:LR]
            for u in range(per):
                i = per * t + u
                kvs[kv_rows(i, nk), :] = _dot(lt, upw[i]).astype(BF16)
                kvs[kv_rows(ngrp + i, nk), :] = _dot(lt, upw[ngrp + i]).astype(BF16)
            return carry

        lax.fori_loop(0, ngrp // per, body, 0)

    c2e = score_scale * 1.4426950408889634

    def o_send(chunk, i):
        cols = pl.ds(pl.multiple_of(i * 512, 512), 512)
        return pltpu.make_async_remote_copy(src_ref=os.at[chunk, theirs[chunk], cols], dst_ref=orx.at[chunk, :, cols],
                                            send_sem=oss.at[chunk], recv_sem=osr.at[chunk],
                                            device_id={"ctx": dpeer}, device_id_type=MESH)

    def attention(chunk, nk, clear):
        nq = 2 * half

        vis = (lax.broadcasted_iota(jnp.int32, (nq, nk - clear), 1)
               <= lax.broadcasted_iota(jnp.int32, (nq, nk - clear), 0) + (first_pos[chunk] - clear))

        def scores(i, h):
            kp = kphi if h % 2 else kplo
            qpe = qp[:, pl.ds(pl.multiple_of(i * 256 + (h // 2) * 128, 128), 128)]
            qh = jnp.concatenate([qn[:, pl.ds(pl.multiple_of(i * 512 + h * 128, 128), 128)], qpe], axis=1)
            kh = jnp.concatenate([kvs[kv_rows(i, nk), h * 128:(h + 1) * 128], kp[0:nk, :]], axis=1)
            return _dot_nt(qh, kh)

        def values(i, h, sc):
            late = jnp.where(vis, sc[:, clear:], NEG_BIG)
            sc = jnp.concatenate([sc[:, :clear], late], axis=1) if clear else late
            top = jnp.max(sc, axis=1, keepdims=True)
            p = jnp.exp2((sc - top) * c2e)
            tot = jnp.sum(p, axis=1, keepdims=True)
            acc = _dot(p.astype(BF16), kvs[kv_rows(ngrp + i, nk), h * 128:(h + 1) * 128])
            os[chunk, :, pl.ds(pl.multiple_of(i * 512 + h * 128, 128), 128)] = (acc / tot).astype(BF16)

        per = UNROLL if chunk == 0 else 1

        def body(t, carry):
            for u in range(per):
                wo_copy(chunk * nblk + per * t + u).start()

            @pl.when(t == ngrp // per - 1)
            def _():
                for extra in range(ngrp, WO_SLOTS - 1):
                    wo_copy(chunk * nblk + extra).start()
            sc = scores(per * t, 0)
            for u in range(4 * per):
                i, h = per * t + u // 4, u % 4
                nxt = scores(per * t + (u + 1) // 4, (u + 1) % 4) if u + 1 < 4 * per else None
                values(i, h, sc)
                sc = nxt
                if h == 3:
                    o_send(chunk, i).start()
            return carry

        lax.fori_loop(0, ngrp // per, body, 0)

    def o_all(chunk):
        return pltpu.make_async_remote_copy(src_ref=os.at[chunk, theirs[chunk], :], dst_ref=orx.at[chunk],
                                            send_sem=oss.at[chunk], recv_sem=osr.at[chunk],
                                            device_id={"ctx": dpeer}, device_id_type=MESH)

    total_wo = 3 * nblk
    ahead = WO_SLOTS - 1
    hc = HC * 128

    def wo_next(L):
        wo_copy(L).wait()
        wo_refill(L)

    def wo_refill(L):
        @pl.when(jnp.logical_and(L + ahead < total_wo, jnp.logical_or(L >= nblk, L + ahead < nblk)))
        def _():
            wo_copy(L + ahead).start()

    def project_here(chunk, L):
        w = arena[pl.ds(pl.multiple_of(lax.rem(L, WO_SLOTS) * hv + core * hc, hc), hc), :]
        return _dot(os[chunk, mine[chunk], :], w)

    def project_there(chunk, L):
        w = arena[pl.ds(pl.multiple_of(lax.rem(L, WO_SLOTS) * hv + (1 - core) * hc, hc), hc), :]
        return _dot(orx[chunk], w)

    def part_copy(chunk, q, src, dst):
        return pltpu.make_async_remote_copy(src_ref=src, dst_ref=dst, send_sem=ps.at[chunk, q], recv_sem=pr.at[chunk, q],
                                            device_id={"tp": 1 - tp}, device_id_type=MESH)

    def part_send(chunk, j):
        return part_copy(chunk, lax.div(j, GROUP), sendb.at[j], recvb.at[chunk * nblk + j])

    def part_group(chunk, q):
        return part_copy(chunk, q, sendb.at[pl.ds(q * GROUP, GROUP)], recvb.at[pl.ds(chunk * nblk + q * GROUP, GROUP)])

    def project_partner(chunk):
        early = 2
        base = chunk * nblk

        def send_slot(j):
            if chunk == 1:
                @pl.when(lax.rem(j, GROUP) == 0)
                def _():
                    part_group(0, lax.div(j, GROUP)).wait_send()

        for j in range(early):
            wo_copy(base + j).wait()
            if j == 0:
                wo_refill(base)
            send_slot(j)
            sendb[j] = project_here(chunk, base + j)
        o_all(chunk).wait_recv()
        for j in range(early):
            sendb[j] += project_there(chunk, base + j)
            part_send(chunk, j).start()
            if j + 1 < early:
                wo_refill(base + j + 1)

        def body(j, carry):
            wo_next(base + j)
            send_slot(j)
            sendb[j] = project_here(chunk, base + j) + project_there(chunk, base + j)
            part_send(chunk, j).start()
            return carry

        lax.fori_loop(early, nblk, body, 0)

    def y_cols(side, j, n):
        return pl.ds(pl.multiple_of(side * own_cols + j * NBLK, NBLK), n)

    def result_copy(ref):
        return pltpu.make_async_remote_copy(src_ref=ref, dst_ref=ref, send_sem=rs.at[0], recv_sem=rr.at[0],
                                            device_id={"tp": 1 - tp}, device_id_type=MESH)

    def give_back(chunk, j, own):
        @pl.when(lax.rem(j, GROUP) == 0)
        def _():
            part_group(chunk, lax.div(j, GROUP)).wait_recv()
        cols = y_cols(tp, j, NBLK)
        y_ref[half_rows[chunk], cols] = (recvb[chunk * nblk + j] + own).astype(BF16)

        @pl.when(lax.rem(j, GROUP) == GROUP - 1)
        def _():
            result_copy(y_ref.at[half_rows[chunk], y_cols(tp, j - (GROUP - 1), GROUP * NBLK)]).start()

    acckv[...] = jnp.zeros_like(acckv)
    acckr[...] = jnp.zeros_like(acckr)
    def a_step(k, carry):
        x_copy(k).wait()
        wait(a_copies(k))

        @pl.when(k == 3)
        def _():
            wait(small)
            rotary(0)

        @pl.when(jnp.logical_and(lax.rem(k, 2) == 0, k < 2 * nb_c - 2))
        def _():
            m = lax.div(k, 2) + 1
            b_copy(m, core * nb_c + m).start()

        @pl.when(k == KCH - 1)
        def _():
            start(q_copies(0))
        cols = pl.ds(pl.multiple_of(k * kc, 128), kc)
        xk = xc[mine[0], cols]
        acckv[...] += _dot(xk, kvs[cols, :])
        acckr[...] += _dot_nt(xk, wkr[:, cols])
        return carry

    b_copy(0, core * nb_c).start()
    pl.semaphore_wait(bar, 3)
    x_share(mine[0]).start()
    with jax.named_scope('lat0'):
        lax.fori_loop(0, KCH, a_step, 0)
        x2_copy().start()
        lat_finish(0, acckv[...], acckr[...])
        lat_share(0)
        rot_send(0).start()
    with jax.named_scope('xwait'):
        x_share(theirs[0]).wait_recv()

    def dq_block(m, rows):
        return _dot(rows, arena[pl.ds(pl.multiple_of(lax.rem(m, DQ_SLOTS) * D, D), D), :])

    def b_step(m, carry):
        n = core * nb_c + m
        b_copy(m, n).wait()
        start(q_copies(m + 1))
        r = dq_block(m, xc[...])
        ownb[2 * n] = r[:half]
        ownb[2 * n + 1] = r[half:]
        half_send(m).start()
        return carry

    with jax.named_scope('qlat0'):
        lax.fori_loop(0, nb_c, b_step, 0)
        for m in range(nb_c + 1, RING):
            start(q_copies(m))
        for i in range(ngrp):
            start(up_copies(i))
    with jax.named_scope('lat1'):
        x2_copy().wait()
        acckv[...] = _dot(x2[...], kvs[0:D, :])
    with jax.named_scope('qfin0'):
        half_all(1 - core).wait_recv()
        for sl in range(2):
            norm_queries(0, half_rows[sl], lambda n, sl=sl: 2 * n + sl)
        rot_recv(0).wait_recv()
    with jax.named_scope('q0'):
        queries(0)
    for which in range(2):
        @pl.when(pair == which)
        def _():
            nk = 2 * half * (which + 1)
            with jax.named_scope('gather0'):
                lat_recv(near[0])
                if which == 1:
                    lat_recv(relayed[0])
                split_rope(0, nk)
            with jax.named_scope('kv0'):
                keys_values(0, nk)
            with jax.named_scope('att0'):
                attention(0, nk, nk - 2 * half)
    with jax.named_scope('part0'):
        project_partner(0)

    def b1_step(n, carry):
        @pl.when(n + 3 < nb_q)
        def _():
            b_copy(n + 3, n + 3).start()
        b_copy(n, n).wait()
        ownb[n] = dq_block(n, x2[...])
        return carry

    with jax.named_scope('qlat1'):
        half_all(core).wait_send()
        for n in range(3):
            b_copy(n, n).start()
        rotary(1)
        rot_send(1).start()
        lat_finish(1, acckv[...], _dot_nt(x2[...], wkr[...]))
        lat_share(1)
        lax.fori_loop(0, nb_q, b1_step, 0)
        norm_queries(1, mine[1], lambda n: n)
        cq_share(mine[1]).start()
    with jax.named_scope('gather1'):
        forward(1)

        @pl.when(pair == 0)
        def _():
            forward(0)
            lat_recv(relayed[0])
            split_rope(2 * half, 4 * half)
        lat_recv(near[1])
        lat_recv(relayed[1])
        split_rope(4 * half, 8 * half)
    with jax.named_scope('kv1'):
        keys_values(1, 8 * half)
    with jax.named_scope('q1'):
        cq_share(theirs[1]).wait_recv()
        rot_recv(1).wait_recv()
        queries(1)
    with jax.named_scope('att1'):
        attention(1, 8 * half, 4 * half)
    with jax.named_scope('part1'):
        project_partner(1)

    def own_body(j, carry):
        L = 2 * nblk + j
        wo_next(L)
        ownb[j] = project_here(1, L) + project_there(1, L)
        give_back(0, j, project_here(0, L) + project_there(0, L))
        return carry

    with jax.named_scope('own'):
        lax.fori_loop(0, nblk, own_body, 0)

    def ret_body(j, carry):
        give_back(1, j, ownb[j])
        return carry

    with jax.named_scope('ret'):
        lax.fori_loop(0, nblk, ret_body, 0)

    with jax.named_scope('drain'):
        for q in range(nblk // GROUP):
            part_group(1, q).wait_send()
        result_copy(y_ref.at[:, y_cols(tp, 0, own_cols)]).wait_send()
        result_copy(y_ref.at[:, y_cols(1 - tp, 0, own_cols)]).wait_recv()
    for slot, piece in ((0, pieces[0]), (1, pieces[0]), (2, pieces[1]), (3, pieces[1]), (4, far[0]), (5, far[1])):
        lat_send(piece, slot, dpeer).wait_send()
    x_share(mine[0]).wait_send()
    cq_share(mine[1]).wait_send()
    for hf in range(2):
        rot_send(hf).wait_send()
        o_all(hf).wait_send()


def solution(mesh):
    tok_spec = P(('dp', 'ctx'), None)
    pos_spec = P(('dp', 'ctx'))
    full_mat = P(None, None)
    full_vec = P(None)
    col_spec = P(None, 'tp')
    row_spec = P('tp', None)

    def local_step(tok_x, tok_pos, w_dq, g_q, w_uq, w_qr, w_dkv, g_kv, w_kr, w_uk, w_uv, w_o):
        rows, D = tok_x.shape
        half = rows // 2
        QR = w_dq.shape[1]
        LR = w_dkv.shape[1]
        HL = w_qr.shape[1] // w_kr.shape[1]
        scale = (128 + w_kr.shape[1]) ** -0.5
        nblk = D // 2 // NBLK
        ngrp = HL // 8
        ntok = 8 * half
        dims = (D, QR, LR, HL, half, scale)
        anyspec = pl.BlockSpec(memory_space=pl.ANY)
        vspec = pl.BlockSpec(memory_space=pltpu.VMEM)
        dma = pltpu.SemaphoreType.DMA
        arena_rows = max(DQ_SLOTS * D, WO_SLOTS * HL * 128)
        return pl.pallas_call(
            functools.partial(layer_kernel, dims),
            out_shape=pltpu.VMEM((rows, D), BF16),
            in_specs=[anyspec, anyspec, anyspec, anyspec, anyspec, anyspec, anyspec, anyspec, anyspec, anyspec, anyspec, anyspec],
            out_specs=vspec,
            scratch_shapes=[
                pltpu.VMEM((2, half), jnp.int32),
                pltpu.VMEM((QR // 128, 128), BF16),
                pltpu.VMEM((LR // 128, 128), BF16),
                pltpu.VMEM((rows, D), BF16),
                pltpu.VMEM((half, D), BF16),
                pltpu.VMEM((max(D, 2 * ngrp * ntok), LR), BF16),
                pltpu.VMEM((64, D), BF16),
                pltpu.VMEM((2 * ngrp, LR, 512), BF16),
                pltpu.VMEM((arena_rows, NBLK), BF16),
                pltpu.VMEM((ntok, LR + 128), BF16),
                pltpu.VMEM((ntok, 128), BF16),
                pltpu.VMEM((ntok, 128), BF16),
                pltpu.VMEM((2, rows, QR), BF16),
                pltpu.VMEM((half, LR), F32),
                pltpu.VMEM((half, 64), F32),
                pltpu.VMEM((2, rows, 256), F32),
                pltpu.VMEM((RING, QR, 512), BF16),
                pltpu.VMEM((RING, QR, 256), BF16),
                pltpu.VMEM((rows, HL * 64), BF16),
                pltpu.VMEM((rows, HL * 32), BF16),
                pltpu.VMEM((2, rows, HL * 64), BF16),
                pltpu.VMEM((2, half, HL * 64), BF16),
                pltpu.VMEM((nblk, half, NBLK), F32),
                pltpu.VMEM((2 * nblk, half, NBLK), F32),
                pltpu.VMEM((max(nblk, 2 * QR // NBLK), half, NBLK), F32),
                dma((3,)), dma((KCH,)), dma((1,)), dma((1,)), dma((1,)), dma((KCH,)), dma((KCH,)), dma((DQ_SLOTS,)), dma((RING, 2)), dma((ngrp, 2)), dma((WO_SLOTS,)),
                dma((6,)), dma((8,)), dma((1,)), dma((1,)), dma((1,)), dma((1,)), dma((2,)), dma((2,)), dma((2,)), dma((2,)),
                dma((2, nblk // GROUP)), dma((2, nblk // GROUP)), dma((1,)), dma((1,)),
            ],
            compiler_params=pltpu.CompilerParams(collective_id=0, has_side_effects=True,
                                                 vmem_limit_bytes=62500 * 1000),
        )(tok_x, tok_pos.reshape(2, half), w_dq, g_q.reshape(QR // 128, 128), w_uq, w_qr, w_dkv, g_kv.reshape(LR // 128, 128), w_kr.T,
          w_uk, w_uv, w_o)

    return jax.shard_map(local_step, mesh=mesh,
                         in_specs=(tok_spec, pos_spec, full_mat, full_vec, col_spec, col_spec, full_mat, full_vec, full_mat, col_spec, col_spec, row_spec),
                         out_specs=tok_spec, check_vma=False)
```

```python
import functools

import jax
import jax.numpy as jnp
from jax import lax
from jax.experimental import pallas as pl
from jax.experimental.pallas import tpu as pltpu
from jax.sharding import PartitionSpec as P

ROPE_BASE = 10000.0
NORM_EPS = 1e-6
NEG_BIG = float("-inf")
MESH = pl.DeviceIdType.MESH
F32 = jnp.float32
BF16 = jnp.bfloat16

KCH = 6
NBLK = 256
RING = 4
DQ_SLOTS = 4
GROUP = 4
UNROLL = 4
KV_PIECES = ((0,), (1,), (2, 3), ())
WO_SLOTS = 6


def _dot(a, b):
    return jnp.dot(a, b, preferred_element_type=F32)


def _dot_nt(a, b):
    return lax.dot_general(a, b, (((1,), (1,)), ((), ())), preferred_element_type=F32)


def layer_kernel(dims, x_hbm, pos_hbm, wdq_hbm, gq_hbm, wuq_hbm, wqr_hbm, wdkv_hbm, gkv_hbm, wkr_hbm, wuk_hbm, wuv_hbm,
                 wo_hbm, y_ref,
                 pos_ref, gq_ref, gkv_ref, xc, x2, kvs, wkr, upw, arena, lat, kplo, kphi, cq, acckv, acckr, rot,
                 uqb, qrb, qn, qp, os, orx, sendb, recvb, ownb,
                 smsem, xsem, x2sem, xps, xpr, kvsem, krsem, qsem, upsem, wosem, lats, latr, cqs, cqr, hs, hr, rots, rotr, oss, osr, ps, pr, rs, rr):
    D, QR, LR, HL, half, score_scale = dims
    HC = HL // 2
    ngrp = HC // 4
    kc = D // KCH
    nb_q = QR // NBLK
    own_cols = D // 2
    nblk = own_cols // NBLK
    hv = HL * 128
    ntok = 8 * half
    tp = lax.axis_index("tp")
    ci = lax.axis_index("ctx")
    core = lax.rem(ci, 2)
    xpeer = lax.rem(ci + 2, 4)
    dpeer = ci + 1 - 2 * core
    pieces = (ci, 7 - ci)
    pair = lax.div(ci, 2)
    mine = tuple(pl.ds(pl.multiple_of(sl * half, half), half) for sl in (core, 1 - core))
    theirs = tuple(pl.ds(pl.multiple_of(sl * half, half), half) for sl in (1 - core, core))
    first_pos = (2 * half * lax.div(ci, 2), half * (6 - 2 * lax.div(ci, 2)))
    half_rows = (slice(0, half), slice(half, 2 * half))

    def x_copy(k):
        cols = pl.ds(pl.multiple_of(k * kc, 128), kc)
        return pltpu.make_async_copy(x_hbm.at[pl.ds(0, half), cols], xc.at[mine[0], cols], xsem.at[k])

    def x2_copy():
        return pltpu.make_async_copy(x_hbm.at[pl.ds(half, half), :], x2, x2sem.at[0])

    def x_share(rows):
        return pltpu.make_async_remote_copy(src_ref=x_hbm.at[pl.ds(0, half), :], dst_ref=xc.at[rows, :], send_sem=xps.at[0],
                                            recv_sem=xpr.at[0], device_id={"ctx": dpeer}, device_id_type=MESH)

    def a_copies(k):
        col = pl.multiple_of(k * kc, 128)
        return (pltpu.make_async_copy(wkr_hbm.at[:, pl.ds(col, kc)], wkr.at[:, pl.ds(col, kc)], krsem.at[k]),
                pltpu.make_async_copy(wdkv_hbm.at[pl.ds(col, kc), :], kvs.at[pl.ds(col, kc), :], kvsem.at[k]))

    def b_copy(m, n):
        s = lax.rem(m, DQ_SLOTS)
        return pltpu.make_async_copy(wdq_hbm.at[:, pl.ds(pl.multiple_of(n * NBLK, NBLK), NBLK)],
                                     arena.at[pl.ds(pl.multiple_of(s * D, D), D), :], wosem.at[s])

    def q_copies(g):
        i = lax.rem(g, ngrp) + core * ngrp
        s = lax.rem(g, RING)
        c4 = pl.ds(pl.multiple_of(i * 512, 512), 512)
        c2 = pl.ds(pl.multiple_of(i * 256, 256), 256)
        return (pltpu.make_async_copy(wuq_hbm.at[:, c4], uqb.at[s], qsem.at[s, 0]),
                pltpu.make_async_copy(wqr_hbm.at[:, c2], qrb.at[s], qsem.at[s, 1]))

    def up_copies(i):
        c4 = pl.ds(pl.multiple_of((i + core * ngrp) * 512, 512), 512)
        return (pltpu.make_async_copy(wuk_hbm.at[:, c4], upw.at[i], upsem.at[i, 0]),
                pltpu.make_async_copy(wuv_hbm.at[:, c4], upw.at[ngrp + i], upsem.at[i, 1]))

    def wo_copy(L):
        j = lax.rem(L, nblk)
        side = jnp.where(L < 2 * nblk, 1 - tp, tp)
        s = lax.rem(L, WO_SLOTS)
        col = pl.multiple_of(side * own_cols + j * NBLK, NBLK)
        return pltpu.make_async_copy(wo_hbm.at[:, pl.ds(col, NBLK)],
                                     arena.at[pl.ds(pl.multiple_of(s * hv, hv), hv), :], wosem.at[s])

    def start(cps):
        for c in cps:
            c.start()

    def wait(cps):
        for c in cps:
            c.wait()

    bar = pltpu.get_barrier_semaphore()
    for dev in ({"ctx": xpeer}, {"tp": 1 - tp}, {"ctx": dpeer}):
        pl.semaphore_signal(bar, inc=1, device_id=dev, device_id_type=MESH)

    small = (pltpu.make_async_copy(pos_hbm, pos_ref, smsem.at[0]), pltpu.make_async_copy(gkv_hbm, gkv_ref, smsem.at[1]),
             pltpu.make_async_copy(gq_hbm, gq_ref, smsem.at[2]))
    start(small)
    for k in range(KCH):
        x_copy(k).start()
        start(a_copies(k))

    lane = lax.broadcasted_iota(jnp.int32, (1, 128), 1)
    first_half = lax.rem(lane, 64) < 32

    def rotary(hf):
        fidx = lax.rem(lane, 32)
        freq = jnp.zeros((1, 128), F32)
        for j in range(32):
            freq = jnp.where(fidx == j, ROPE_BASE ** (-j * 2.0 / 64), freq)
        eye = (lax.broadcasted_iota(jnp.int32, (half, half), 0) == lax.broadcasted_iota(jnp.int32, (half, half), 1))
        prow = pos_ref[hf:hf + 1, :].astype(F32)
        pcol = jnp.sum(jnp.where(eye, jnp.broadcast_to(prow, (half, half)), 0.0), axis=1, keepdims=True)
        ang = pcol * freq
        rot[hf, mine[hf], 0:128] = jnp.cos(ang)
        sn = jnp.sin(ang)
        rot[hf, mine[hf], 128:256] = jnp.where(first_half, -sn, sn)

    def turn(a, table):
        swapped = jnp.where(first_half, pltpu.roll(a, 96, 1), pltpu.roll(a, 32, 1))
        return a * table[:, 0:128] + swapped * table[:, 128:256]

    def to_core(ref, ssem, rsem):
        return pltpu.make_async_remote_copy(src_ref=ref, dst_ref=ref, send_sem=ssem, recv_sem=rsem,
                                            device_id={"ctx": dpeer}, device_id_type=MESH)

    def rot_send(hf):
        return to_core(rot.at[hf, mine[hf], :], rots.at[hf], rotr.at[hf])

    def rot_recv(hf):
        return to_core(rot.at[hf, theirs[hf], :], rots.at[hf], rotr.at[hf])

    def lat_send(piece, dev):
        ref = lat.at[pl.ds(pl.multiple_of(piece * half, half), half), :]
        return pltpu.make_async_remote_copy(src_ref=ref, dst_ref=ref, send_sem=lats.at[0], recv_sem=latr.at[piece],
                                            device_id={"ctx": dev}, device_id_type=MESH)

    def lat_finish(hf, a, kr):
        inv = lax.rsqrt(jnp.mean(a * a, axis=-1, keepdims=True) + NORM_EPS)
        kr2 = turn(jnp.concatenate([kr, kr], axis=1), rot[hf, mine[hf], :])
        row0 = pl.multiple_of(pieces[hf] * half, half)
        for c in range(LR // 128):
            cols = slice(c * 128, (c + 1) * 128)
            lat[pl.ds(row0, half), cols] = (a[:, cols] * inv * gkv_ref[c:c + 1, :].astype(F32)).astype(BF16)
        lat[pl.ds(row0, half), LR:LR + 128] = kr2.astype(BF16)

    def lat_share(hf):
        lat_send(pieces[hf], xpeer).start()
        lat_send(pieces[hf], dpeer).start()

    far = (xpeer, 7 - xpeer)
    near = (dpeer, 7 - dpeer)
    relayed = (3 - ci, 4 + ci)

    def lat_recv(piece):
        lat_send(piece, dpeer).wait_recv()

    def forward(hf):
        lat_recv(far[hf])
        lat_send(far[hf], dpeer).start()

    def split_rope(lo, hi):
        rows = slice(lo, hi)
        kp = lat[rows, LR:LR + 128].astype(F32)
        low = lane < 64
        kplo[rows, :] = jnp.where(low, kp, 0.0).astype(BF16)
        kphi[rows, :] = jnp.where(low, 0.0, kp).astype(BF16)

    nb_c = nb_q // 2

    def half_send(m):
        ref = ownb.at[pl.ds(2 * (core * nb_c + m), 2)]
        return to_core(ref, hs.at[0], hr.at[0])

    def half_all(side):
        ref = ownb.at[pl.ds(2 * side * nb_c, 2 * nb_c)]
        return to_core(ref, hs.at[0], hr.at[0])

    def norm_queries(chunk, rows, block):
        sq = 0.0
        for n in range(nb_q):
            a = ownb[block(n)]
            sq = sq + jnp.sum(a * a, axis=-1, keepdims=True)
        inv = lax.rsqrt(sq * (1.0 / QR) + NORM_EPS)
        for n in range(nb_q):
            a = ownb[block(n)] * inv
            for u in range(NBLK // 128):
                c = n * (NBLK // 128) + u
                cq[chunk, rows, c * 128:(c + 1) * 128] = (
                    a[:, u * 128:(u + 1) * 128] * gq_ref[c:c + 1, :].astype(F32)).astype(BF16)

    def cq_share(rows):
        return to_core(cq.at[1, rows, :], cqs.at[0], cqr.at[0])

    def queries(chunk):
        def body(t, carry):
            if chunk == 0:
                @pl.when(jnp.logical_and(t == 1, pair == 1))
                def _():
                    forward(0)
            gs = [2 * t + u + chunk * ngrp for u in range(2)]
            for g in gs:
                wait(q_copies(g))
            c = cq[chunk]
            for u in range(2):
                i = 2 * t + u
                s = lax.rem(gs[u], RING)
                r = _dot(c, qrb[s])
                qn[:, pl.ds(pl.multiple_of(i * 512, 512), 512)] = _dot(c, uqb[s]).astype(BF16)
                for v in range(2):
                    qp[:, pl.ds(pl.multiple_of(i * 256 + v * 128, 128), 128)] = turn(
                        r[:, v * 128:(v + 1) * 128], rot[chunk]).astype(BF16)
            for g in gs:
                @pl.when(g + RING < 2 * ngrp)
                def _():
                    start(q_copies(g + RING))
            return carry

        lax.fori_loop(0, ngrp // 2, body, 0)

    def kv_rows(i, n):
        if isinstance(i, int):
            return slice(i * ntok, i * ntok + n)
        return pl.ds(pl.multiple_of(i * ntok, ntok), n)

    def kv_part(i, quarter, nk):
        m = i + ngrp * (quarter // 2)
        cols = slice(256 * (quarter % 2), 256 * (quarter % 2) + 256)
        kvs[m * ntok:m * ntok + nk, cols] = _dot(lat[0:nk, 0:LR], upw[m, :, cols]).astype(BF16)

    def keys_values(chunk, nk):
        if chunk == 0:
            for i in range(ngrp):
                wait(up_copies(i))
            for quarter in range(4):
                kv_part(0, quarter, nk)
            return

        def body(i, carry):
            lt = lat[0:nk, 0:LR]
            kvs[kv_rows(i, nk), :] = _dot(lt, upw[i]).astype(BF16)
            kvs[kv_rows(ngrp + i, nk), :] = _dot(lt, upw[ngrp + i]).astype(BF16)
            return carry

        lax.fori_loop(0, ngrp, body, 0)

    c2e = score_scale * 1.4426950408889634

    def o_send(chunk, i):
        cols = pl.ds(pl.multiple_of(i * 512, 512), 512)
        return pltpu.make_async_remote_copy(src_ref=os.at[chunk, theirs[chunk], cols], dst_ref=orx.at[chunk, :, cols],
                                            send_sem=oss.at[chunk], recv_sem=osr.at[chunk],
                                            device_id={"ctx": dpeer}, device_id_type=MESH)

    def attention(chunk, nk, clear):
        nq = 2 * half

        vis = (lax.broadcasted_iota(jnp.int32, (nq, nk - clear), 1)
               <= lax.broadcasted_iota(jnp.int32, (nq, nk - clear), 0) + (first_pos[chunk] - clear))

        def scores(i, h):
            kp = kphi if h % 2 else kplo
            qpe = qp[:, pl.ds(pl.multiple_of(i * 256 + (h // 2) * 128, 128), 128)]
            qh = jnp.concatenate([qn[:, pl.ds(pl.multiple_of(i * 512 + h * 128, 128), 128)], qpe], axis=1)
            kh = jnp.concatenate([kvs[kv_rows(i, nk), h * 128:(h + 1) * 128], kp[0:nk, :]], axis=1)
            return _dot_nt(qh, kh)

        def values(i, h, sc):
            late = jnp.where(vis, sc[:, clear:], NEG_BIG)
            sc = jnp.concatenate([sc[:, :clear], late], axis=1) if clear else late
            top = jnp.max(sc, axis=1, keepdims=True)
            p = jnp.exp2((sc - top) * c2e)
            tot = jnp.sum(p, axis=1, keepdims=True)
            acc = _dot(p.astype(BF16), kvs[kv_rows(ngrp + i, nk), h * 128:(h + 1) * 128])
            os[chunk, :, pl.ds(pl.multiple_of(i * 512 + h * 128, 128), 128)] = (acc / tot).astype(BF16)

        per = UNROLL if chunk == 0 else 1

        def body(t, carry):
            for u in range(per):
                wo_copy(chunk * nblk + per * t + u).start()

            def rest():
                for extra in range(ngrp, WO_SLOTS - 1):
                    wo_copy(chunk * nblk + extra).start()

            if per == ngrp:
                rest()
            else:
                pl.when(t == ngrp // per - 1)(rest)
            sc = scores(per * t, 0)
            for u in range(4 * per):
                i, h = per * t + u // 4, u % 4
                nxt = scores(per * t + (u + 1) // 4, (u + 1) % 4) if u + 1 < 4 * per else None
                if per == ngrp and i + 1 < ngrp:
                    for quarter in KV_PIECES[h]:
                        kv_part(i + 1, quarter, nk)
                values(i, h, sc)
                sc = nxt
                if h == 3:
                    o_send(chunk, i).start()
            return carry

        if per == ngrp:
            body(0, 0)
        else:
            lax.fori_loop(0, ngrp // per, body, 0)

    def o_all(chunk):
        return pltpu.make_async_remote_copy(src_ref=os.at[chunk, theirs[chunk], :], dst_ref=orx.at[chunk],
                                            send_sem=oss.at[chunk], recv_sem=osr.at[chunk],
                                            device_id={"ctx": dpeer}, device_id_type=MESH)

    total_wo = 3 * nblk
    ahead = WO_SLOTS - 1
    hc = HC * 128

    def wo_next(L):
        wo_copy(L).wait()
        wo_refill(L)

    def wo_refill(L):
        @pl.when(jnp.logical_and(L + ahead < total_wo, jnp.logical_or(L >= nblk, L + ahead < nblk)))
        def _():
            wo_copy(L + ahead).start()

    def project_here(chunk, L):
        w = arena[pl.ds(pl.multiple_of(lax.rem(L, WO_SLOTS) * hv + core * hc, hc), hc), :]
        return _dot(os[chunk, mine[chunk], :], w)

    def project_there(chunk, L):
        w = arena[pl.ds(pl.multiple_of(lax.rem(L, WO_SLOTS) * hv + (1 - core) * hc, hc), hc), :]
        return _dot(orx[chunk], w)

    def part_copy(chunk, q, src, dst):
        return pltpu.make_async_remote_copy(src_ref=src, dst_ref=dst, send_sem=ps.at[chunk, q], recv_sem=pr.at[chunk, q],
                                            device_id={"tp": 1 - tp}, device_id_type=MESH)

    def part_send(chunk, j):
        return part_copy(chunk, lax.div(j, GROUP), sendb.at[j], recvb.at[chunk * nblk + j])

    def part_group(chunk, q):
        return part_copy(chunk, q, sendb.at[pl.ds(q * GROUP, GROUP)], recvb.at[pl.ds(chunk * nblk + q * GROUP, GROUP)])

    def project_partner(chunk):
        early = 2
        base = chunk * nblk

        def send_slot(j):
            if chunk == 1:
                @pl.when(lax.rem(j, GROUP) == 0)
                def _():
                    part_group(0, lax.div(j, GROUP)).wait_send()

        for j in range(early):
            wo_copy(base + j).wait()
            if j == 0:
                wo_refill(base)
            send_slot(j)
            sendb[j] = project_here(chunk, base + j)
        o_all(chunk).wait_recv()
        for j in range(early):
            sendb[j] += project_there(chunk, base + j)
            part_send(chunk, j).start()
            if j + 1 < early:
                wo_refill(base + j + 1)

        def body(j, carry):
            wo_next(base + j)
            send_slot(j)
            sendb[j] = project_here(chunk, base + j) + project_there(chunk, base + j)
            part_send(chunk, j).start()
            return carry

        lax.fori_loop(early, nblk, body, 0)

    def y_cols(side, j, n):
        return pl.ds(pl.multiple_of(side * own_cols + j * NBLK, NBLK), n)

    def result_copy(ref):
        return pltpu.make_async_remote_copy(src_ref=ref, dst_ref=ref, send_sem=rs.at[0], recv_sem=rr.at[0],
                                            device_id={"tp": 1 - tp}, device_id_type=MESH)

    def give_back(chunk, j, own):
        @pl.when(lax.rem(j, GROUP) == 0)
        def _():
            part_group(chunk, lax.div(j, GROUP)).wait_recv()
        cols = y_cols(tp, j, NBLK)
        y_ref[half_rows[chunk], cols] = (recvb[chunk * nblk + j] + own).astype(BF16)

        @pl.when(lax.rem(j, GROUP) == GROUP - 1)
        def _():
            result_copy(y_ref.at[half_rows[chunk], y_cols(tp, j - (GROUP - 1), GROUP * NBLK)]).start()

    acckv[...] = jnp.zeros_like(acckv)
    acckr[...] = jnp.zeros_like(acckr)
    def a_step(k, carry):
        x_copy(k).wait()
        wait(a_copies(k))

        @pl.when(k == 3)
        def _():
            wait(small)
            rotary(0)

        @pl.when(jnp.logical_and(lax.rem(k, 2) == 0, k < 2 * nb_c - 2))
        def _():
            m = lax.div(k, 2) + 1
            b_copy(m, core * nb_c + m).start()

        @pl.when(k == KCH - 1)
        def _():
            start(q_copies(0))
        cols = pl.ds(pl.multiple_of(k * kc, 128), kc)
        xk = xc[mine[0], cols]
        acckv[...] += _dot(xk, kvs[cols, :])
        acckr[...] += _dot_nt(xk, wkr[:, cols])
        return carry

    b_copy(0, core * nb_c).start()
    pl.semaphore_wait(bar, 3)
    x_share(mine[0]).start()
    with jax.named_scope('lat0'):
        lax.fori_loop(0, KCH, a_step, 0)
        x2_copy().start()
        lat_finish(0, acckv[...], acckr[...])
        lat_share(0)
        rot_send(0).start()
    with jax.named_scope('xwait'):
        x_share(theirs[0]).wait_recv()

    def dq_block(m, rows):
        return _dot(rows, arena[pl.ds(pl.multiple_of(lax.rem(m, DQ_SLOTS) * D, D), D), :])

    def b_step(m, carry):
        n = core * nb_c + m
        b_copy(m, n).wait()
        start(q_copies(m + 1))
        r = dq_block(m, xc[...])
        ownb[2 * n] = r[:half]
        ownb[2 * n + 1] = r[half:]
        half_send(m).start()
        return carry

    with jax.named_scope('qlat0'):
        lax.fori_loop(0, nb_c, b_step, 0)
        for m in range(nb_c + 1, RING):
            start(q_copies(m))
        for i in range(ngrp):
            start(up_copies(i))
    with jax.named_scope('lat1'):
        x2_copy().wait()
        acckv[...] = _dot(x2[...], kvs[0:D, :])
    with jax.named_scope('qfin0'):
        half_all(1 - core).wait_recv()
        for sl in range(2):
            norm_queries(0, half_rows[sl], lambda n, sl=sl: 2 * n + sl)
        rot_recv(0).wait_recv()
    with jax.named_scope('q0'):
        queries(0)
    for which in range(2):
        @pl.when(pair == which)
        def _():
            nk = 2 * half * (which + 1)
            with jax.named_scope('gather0'):
                lat_recv(near[0])
                if which == 1:
                    lat_recv(relayed[0])
                split_rope(0, nk)
            with jax.named_scope('kv0'):
                keys_values(0, nk)
            with jax.named_scope('att0'):
                attention(0, nk, nk - 2 * half)
    with jax.named_scope('part0'):
        project_partner(0)

    def b1_step(n, carry):
        @pl.when(n + 3 < nb_q)
        def _():
            b_copy(n + 3, n + 3).start()
        b_copy(n, n).wait()
        ownb[n] = dq_block(n, x2[...])
        return carry

    with jax.named_scope('qlat1'):
        half_all(core).wait_send()
        for n in range(3):
            b_copy(n, n).start()
        rotary(1)
        rot_send(1).start()
        lat_finish(1, acckv[...], _dot_nt(x2[...], wkr[...]))
        lat_share(1)
        lax.fori_loop(0, nb_q, b1_step, 0)
        norm_queries(1, mine[1], lambda n: n)
        cq_share(mine[1]).start()
    with jax.named_scope('gather1'):
        forward(1)

        @pl.when(pair == 0)
        def _():
            forward(0)
            lat_recv(relayed[0])
            split_rope(2 * half, 4 * half)
        lat_recv(near[1])
        lat_recv(relayed[1])
        split_rope(4 * half, 8 * half)
    with jax.named_scope('kv1'):
        keys_values(1, 8 * half)
    with jax.named_scope('q1'):
        cq_share(theirs[1]).wait_recv()
        rot_recv(1).wait_recv()
        queries(1)
    with jax.named_scope('att1'):
        attention(1, 8 * half, 4 * half)
    with jax.named_scope('part1'):
        project_partner(1)

    def own_body(j, carry):
        L = 2 * nblk + j
        wo_next(L)
        ownb[j] = project_here(1, L) + project_there(1, L)
        give_back(0, j, project_here(0, L) + project_there(0, L))
        return carry

    with jax.named_scope('own'):
        lax.fori_loop(0, nblk, own_body, 0)

    def ret_body(j, carry):
        give_back(1, j, ownb[j])
        return carry

    with jax.named_scope('ret'):
        lax.fori_loop(0, nblk, ret_body, 0)

    with jax.named_scope('drain'):
        for q in range(nblk // GROUP):
            part_group(1, q).wait_send()
        result_copy(y_ref.at[:, y_cols(tp, 0, own_cols)]).wait_send()
        result_copy(y_ref.at[:, y_cols(1 - tp, 0, own_cols)]).wait_recv()
    six = lat.at[pl.ds(0, 6 * half), :]
    pltpu.make_async_remote_copy(src_ref=six, dst_ref=six, send_sem=lats.at[0], recv_sem=latr.at[0],
                                 device_id={"ctx": dpeer}, device_id_type=MESH).wait_send()
    x_share(mine[0]).wait_send()
    cq_share(mine[1]).wait_send()
    for hf in range(2):
        rot_send(hf).wait_send()
        o_all(hf).wait_send()


def solution(mesh):
    tok_spec = P(('dp', 'ctx'), None)
    pos_spec = P(('dp', 'ctx'))
    full_mat = P(None, None)
    full_vec = P(None)
    col_spec = P(None, 'tp')
    row_spec = P('tp', None)

    def local_step(tok_x, tok_pos, w_dq, g_q, w_uq, w_qr, w_dkv, g_kv, w_kr, w_uk, w_uv, w_o):
        rows, D = tok_x.shape
        half = rows // 2
        QR = w_dq.shape[1]
        LR = w_dkv.shape[1]
        HL = w_qr.shape[1] // w_kr.shape[1]
        scale = (128 + w_kr.shape[1]) ** -0.5
        nblk = D // 2 // NBLK
        ngrp = HL // 8
        ntok = 8 * half
        dims = (D, QR, LR, HL, half, scale)
        anyspec = pl.BlockSpec(memory_space=pl.ANY)
        vspec = pl.BlockSpec(memory_space=pltpu.VMEM)
        dma = pltpu.SemaphoreType.DMA
        arena_rows = max(DQ_SLOTS * D, WO_SLOTS * HL * 128)
        return pl.pallas_call(
            functools.partial(layer_kernel, dims),
            out_shape=pltpu.VMEM((rows, D), BF16),
            in_specs=[anyspec, anyspec, anyspec, anyspec, anyspec, anyspec, anyspec, anyspec, anyspec, anyspec, anyspec, anyspec],
            out_specs=vspec,
            scratch_shapes=[
                pltpu.VMEM((2, half), jnp.int32),
                pltpu.VMEM((QR // 128, 128), BF16),
                pltpu.VMEM((LR // 128, 128), BF16),
                pltpu.VMEM((rows, D), BF16),
                pltpu.VMEM((half, D), BF16),
                pltpu.VMEM((max(D, 2 * ngrp * ntok), LR), BF16),
                pltpu.VMEM((64, D), BF16),
                pltpu.VMEM((2 * ngrp, LR, 512), BF16),
                pltpu.VMEM((arena_rows, NBLK), BF16),
                pltpu.VMEM((ntok, LR + 128), BF16),
                pltpu.VMEM((ntok, 128), BF16),
                pltpu.VMEM((ntok, 128), BF16),
                pltpu.VMEM((2, rows, QR), BF16),
                pltpu.VMEM((half, LR), F32),
                pltpu.VMEM((half, 64), F32),
                pltpu.VMEM((2, rows, 256), F32),
                pltpu.VMEM((RING, QR, 512), BF16),
                pltpu.VMEM((RING, QR, 256), BF16),
                pltpu.VMEM((rows, HL * 64), BF16),
                pltpu.VMEM((rows, HL * 32), BF16),
                pltpu.VMEM((2, rows, HL * 64), BF16),
                pltpu.VMEM((2, half, HL * 64), BF16),
                pltpu.VMEM((nblk, half, NBLK), F32),
                pltpu.VMEM((2 * nblk, half, NBLK), F32),
                pltpu.VMEM((max(nblk, 2 * QR // NBLK), half, NBLK), F32),
                dma((3,)), dma((KCH,)), dma((1,)), dma((1,)), dma((1,)), dma((KCH,)), dma((KCH,)), dma((RING, 2)), dma((ngrp, 2)), dma((WO_SLOTS,)),
                dma((1,)), dma((8,)), dma((1,)), dma((1,)), dma((1,)), dma((1,)), dma((2,)), dma((2,)), dma((2,)), dma((2,)),
                dma((2, nblk // GROUP)), dma((2, nblk // GROUP)), dma((1,)), dma((1,)),
            ],
            compiler_params=pltpu.CompilerParams(collective_id=0, has_side_effects=True,
                                                 vmem_limit_bytes=62500 * 1000),
        )(tok_x, tok_pos.reshape(2, half), w_dq, g_q.reshape(QR // 128, 128), w_uq, w_qr, w_dkv, g_kv.reshape(LR // 128, 128), w_kr.T,
          w_uk, w_uv, w_o)

    return jax.shard_map(local_step, mesh=mesh,
                         in_specs=(tok_spec, pos_spec, full_mat, full_vec, col_spec, col_spec, full_mat, full_vec, full_mat, col_spec, col_spec, row_spec),
                         out_specs=tok_spec, check_vma=False)
```

```python
import functools

import jax
import jax.numpy as jnp
from jax import lax
from jax.experimental import pallas as pl
from jax.experimental.pallas import tpu as pltpu
from jax.sharding import PartitionSpec as P

ROPE_BASE = 10000.0
NORM_EPS = 1e-6
NEG_BIG = float("-inf")
MESH = pl.DeviceIdType.MESH
F32 = jnp.float32
BF16 = jnp.bfloat16

KCH = 6
NBLK = 256
RING = 4
DQ_SLOTS = 4
GROUP = 4
UNROLL = 4
KV_PIECES = ((0,), (1,), (2, 3), ())
WO_SLOTS = 6


def _dot(a, b):
    return jnp.dot(a, b, preferred_element_type=F32)


def _dot_nt(a, b):
    return lax.dot_general(a, b, (((1,), (1,)), ((), ())), preferred_element_type=F32)


def layer_kernel(dims, x_hbm, pos_hbm, wdq_hbm, gq_hbm, wuq_hbm, wqr_hbm, wdkv_hbm, gkv_hbm, wkr_hbm, wuk_hbm, wuv_hbm,
                 wo_hbm, y_ref,
                 pos_ref, gq_ref, gkv_ref, xc, x2, kvs, wkr, upw, arena, lat, kplo, kphi, cq, acckv, acckr, rot,
                 uqb, qrb, qn, qp, os, orx, sendb, recvb, ownb,
                 smsem, xsem, x2sem, xps, xpr, kvsem, krsem, qsem, upsem, wosem, lats, latr, cqs, cqr, hs, hr, rots, rotr, oss, osr, ps, pr, rs, rr):
    D, QR, LR, HL, half, score_scale = dims
    HC = HL // 2
    ngrp = HC // 4
    kc = D // KCH
    nb_q = QR // NBLK
    own_cols = D // 2
    nblk = own_cols // NBLK
    hv = HL * 128
    ntok = 8 * half
    tp = lax.axis_index("tp")
    ci = lax.axis_index("ctx")
    core = lax.rem(ci, 2)
    xpeer = lax.rem(ci + 2, 4)
    dpeer = ci + 1 - 2 * core
    pieces = (ci, 7 - ci)
    pair = lax.div(ci, 2)
    mine = tuple(pl.ds(pl.multiple_of(sl * half, half), half) for sl in (core, 1 - core))
    theirs = tuple(pl.ds(pl.multiple_of(sl * half, half), half) for sl in (1 - core, core))
    first_pos = (2 * half * lax.div(ci, 2), half * (6 - 2 * lax.div(ci, 2)))
    half_rows = (slice(0, half), slice(half, 2 * half))

    def x_copy(k):
        cols = pl.ds(pl.multiple_of(k * kc, 128), kc)
        return pltpu.make_async_copy(x_hbm.at[pl.ds(0, half), cols], xc.at[mine[0], cols], xsem.at[k])

    def x2_copy():
        return pltpu.make_async_copy(x_hbm.at[pl.ds(half, half), :], x2, x2sem.at[0])

    def x_share(rows):
        return pltpu.make_async_remote_copy(src_ref=x_hbm.at[pl.ds(0, half), :], dst_ref=xc.at[rows, :], send_sem=xps.at[0],
                                            recv_sem=xpr.at[0], device_id={"ctx": dpeer}, device_id_type=MESH)

    def a_copies(k):
        col = pl.multiple_of(k * kc, 128)
        return (pltpu.make_async_copy(wkr_hbm.at[:, pl.ds(col, kc)], wkr.at[:, pl.ds(col, kc)], krsem.at[k]),
                pltpu.make_async_copy(wdkv_hbm.at[pl.ds(col, kc), :], kvs.at[pl.ds(col, kc), :], kvsem.at[k]))

    def b_copy(m, n):
        s = lax.rem(m, DQ_SLOTS)
        return pltpu.make_async_copy(wdq_hbm.at[:, pl.ds(pl.multiple_of(n * NBLK, NBLK), NBLK)],
                                     arena.at[pl.ds(pl.multiple_of(s * D, D), D), :], wosem.at[s])

    def q_copies(g):
        i = lax.rem(g, ngrp) + core * ngrp
        s = lax.rem(g, RING)
        c4 = pl.ds(pl.multiple_of(i * 512, 512), 512)
        c2 = pl.ds(pl.multiple_of(i * 256, 256), 256)
        return (pltpu.make_async_copy(wuq_hbm.at[:, c4], uqb.at[s], qsem.at[s, 0]),
                pltpu.make_async_copy(wqr_hbm.at[:, c2], qrb.at[s], qsem.at[s, 1]))

    def up_copies(i):
        c4 = pl.ds(pl.multiple_of((i + core * ngrp) * 512, 512), 512)
        return (pltpu.make_async_copy(wuk_hbm.at[:, c4], upw.at[i], upsem.at[i, 0]),
                pltpu.make_async_copy(wuv_hbm.at[:, c4], upw.at[ngrp + i], upsem.at[i, 1]))

    def wo_copy(L):
        j = lax.rem(L, nblk)
        side = jnp.where(L < 2 * nblk, 1 - tp, tp)
        s = lax.rem(L, WO_SLOTS)
        col = pl.multiple_of(side * own_cols + j * NBLK, NBLK)
        return pltpu.make_async_copy(wo_hbm.at[:, pl.ds(col, NBLK)],
                                     arena.at[pl.ds(pl.multiple_of(s * hv, hv), hv), :], wosem.at[s])

    def start(cps):
        for c in cps:
            c.start()

    def wait(cps):
        for c in cps:
            c.wait()

    bar = pltpu.get_barrier_semaphore()
    for dev in ({"ctx": xpeer}, {"tp": 1 - tp}, {"ctx": dpeer}):
        pl.semaphore_signal(bar, inc=1, device_id=dev, device_id_type=MESH)

    small = (pltpu.make_async_copy(pos_hbm, pos_ref, smsem.at[0]), pltpu.make_async_copy(gkv_hbm, gkv_ref, smsem.at[1]),
             pltpu.make_async_copy(gq_hbm, gq_ref, smsem.at[2]))
    start(small)
    for k in range(KCH):
        x_copy(k).start()
        start(a_copies(k))

    lane = lax.broadcasted_iota(jnp.int32, (1, 128), 1)
    first_half = lax.rem(lane, 64) < 32

    def rotary(hf):
        fidx = lax.rem(lane, 32)
        freq = jnp.zeros((1, 128), F32)
        for j in range(32):
            freq = jnp.where(fidx == j, ROPE_BASE ** (-j * 2.0 / 64), freq)
        eye = (lax.broadcasted_iota(jnp.int32, (half, half), 0) == lax.broadcasted_iota(jnp.int32, (half, half), 1))
        prow = pos_ref[hf:hf + 1, :].astype(F32)
        pcol = jnp.sum(jnp.where(eye, jnp.broadcast_to(prow, (half, half)), 0.0), axis=1, keepdims=True)
        ang = pcol * freq
        rot[hf, mine[hf], 0:128] = jnp.cos(ang)
        sn = jnp.sin(ang)
        rot[hf, mine[hf], 128:256] = jnp.where(first_half, -sn, sn)

    def turn(a, table):
        swapped = jnp.where(first_half, pltpu.roll(a, 96, 1), pltpu.roll(a, 32, 1))
        return a * table[:, 0:128] + swapped * table[:, 128:256]

    def to_core(ref, ssem, rsem):
        return pltpu.make_async_remote_copy(src_ref=ref, dst_ref=ref, send_sem=ssem, recv_sem=rsem,
                                            device_id={"ctx": dpeer}, device_id_type=MESH)

    def rot_send(hf):
        return to_core(rot.at[hf, mine[hf], :], rots.at[hf], rotr.at[hf])

    def rot_recv(hf):
        return to_core(rot.at[hf, theirs[hf], :], rots.at[hf], rotr.at[hf])

    def lat_send(piece, dev):
        ref = lat.at[pl.ds(pl.multiple_of(piece * half, half), half), :]
        return pltpu.make_async_remote_copy(src_ref=ref, dst_ref=ref, send_sem=lats.at[0], recv_sem=latr.at[piece],
                                            device_id={"ctx": dev}, device_id_type=MESH)

    def lat_finish(hf, a, kr):
        inv = lax.rsqrt(jnp.mean(a * a, axis=-1, keepdims=True) + NORM_EPS)
        kr2 = turn(jnp.concatenate([kr, kr], axis=1), rot[hf, mine[hf], :])
        row0 = pl.multiple_of(pieces[hf] * half, half)
        for c in range(LR // 128):
            cols = slice(c * 128, (c + 1) * 128)
            lat[pl.ds(row0, half), cols] = (a[:, cols] * inv * gkv_ref[c:c + 1, :].astype(F32)).astype(BF16)
        lat[pl.ds(row0, half), LR:LR + 128] = kr2.astype(BF16)

    def lat_share(hf):
        lat_send(pieces[hf], xpeer).start()
        lat_send(pieces[hf], dpeer).start()

    far = (xpeer, 7 - xpeer)
    near = (dpeer, 7 - dpeer)
    relayed = (3 - ci, 4 + ci)

    def lat_recv(piece):
        lat_send(piece, dpeer).wait_recv()

    def forward(hf):
        lat_recv(far[hf])
        lat_send(far[hf], dpeer).start()

    def split_rope(lo, hi):
        rows = slice(lo, hi)
        kp = lat[rows, LR:LR + 128].astype(F32)
        low = lane < 64
        kplo[rows, :] = jnp.where(low, kp, 0.0).astype(BF16)
        kphi[rows, :] = jnp.where(low, 0.0, kp).astype(BF16)

    nb_c = nb_q // 2

    def half_send(m):
        ref = ownb.at[pl.ds(2 * (core * nb_c + m), 2)]
        return to_core(ref, hs.at[0], hr.at[0])

    def half_all(side):
        ref = ownb.at[pl.ds(2 * side * nb_c, 2 * nb_c)]
        return to_core(ref, hs.at[0], hr.at[0])

    def norm_queries(chunk, rows, block):
        sq = 0.0
        for n in range(nb_q):
            a = ownb[block(n)]
            sq = sq + jnp.sum(a * a, axis=-1, keepdims=True)
        inv = lax.rsqrt(sq * (1.0 / QR) + NORM_EPS)
        for n in range(nb_q):
            a = ownb[block(n)] * inv
            for u in range(NBLK // 128):
                c = n * (NBLK // 128) + u
                cq[chunk, rows, c * 128:(c + 1) * 128] = (
                    a[:, u * 128:(u + 1) * 128] * gq_ref[c:c + 1, :].astype(F32)).astype(BF16)

    def cq_share(rows):
        return to_core(cq.at[1, rows, :], cqs.at[0], cqr.at[0])

    def queries(chunk):
        per = ngrp if chunk == 0 else 2

        def body(t, carry):
            gs = [per * t + u + chunk * ngrp for u in range(per)]
            for g in gs:
                wait(q_copies(g))
            c = cq[chunk]
            for u in range(per):
                i = per * t + u
                s = lax.rem(gs[u], RING)
                r = _dot(c, qrb[s])
                qn[:, pl.ds(pl.multiple_of(i * 512, 512), 512)] = _dot(c, uqb[s]).astype(BF16)
                for v in range(2):
                    qp[:, pl.ds(pl.multiple_of(i * 256 + v * 128, 128), 128)] = turn(
                        r[:, v * 128:(v + 1) * 128], rot[chunk]).astype(BF16)
            for g in gs:
                @pl.when(g + RING < 2 * ngrp)
                def _():
                    start(q_copies(g + RING))
            return carry

        lax.fori_loop(0, ngrp // per, body, 0)

    def kv_rows(i, n):
        if isinstance(i, int):
            return slice(i * ntok, i * ntok + n)
        return pl.ds(pl.multiple_of(i * ntok, ntok), n)

    def kv_part(i, quarter, nk):
        m = i + ngrp * (quarter // 2)
        cols = slice(256 * (quarter % 2), 256 * (quarter % 2) + 256)
        kvs[m * ntok:m * ntok + nk, cols] = _dot(lat[0:nk, 0:LR], upw[m, :, cols]).astype(BF16)

    def keys_values(chunk, nk):
        if chunk == 0:
            for i in range(ngrp):
                wait(up_copies(i))
            for quarter in range(4):
                kv_part(0, quarter, nk)
            return

        def body(i, carry):
            lt = lat[0:nk, 0:LR]
            kvs[kv_rows(i, nk), :] = _dot(lt, upw[i]).astype(BF16)
            kvs[kv_rows(ngrp + i, nk), :] = _dot(lt, upw[ngrp + i]).astype(BF16)
            return carry

        lax.fori_loop(0, ngrp, body, 0)

    c2e = score_scale * 1.4426950408889634

    def o_send(chunk, i):
        cols = pl.ds(pl.multiple_of(i * 512, 512), 512)
        return pltpu.make_async_remote_copy(src_ref=os.at[chunk, theirs[chunk], cols], dst_ref=orx.at[chunk, :, cols],
                                            send_sem=oss.at[chunk], recv_sem=osr.at[chunk],
                                            device_id={"ctx": dpeer}, device_id_type=MESH)

    def attention(chunk, nk, clear):
        nq = 2 * half

        vis = (lax.broadcasted_iota(jnp.int32, (nq, nk - clear), 1)
               <= lax.broadcasted_iota(jnp.int32, (nq, nk - clear), 0) + (first_pos[chunk] - clear))

        def scores(i, h):
            kp = kphi if h % 2 else kplo
            qpe = qp[:, pl.ds(pl.multiple_of(i * 256 + (h // 2) * 128, 128), 128)]
            qh = jnp.concatenate([qn[:, pl.ds(pl.multiple_of(i * 512 + h * 128, 128), 128)], qpe], axis=1)
            kh = jnp.concatenate([kvs[kv_rows(i, nk), h * 128:(h + 1) * 128], kp[0:nk, :]], axis=1)
            return _dot_nt(qh, kh)

        def values(i, h, sc):
            late = jnp.where(vis, sc[:, clear:], NEG_BIG)
            sc = jnp.concatenate([sc[:, :clear], late], axis=1) if clear else late
            top = jnp.max(sc, axis=1, keepdims=True)
            p = jnp.exp2((sc - top) * c2e)
            tot = jnp.sum(p, axis=1, keepdims=True)
            acc = _dot(p.astype(BF16), kvs[kv_rows(ngrp + i, nk), h * 128:(h + 1) * 128])
            os[chunk, :, pl.ds(pl.multiple_of(i * 512 + h * 128, 128), 128)] = (acc / tot).astype(BF16)

        per = UNROLL if chunk == 0 else 1

        def body(t, carry):
            for u in range(per):
                wo_copy(chunk * nblk + per * t + u).start()

            def rest():
                for extra in range(ngrp, WO_SLOTS - 1):
                    wo_copy(chunk * nblk + extra).start()

            if per == ngrp:
                rest()
            else:
                pl.when(t == ngrp // per - 1)(rest)
            sc = scores(per * t, 0)
            for u in range(4 * per):
                i, h = per * t + u // 4, u % 4
                nxt = scores(per * t + (u + 1) // 4, (u + 1) % 4) if u + 1 < 4 * per else None
                if per == ngrp and i + 1 < ngrp:
                    for quarter in KV_PIECES[h]:
                        kv_part(i + 1, quarter, nk)
                values(i, h, sc)
                sc = nxt
                if h == 3:
                    o_send(chunk, i).start()
            return carry

        if per == ngrp:
            body(0, 0)
        else:
            lax.fori_loop(0, ngrp // per, body, 0)

    def o_all(chunk):
        return pltpu.make_async_remote_copy(src_ref=os.at[chunk, theirs[chunk], :], dst_ref=orx.at[chunk],
                                            send_sem=oss.at[chunk], recv_sem=osr.at[chunk],
                                            device_id={"ctx": dpeer}, device_id_type=MESH)

    total_wo = 3 * nblk
    ahead = WO_SLOTS - 1
    hc = HC * 128

    def wo_next(L):
        wo_copy(L).wait()
        wo_refill(L)

    def wo_refill(L):
        @pl.when(jnp.logical_and(L + ahead < total_wo, jnp.logical_or(L >= nblk, L + ahead < nblk)))
        def _():
            wo_copy(L + ahead).start()

    def project_here(chunk, L):
        w = arena[pl.ds(pl.multiple_of(lax.rem(L, WO_SLOTS) * hv + core * hc, hc), hc), :]
        return _dot(os[chunk, mine[chunk], :], w)

    def project_there(chunk, L):
        w = arena[pl.ds(pl.multiple_of(lax.rem(L, WO_SLOTS) * hv + (1 - core) * hc, hc), hc), :]
        return _dot(orx[chunk], w)

    def part_copy(chunk, q, src, dst):
        return pltpu.make_async_remote_copy(src_ref=src, dst_ref=dst, send_sem=ps.at[chunk, q], recv_sem=pr.at[chunk, q],
                                            device_id={"tp": 1 - tp}, device_id_type=MESH)

    def part_send(chunk, j):
        return part_copy(chunk, lax.div(j, GROUP), sendb.at[j], recvb.at[chunk * nblk + j])

    def part_group(chunk, q):
        return part_copy(chunk, q, sendb.at[pl.ds(q * GROUP, GROUP)], recvb.at[pl.ds(chunk * nblk + q * GROUP, GROUP)])

    def project_partner(chunk):
        early = 2
        base = chunk * nblk

        def send_slot(j):
            if chunk == 1:
                @pl.when(lax.rem(j, GROUP) == 0)
                def _():
                    part_group(0, lax.div(j, GROUP)).wait_send()

        for j in range(early):
            wo_copy(base + j).wait()
            if j == 0:
                wo_refill(base)
            send_slot(j)
            sendb[j] = project_here(chunk, base + j)
        o_all(chunk).wait_recv()
        for j in range(early):
            sendb[j] += project_there(chunk, base + j)
            part_send(chunk, j).start()
            if j + 1 < early:
                wo_refill(base + j + 1)

        def body(j, carry):
            wo_next(base + j)
            send_slot(j)
            sendb[j] = project_here(chunk, base + j) + project_there(chunk, base + j)
            part_send(chunk, j).start()
            return carry

        lax.fori_loop(early, nblk, body, 0)

    def y_cols(side, j, n):
        return pl.ds(pl.multiple_of(side * own_cols + j * NBLK, NBLK), n)

    def result_copy(ref):
        return pltpu.make_async_remote_copy(src_ref=ref, dst_ref=ref, send_sem=rs.at[0], recv_sem=rr.at[0],
                                            device_id={"tp": 1 - tp}, device_id_type=MESH)

    def give_back(chunk, j, own):
        @pl.when(lax.rem(j, GROUP) == 0)
        def _():
            part_group(chunk, lax.div(j, GROUP)).wait_recv()
        cols = y_cols(tp, j, NBLK)
        y_ref[half_rows[chunk], cols] = (recvb[chunk * nblk + j] + own).astype(BF16)

        @pl.when(lax.rem(j, GROUP) == GROUP - 1)
        def _():
            result_copy(y_ref.at[half_rows[chunk], y_cols(tp, j - (GROUP - 1), GROUP * NBLK)]).start()

    acckv[...] = jnp.zeros_like(acckv)
    acckr[...] = jnp.zeros_like(acckr)
    def a_step(k, carry):
        x_copy(k).wait()
        wait(a_copies(k))

        @pl.when(k == 3)
        def _():
            wait(small)
            rotary(0)

        @pl.when(jnp.logical_and(lax.rem(k, 2) == 0, k < 2 * nb_c - 2))
        def _():
            m = lax.div(k, 2) + 1
            b_copy(m, core * nb_c + m).start()

        @pl.when(k == KCH - 1)
        def _():
            start(q_copies(0))
            start(q_copies(1))
        cols = pl.ds(pl.multiple_of(k * kc, 128), kc)
        xk = xc[mine[0], cols]
        acckv[...] += _dot(xk, kvs[cols, :])
        acckr[...] += _dot_nt(xk, wkr[:, cols])
        return carry

    b_copy(0, core * nb_c).start()
    pl.semaphore_wait(bar, 3)
    x_share(mine[0]).start()
    with jax.named_scope('lat0'):
        lax.fori_loop(0, KCH, a_step, 0)
        x2_copy().start()
        lat_finish(0, acckv[...], acckr[...])
        lat_share(0)
        rot_send(0).start()
    with jax.named_scope('xwait'):
        x_share(theirs[0]).wait_recv()

    def dq_block(m, rows):
        return _dot(rows, arena[pl.ds(pl.multiple_of(lax.rem(m, DQ_SLOTS) * D, D), D), :])

    def b_step(m, carry):
        n = core * nb_c + m
        b_copy(m, n).wait()

        @pl.when(m + 2 < RING)
        def _():
            start(q_copies(m + 2))
        r = dq_block(m, xc[...])
        ownb[2 * n] = r[:half]
        ownb[2 * n + 1] = r[half:]
        half_send(m).start()
        return carry

    with jax.named_scope('qlat0'):
        lax.fori_loop(0, nb_c, b_step, 0)
        for m in range(nb_c + 1, RING):
            start(q_copies(m))
        for i in range(ngrp):
            start(up_copies(i))
    with jax.named_scope('lat1'):
        x2_copy().wait()
        acckv[...] = _dot(x2[...], kvs[0:D, :])
    with jax.named_scope('qfin0'):
        half_all(1 - core).wait_recv()
        for sl in range(2):
            norm_queries(0, half_rows[sl], lambda n, sl=sl: 2 * n + sl)
        rot_recv(0).wait_recv()
    with jax.named_scope('q0'):
        @pl.when(pair == 1)
        def _():
            forward(0)
        queries(0)
    for which in range(2):
        @pl.when(pair == which)
        def _():
            nk = 2 * half * (which + 1)
            with jax.named_scope('gather0'):
                lat_recv(near[0])
                if which == 1:
                    lat_recv(relayed[0])
                split_rope(0, nk)
            with jax.named_scope('kv0'):
                keys_values(0, nk)
            with jax.named_scope('att0'):
                attention(0, nk, nk - 2 * half)
    with jax.named_scope('part0'):
        project_partner(0)

    def b1_step(n, carry):
        @pl.when(n + 3 < nb_q)
        def _():
            b_copy(n + 3, n + 3).start()
        b_copy(n, n).wait()
        ownb[n] = dq_block(n, x2[...])
        return carry

    with jax.named_scope('qlat1'):
        half_all(core).wait_send()
        for n in range(3):
            b_copy(n, n).start()
        rotary(1)
        rot_send(1).start()
        lat_finish(1, acckv[...], _dot_nt(x2[...], wkr[...]))
        lat_share(1)
        lax.fori_loop(0, nb_q, b1_step, 0)
        norm_queries(1, mine[1], lambda n: n)
        cq_share(mine[1]).start()
    with jax.named_scope('gather1'):
        forward(1)

        @pl.when(pair == 0)
        def _():
            forward(0)
            lat_recv(relayed[0])
            split_rope(2 * half, 4 * half)
        lat_recv(near[1])
        lat_recv(relayed[1])
        split_rope(4 * half, 8 * half)
    with jax.named_scope('kv1'):
        keys_values(1, 8 * half)
    with jax.named_scope('q1'):
        cq_share(theirs[1]).wait_recv()
        rot_recv(1).wait_recv()
        queries(1)
    with jax.named_scope('att1'):
        attention(1, 8 * half, 4 * half)
    with jax.named_scope('part1'):
        project_partner(1)

    def own_body(j, carry):
        L = 2 * nblk + j
        wo_next(L)
        ownb[j] = project_here(1, L) + project_there(1, L)
        give_back(0, j, project_here(0, L) + project_there(0, L))
        return carry

    with jax.named_scope('own'):
        lax.fori_loop(0, nblk, own_body, 0)

    def ret_body(j, carry):
        give_back(1, j, ownb[j])
        return carry

    with jax.named_scope('ret'):
        lax.fori_loop(0, nblk, ret_body, 0)

    with jax.named_scope('drain'):
        for q in range(nblk // GROUP):
            part_group(1, q).wait_send()
        result_copy(y_ref.at[:, y_cols(tp, 0, own_cols)]).wait_send()
        result_copy(y_ref.at[:, y_cols(1 - tp, 0, own_cols)]).wait_recv()
    six = lat.at[pl.ds(0, 6 * half), :]
    pltpu.make_async_remote_copy(src_ref=six, dst_ref=six, send_sem=lats.at[0], recv_sem=latr.at[0],
                                 device_id={"ctx": dpeer}, device_id_type=MESH).wait_send()
    x_share(mine[0]).wait_send()
    cq_share(mine[1]).wait_send()
    for hf in range(2):
        rot_send(hf).wait_send()
        o_all(hf).wait_send()


def solution(mesh):
    tok_spec = P(('dp', 'ctx'), None)
    pos_spec = P(('dp', 'ctx'))
    full_mat = P(None, None)
    full_vec = P(None)
    col_spec = P(None, 'tp')
    row_spec = P('tp', None)

    def local_step(tok_x, tok_pos, w_dq, g_q, w_uq, w_qr, w_dkv, g_kv, w_kr, w_uk, w_uv, w_o):
        rows, D = tok_x.shape
        half = rows // 2
        QR = w_dq.shape[1]
        LR = w_dkv.shape[1]
        HL = w_qr.shape[1] // w_kr.shape[1]
        scale = (128 + w_kr.shape[1]) ** -0.5
        nblk = D // 2 // NBLK
        ngrp = HL // 8
        ntok = 8 * half
        dims = (D, QR, LR, HL, half, scale)
        anyspec = pl.BlockSpec(memory_space=pl.ANY)
        vspec = pl.BlockSpec(memory_space=pltpu.VMEM)
        dma = pltpu.SemaphoreType.DMA
        arena_rows = max(DQ_SLOTS * D, WO_SLOTS * HL * 128)
        return pl.pallas_call(
            functools.partial(layer_kernel, dims),
            out_shape=pltpu.VMEM((rows, D), BF16),
            in_specs=[anyspec, anyspec, anyspec, anyspec, anyspec, anyspec, anyspec, anyspec, anyspec, anyspec, anyspec, anyspec],
            out_specs=vspec,
            scratch_shapes=[
                pltpu.VMEM((2, half), jnp.int32),
                pltpu.VMEM((QR // 128, 128), BF16),
                pltpu.VMEM((LR // 128, 128), BF16),
                pltpu.VMEM((rows, D), BF16),
                pltpu.VMEM((half, D), BF16),
                pltpu.VMEM((max(D, 2 * ngrp * ntok), LR), BF16),
                pltpu.VMEM((64, D), BF16),
                pltpu.VMEM((2 * ngrp, LR, 512), BF16),
                pltpu.VMEM((arena_rows, NBLK), BF16),
                pltpu.VMEM((ntok, LR + 128), BF16),
                pltpu.VMEM((ntok, 128), BF16),
                pltpu.VMEM((ntok, 128), BF16),
                pltpu.VMEM((2, rows, QR), BF16),
                pltpu.VMEM((half, LR), F32),
                pltpu.VMEM((half, 64), F32),
                pltpu.VMEM((2, rows, 256), F32),
                pltpu.VMEM((RING, QR, 512), BF16),
                pltpu.VMEM((RING, QR, 256), BF16),
                pltpu.VMEM((rows, HL * 64), BF16),
                pltpu.VMEM((rows, HL * 32), BF16),
                pltpu.VMEM((2, rows, HL * 64), BF16),
                pltpu.VMEM((2, half, HL * 64), BF16),
                pltpu.VMEM((nblk, half, NBLK), F32),
                pltpu.VMEM((2 * nblk, half, NBLK), F32),
                pltpu.VMEM((max(nblk, 2 * QR // NBLK), half, NBLK), F32),
                dma((3,)), dma((KCH,)), dma((1,)), dma((1,)), dma((1,)), dma((KCH,)), dma((KCH,)), dma((RING, 2)), dma((ngrp, 2)), dma((WO_SLOTS,)),
                dma((1,)), dma((8,)), dma((1,)), dma((1,)), dma((1,)), dma((1,)), dma((2,)), dma((2,)), dma((2,)), dma((2,)),
                dma((2, nblk // GROUP)), dma((2, nblk // GROUP)), dma((1,)), dma((1,)),
            ],
            compiler_params=pltpu.CompilerParams(collective_id=0, has_side_effects=True,
                                                 vmem_limit_bytes=62500 * 1000),
        )(tok_x, tok_pos.reshape(2, half), w_dq, g_q.reshape(QR // 128, 128), w_uq, w_qr, w_dkv, g_kv.reshape(LR // 128, 128), w_kr.T,
          w_uk, w_uv, w_o)

    return jax.shard_map(local_step, mesh=mesh,
                         in_specs=(tok_spec, pos_spec, full_mat, full_vec, col_spec, col_spec, full_mat, full_vec, full_mat, col_spec, col_spec, row_spec),
                         out_specs=tok_spec, check_vma=False)
```
